128 devices in a mesh: gx: 4 (over z), gy: 8 (over x_lo, y), gz: 4 (over x_hi, core).
Axes of the slice: x: 4 (x_hi: 2, x_lo: 2; x = x_hi * 2 + x_lo), y: 4, z: 4, core: 2. Of those that a mesh axis runs over, the one named last changes fastest.
Arguments:
- cell_counts: int32 [16, 16, 16], P('gx', 'gy', 'gz'), may hold values from 64 to 128
- grid_offset: int32 [16, 16, 16, 3, 128], P('gx', 'gy', 'gz'), may hold values from 0 to 14
- fraction: float32 [16, 16, 16, 3, 128], P('gx', 'gy', 'gz'), may hold values from 0 to 1
- species: int32 [16, 16, 16, 128], P('gx', 'gy', 'gz'), may hold values from 0 to 1
- species_density: float32 [2], replicated, may hold values from 0.01 to 0.03
- species_pair: float32 [2], replicated, may hold values from 0.05 to 0.2
- species_embed: float32 [2], replicated, may hold values from 0.5 to 2
- species_charge: float32 [2], replicated, may hold values from -3 to 3
Outputs:
- forces: float32 [16, 16, 16, 3, 128], P('gx', 'gy', 'gz')
- density: float32 [16, 16, 16, 128], P('gx', 'gy', 'gz')
The draws below stay inside these ranges and needn't reach their ends.
Inputs may be any that keep to these rules, and one draw needn't show every extreme that they name: `cell_counts`: slots below the count hold atoms; the others are padding. `grid_offset`: an atom's stencil points lie in its own cell.
All inputs are finite; a program needn't handle non-finite values.
Results may differ from the reference program's by a relative error of at most 0.0003.
Values sent between devices are 32-bit elements; how exact they have to be, the bound alone decides.
A program may use at most 128 MiB of HBM per device.

```python
import math
import jax
import jax.numpy as jnp
from jax import lax

SLOTS = 128
NSPEC = 2
PPC = 16
NX = 16
NY = 16
NZ = 16


def plant(values, key, smallest, top_value):
    longest = values.shape.index(max(values.shape))
    spots = []
    for shift in (0, 1):
        where = [jax.random.randint(jax.random.fold_in(key, axis), (), 0, length) for axis, length in enumerate(values.shape)]
        where[longest] = (where[longest] + shift) % values.shape[longest]
        spots.append(tuple(where))
    return values.at[spots[0]].set(smallest).at[spots[1]].set(top_value)


def block_levels(stream_key, dims, shards, low, largest):
    def one(axis_at, blocks):
        heights = jax.random.uniform(jax.random.fold_in(jax.random.fold_in(stream_key, 6), axis_at), (blocks,), jnp.float32, low / len(shards), largest / len(shards))
        return jnp.repeat(jnp.exp(heights), dims[axis_at] // blocks).reshape((-1,) + (1,) * (len(dims) - axis_at - 1))

    factor_of = one(*shards[0])
    for cut in shards[1:]:
        factor_of = factor_of * one(*cut)
    return factor_of


def noise(stream_key, shape, scale, limit, kind=jnp.bfloat16):
    return jnp.clip(scale * jax.random.normal(stream_key, shape, jnp.float32), -limit, limit).astype(kind)


def setup_inputs(seed: int = 0) -> dict:
    arg_keys = jax.random.split(jax.random.key(seed), 9)
    return {
        "cell_counts": plant(jax.random.randint(arg_keys[0], (NX, NY, NZ), SLOTS // 2, SLOTS + 1), jax.random.fold_in(arg_keys[0], 1), SLOTS // 2, SLOTS).astype(jnp.int32),
        "grid_offset": plant(jax.random.randint(arg_keys[1], (NX, NY, NZ, 3, SLOTS), 0, PPC - 1), jax.random.fold_in(arg_keys[1], 1), 0, (PPC - 1) - 1).astype(jnp.int32),
        "fraction": jnp.clip(1.0 * jax.random.uniform(arg_keys[2], (NX, NY, NZ, 3, SLOTS), jnp.float32) ** block_levels(arg_keys[2], (NX, NY, NZ, 3, SLOTS), ((0, 4), (1, 8), (2, 4)), -0.2, 0.2), 0.0, 1.0),
        "species": plant(jax.random.randint(arg_keys[3], (NX, NY, NZ, SLOTS), 0, NSPEC), jax.random.fold_in(arg_keys[3], 1), 0, NSPEC - 1).astype(jnp.int32),
        "species_density": jnp.clip(jnp.exp(jax.random.uniform(arg_keys[4], (NSPEC,), jnp.float32, math.log(0.01), math.log(0.03))), 0.01, 0.03),
        "species_pair": jnp.clip(jnp.exp(jax.random.uniform(arg_keys[5], (NSPEC,), jnp.float32, math.log(0.05), math.log(0.2))), 0.05, 0.2),
        "species_embed": jnp.clip(jnp.exp(jax.random.uniform(arg_keys[6], (NSPEC,), jnp.float32, math.log(0.5), math.log(2.0))), 0.5, 2.0),
        "species_charge": noise(arg_keys[7], (NSPEC,), 1.0, 3.0, jnp.float32),
    }


EWALD_SPLIT = 0.7
COUPLING = 8.0
HIGHEST_PRECISION = lax.Precision.HIGHEST
neighbour_shifts = [(shift_x, shift_y, shift_z) for shift_x in (-1, 0, 1) for shift_y in (-1, 0, 1) for shift_z in (-1, 0, 1)]

def species_value(species, lookup_table):
    result = jnp.zeros(species.shape, jnp.float32)
    for kind_index in range(NSPEC):
        result = result + jnp.where(species == kind_index, lookup_table[kind_index], 0.0)
    return result

def stencil(offsets, fractions):
    points = lax.broadcasted_iota(jnp.int32, offsets.shape + (PPC,), offsets.ndim)
    lower_point = (points == offsets[..., None]).astype(jnp.float32)
    upper_point = (points == offsets[..., None] + 1).astype(jnp.float32)
    weights = lower_point * (1.0 - fractions[..., None]) + upper_point * fractions[..., None]
    return (weights, upper_point - lower_point)

def spread_cells(charges, weights_x, weights_y, weights_z):
    batch_size, slot_count = charges.shape
    pair_plane = (weights_y[:, :, :, None] * weights_z[:, :, None, :]).reshape(batch_size, slot_count, PPC * PPC)
    return jnp.einsum('bax,bay->bxy', weights_x * charges[:, :, None], pair_plane, precision=HIGHEST_PRECISION)

def outer_plane(first_weights, second_weights):
    batch_size, slot_count, width_count = first_weights.shape
    return (first_weights[:, :, :, None] * second_weights[:, :, None, :]).reshape(batch_size, slot_count, width_count * width_count)

def sample_cells(blocks, charges, weights_x, weights_y, weights_z, slope_x, slope_y, slope_z):
    plain_x = jnp.einsum('bax,bxy->bay', weights_x, blocks, precision=HIGHEST_PRECISION)
    tilted_x = jnp.einsum('bax,bxy->bay', slope_x, blocks, precision=HIGHEST_PRECISION)
    force_x = -charges * lax.optimization_barrier(jnp.sum(tilted_x * outer_plane(weights_y, weights_z), axis=2))
    force_y = -charges * lax.optimization_barrier(jnp.sum(plain_x * outer_plane(slope_y, weights_z), axis=2))
    force_z = -charges * lax.optimization_barrier(jnp.sum(plain_x * outer_plane(weights_y, slope_z), axis=2))
    return jnp.stack([force_x, force_y, force_z], axis=1)

def signed_modes(indices, total):
    return jnp.where(2 * indices >= total, indices - total, indices)

def green_factor(modes_x, modes_y, modes_z, length_x, length_y, length_z):
    wave_x = modes_x.astype(jnp.float32) * (2.0 * math.pi / length_x)
    wave_y = modes_y.astype(jnp.float32) * (2.0 * math.pi / length_y)
    wave_z = modes_z.astype(jnp.float32) * (2.0 * math.pi / length_z)
    squared = wave_x * wave_x + wave_y * wave_y + wave_z * wave_z
    anchor = (modes_x == 0) & (modes_y == 0) & (modes_z == 0)
    safe_square = jnp.where(anchor, 1.0, squared)
    return jnp.where(anchor, 0.0, 4.0 * math.pi * jnp.exp(-squared / (4.0 * EWALD_SPLIT * EWALD_SPLIT)) / safe_square)

def periodic(values):
    widths = [(1, 1), (1, 1), (1, 1)] + [(0, 0)] * (values.ndim - 3)
    return jnp.pad(values, widths, mode='wrap')

def pair_terms(positions, other_positions, shift_triple, not_self):
    shift_vector = jnp.asarray(shift_triple, jnp.float32)
    separation = shift_vector[:, None, None] + other_positions[..., :, None, :] - positions[..., :, :, None]
    squared = lax.optimization_barrier(jnp.sum(separation * separation, axis=-3))
    weight = jnp.maximum(1.0 - squared, 0.0)
    if shift_triple == (0, 0, 0):
        weight = weight * not_self
    return (separation, weight)

def window(rows, shift_triple, cells_y, cells_z):
    return rows[1 + shift_triple[0], 1 + shift_triple[1]:1 + shift_triple[1] + cells_y, 1 + shift_triple[2]:1 + shift_triple[2] + cells_z]

def reference(cell_counts, grid_offset, fraction, species, species_density, species_pair, species_embed, species_charge):
    slot_index = lax.broadcasted_iota(jnp.int32, species.shape, 3)
    alive_mask = (slot_index < cell_counts[..., None]).astype(jnp.float32)
    positions = (grid_offset.astype(jnp.float32) + 0.5 + fraction) / PPC
    density_coef = species_value(species, species_density) * alive_mask
    repulsion = species_value(species, species_pair) * alive_mask
    embedding = species_value(species, species_embed)
    charges = species_value(species, species_charge) * alive_mask
    not_self = (lax.broadcasted_iota(jnp.int32, (SLOTS, SLOTS), 0) != lax.broadcasted_iota(jnp.int32, (SLOTS, SLOTS), 1)).astype(jnp.float32)
    wide_positions = periodic(positions)
    wide_density = periodic(density_coef)
    wide_repulsion = periodic(repulsion)
    row_ids = jnp.arange(NX, dtype=jnp.int32)

    def density_row(row):
        near_pos = lax.dynamic_slice_in_dim(wide_positions, row, 3, 0)
        near_coef = lax.dynamic_slice_in_dim(wide_density, row, 3, 0)
        own = lax.dynamic_index_in_dim(positions, row, 0, keepdims=False)
        total = jnp.zeros((NY, NZ, SLOTS), jnp.float32)
        for shift_triple in neighbour_shifts:
            separation, weight = pair_terms(own, window(near_pos, shift_triple, NY, NZ), shift_triple, not_self)
            total = total + lax.optimization_barrier(jnp.sum(weight * weight * weight * window(near_coef, shift_triple, NY, NZ)[..., None, :], axis=-1))
        return total
    density = lax.map(density_row, row_ids) * alive_mask
    slope_embed = -embedding * alive_mask / (2.0 * jnp.sqrt(1.0 + density))
    wide_slope = periodic(slope_embed)

    def force_row(row):
        near_pos = lax.dynamic_slice_in_dim(wide_positions, row, 3, 0)
        near_coef = lax.dynamic_slice_in_dim(wide_density, row, 3, 0)
        near_rep = lax.dynamic_slice_in_dim(wide_repulsion, row, 3, 0)
        near_slp = lax.dynamic_slice_in_dim(wide_slope, row, 3, 0)
        own = lax.dynamic_index_in_dim(positions, row, 0, keepdims=False)
        own_rep = lax.dynamic_index_in_dim(repulsion, row, 0, keepdims=False)
        own_coef = lax.dynamic_index_in_dim(density_coef, row, 0, keepdims=False)
        own_slope = lax.dynamic_index_in_dim(slope_embed, row, 0, keepdims=False)
        total = jnp.zeros((NY, NZ, 3, SLOTS), jnp.float32)
        for shift_triple in neighbour_shifts:
            separation, weight = pair_terms(own, window(near_pos, shift_triple, NY, NZ), shift_triple, not_self)
            other_coef = window(near_coef, shift_triple, NY, NZ)[..., None, :]
            other_rep = window(near_rep, shift_triple, NY, NZ)[..., None, :]
            other_slope = window(near_slp, shift_triple, NY, NZ)[..., None, :]
            coefficient = -2.0 * own_rep[..., :, None] * other_rep * weight - 3.0 * weight * weight * (own_slope[..., :, None] * other_coef + other_slope * own_coef[..., :, None])
            total = total + 2.0 * lax.optimization_barrier(jnp.sum(coefficient[..., None, :, :] * separation, axis=-1))
        return total
    eam_force = lax.map(force_row, row_ids)
    stencils = [stencil(grid_offset[:, :, :, axis_index, :], fraction[:, :, :, axis_index, :]) for axis_index in range(3)]
    row_cells = NY * NZ

    def spread_row(row_items):
        charge_row, first_row, second_row, third_row = row_items
        return spread_cells(charge_row.reshape(row_cells, SLOTS), first_row.reshape(row_cells, SLOTS, PPC), second_row.reshape(row_cells, SLOTS, PPC), third_row.reshape(row_cells, SLOTS, PPC))
    blocks = lax.map(spread_row, (charges, stencils[0][0], stencils[1][0], stencils[2][0]))
    length_x, length_y, length_z = (NX * PPC, NY * PPC, NZ * PPC)
    charge_grid = blocks.reshape(NX, NY, NZ, PPC, PPC, PPC).transpose(0, 3, 1, 4, 2, 5).reshape(length_x, length_y, length_z)
    modes_x = signed_modes(jnp.arange(length_x, dtype=jnp.int32), length_x)[:, None, None]
    modes_y = signed_modes(jnp.arange(length_y, dtype=jnp.int32), length_y)[None, :, None]
    modes_z = signed_modes(jnp.arange(length_z, dtype=jnp.int32), length_z)[None, None, :]
    factor = green_factor(modes_x, modes_y, modes_z, length_x, length_y, length_z)
    potential = jnp.real(jnp.fft.ifftn(jnp.fft.fftn(charge_grid) * factor)).astype(jnp.float32)
    blocks_back = potential.reshape(NX, PPC, NY, PPC, NZ, PPC).transpose(0, 2, 4, 1, 3, 5).reshape(NX, row_cells, PPC, PPC * PPC)

    def sample_row(row_items):
        block_row, charge_row, first_w, second_w, third_w, first_s, second_s, third_s = row_items

        def shaped(values):
            return values.reshape(row_cells, SLOTS, PPC)
        return sample_cells(block_row, charge_row.reshape(row_cells, SLOTS), shaped(first_w), shaped(second_w), shaped(third_w), shaped(first_s), shaped(second_s), shaped(third_s))
    electric = lax.map(sample_row, (blocks_back, charges, stencils[0][0], stencils[1][0], stencils[2][0], stencils[0][1], stencils[1][1], stencils[2][1]))
    electric = electric.reshape(NX, NY, NZ, 3, SLOTS)
    forces = (eam_force + COUPLING * electric) * alive_mask[:, :, :, None, :]
    return (forces, density)
```

```python
import itertools
import math

import jax
import jax.numpy as jnp
import numpy as np
from jax import lax
from jax.experimental import pallas as pl
from jax.experimental.pallas import tpu as pltpu
from jax.sharding import PartitionSpec as P

NSPEC = 2
PPC = 16
COUPLING = 8.0
F32, BF16 = jnp.float32, jnp.bfloat16
VMEM_SPEC = pl.BlockSpec(memory_space=pltpu.VMEM)
SMEM_SPEC = pl.BlockSpec(memory_space=pltpu.SMEM)


MESH = pl.DeviceIdType.MESH
AXES = ("gx", "gy", "gz")
SIZES = (4, 8, 4)
SIDES = [side for side in itertools.product((-1, 0, 1), repeat=3) if side != (0, 0, 0)]


def here():
    return [lax.axis_index(axis) for axis in AXES]


def toward(place, side):
    return tuple(lax.rem(p + s + n, n) for p, s, n in zip(place, side, SIZES))


def greet(devices):
    barrier = pltpu.get_barrier_semaphore()
    for device in devices:
        pl.semaphore_signal(barrier, inc=1, device_id=device, device_id_type=MESH)
    pl.semaphore_wait(barrier, len(devices))


def send(src, dst, send_sem, recv_sem, device):
    copy = pltpu.make_async_remote_copy(
        src_ref=src, dst_ref=dst, send_sem=send_sem, recv_sem=recv_sem, device_id=device, device_id_type=MESH)
    copy.start()
    return copy


def halo_copies(own_ref, ext_ref, place, send_sem, recv_sem):
    copies = []
    for n, side in enumerate(SIDES):
        src, dst = [], []
        for s, cells in zip(side, (4, 2, 4)):
            src.append(pl.ds(0, cells) if s == 0 else pl.ds(cells - 1 if s == 1 else 0, 1))
            dst.append(pl.ds(1, cells) if s == 0 else pl.ds(0 if s == 1 else cells + 1, 1))
        copies.append(send(own_ref.at[tuple(src)], ext_ref.at[tuple(dst)], send_sem.at[n], recv_sem.at[n],
                           toward(place, side)))
    return copies


def column_copies(src_ref, dst_ref, place, send_sem, recv_sem):
    gx, gy, gz = place
    copies = []
    for n in range(3):
        other = lax.rem(gz + n + 1, 4)
        copies.append(send(src_ref.at[other], dst_ref.at[gz], send_sem.at[n], recv_sem.at[n], (gx, gy, other)))
    return copies


def column_devices(place):
    gx, gy, gz = place
    return [(gx, gy, lax.rem(gz + n + 1, 4)) for n in range(3)]


def halo_kernel(own_ref, atoms_ref, ext_ref, got_ref, send_sem, recv_sem, column_send, column_recv, local_sem):
    place = here()
    greet([toward(place, side) for side in SIDES] + [column_devices(place)[1]])
    copies = column_copies(atoms_ref, got_ref, place, column_send, column_recv)
    copies += halo_copies(own_ref, ext_ref, place, send_sem, recv_sem)
    inner = pltpu.make_async_copy(own_ref, ext_ref.at[pl.ds(1, 4), pl.ds(1, 2), pl.ds(1, 4)], local_sem.at[0])
    inner.start()
    mine = pltpu.make_async_copy(atoms_ref.at[place[2]], got_ref.at[place[2]], local_sem.at[1])
    mine.start()
    inner.wait()
    mine.wait()
    for copy in copies:
        copy.wait()


def slope_kernel(own_ref, ext_ref, send_sem, recv_sem, local_sem):
    place = here()
    greet([toward(place, side) for side in SIDES])
    copies = halo_copies(own_ref, ext_ref, place, send_sem, recv_sem)
    inner = pltpu.make_async_copy(own_ref, ext_ref.at[pl.ds(1, 4), pl.ds(1, 2), pl.ds(1, 4)], local_sem.at[0])
    inner.start()
    inner.wait()
    for copy in copies:
        copy.wait()


def return_kernel(src_ref, dst_ref, send_sem, recv_sem, local_sem):
    place = here()
    greet(column_devices(place))
    copies = column_copies(src_ref, dst_ref, place, send_sem, recv_sem)
    mine = pltpu.make_async_copy(src_ref.at[place[2]], dst_ref.at[place[2]], local_sem.at[0])
    mine.start()
    mine.wait()
    for copy in copies:
        copy.wait()


COMM_SPEC = pl.BlockSpec(memory_space=pltpu.VMEM)
DMA = pltpu.SemaphoreType.DMA


def comm_params(number):
    return pltpu.CompilerParams(collective_id=number, has_side_effects=True, vmem_limit_bytes=16 << 20)


def halo_exchange(own, atoms):
    return pl.pallas_call(
        halo_kernel,
        out_shape=[jax.ShapeDtypeStruct((6, 4, 6, 8, 128), F32), jax.ShapeDtypeStruct((4, 8, 8, 128), F32)],
        in_specs=[COMM_SPEC] * 2,
        out_specs=[COMM_SPEC] * 2,
        scratch_shapes=[DMA((26,)), DMA((26,)), DMA((3,)), DMA((3,)), DMA((2,))],
        compiler_params=comm_params(0),
        name="halo_exchange",
    )(own, atoms)


def slope_exchange(own):
    return pl.pallas_call(
        slope_kernel,
        out_shape=jax.ShapeDtypeStruct((6, 4, 6, 1, 128), F32),
        in_specs=[COMM_SPEC],
        out_specs=COMM_SPEC,
        scratch_shapes=[DMA((26,)), DMA((26,)), DMA((1,))],
        compiler_params=comm_params(1),
        name="slope_exchange",
    )(own)


def return_exchange(electric):
    return pl.pallas_call(
        return_kernel,
        out_shape=jax.ShapeDtypeStruct((4, 8, 8, 128), F32),
        in_specs=[COMM_SPEC],
        out_specs=COMM_SPEC,
        scratch_shapes=[DMA((3,)), DMA((3,)), DMA((1,))],
        compiler_params=comm_params(2),
        name="return_exchange",
    )(electric)


ROWS = 32
KF = 32


def pieces(value):
    first = value.astype(BF16).astype(F32)
    rest = value - first
    second = rest.astype(BF16).astype(F32)
    third = (rest - second).astype(BF16).astype(F32)
    return first, second, third


def cell_rows(ref, f, cells):
    return ref[pl.ds(f, cells, stride=8), :]


def source_features(ext_ref, coord, feat_f, feat_b, scale_row):
    cell = lax.broadcasted_iota(jnp.int32, (144, 128), 0)
    x = cell_rows(ext_ref, 0, 144) + (lax.div(cell, 24) - 3).astype(F32)
    y = cell_rows(ext_ref, 1, 144) + (lax.rem(lax.div(cell, 6), 4) - 2).astype(F32)
    z = cell_rows(ext_ref, 2, 144) + (lax.rem(cell, 6) - 3).astype(F32)
    if coord is not None:
        coord[0], coord[1], coord[2] = x, y, z
    scale = cell_rows(ext_ref, scale_row, 144)
    square = x * x + y * y + z * z
    k = 0
    for value in (scale, 2.0 * scale * x, 2.0 * scale * y, 2.0 * scale * z):
        first, second, third = pieces(value)
        for piece in (first, second, first, second, third, first):
            feat_f[pl.ds(k, 144, stride=KF), :] = piece
            k += 1
    for piece in pieces(-scale * square):
        feat_f[pl.ds(k, 144, stride=KF), :] = piece
        k += 1
    for k in range(k, KF):
        feat_f[pl.ds(k, 144, stride=KF), :] = jnp.zeros((144, 128), F32)
    feat_b[...] = feat_f[...].astype(BF16)


def target_features(own_ref, own_f, own_t, extra):
    cell = lax.broadcasted_iota(jnp.int32, (32, 128), 0)
    x = cell_rows(own_ref, 0, 32) + (lax.div(cell, 8) - 2).astype(F32)
    y = cell_rows(own_ref, 1, 32) + (lax.rem(lax.div(cell, 4), 2) - 1).astype(F32)
    z = cell_rows(own_ref, 2, 32) + (lax.rem(cell, 4) - 2).astype(F32)
    k = 0
    for value in (1.0 - (x * x + y * y + z * z), x, y, z):
        first, second, third = pieces(value)
        for piece in (first, first, second, second, first, third):
            own_f[pl.ds(k, 32, stride=KF), :] = piece
            k += 1
    for k in range(k, k + 3):
        own_f[pl.ds(k, 32, stride=KF), :] = jnp.ones((32, 128), F32)
    k = 27
    for value in extra:
        first, second, third = pieces(value)
        for piece in (first, second):
            own_f[pl.ds(k, 32, stride=KF), :] = piece
            k += 1
    for k in range(k, KF):
        own_f[pl.ds(k, 32, stride=KF), :] = jnp.zeros((32, 128), F32)

    def turn(t, _):
        own_t[t] = own_f[pl.ds(pl.multiple_of(t * KF, KF), KF), :].T.astype(BF16)
        return 0

    lax.fori_loop(0, 32, turn, 0)
    return x, y, z


def right_side(feat_b, cell):
    r = pl.multiple_of(cell * KF, KF)
    return jnp.concatenate([feat_b[pl.ds(r + KF * dz, KF), :] for dz in range(3)], axis=1)


def density_kernel(own_ref, ext_ref, density_ref, slope_ref, feat_f, feat_b, own_f, own_t, mat):
    source_features(ext_ref, None, feat_f, feat_b, 3)
    target_features(own_ref, own_f, own_t, ())
    mat[...] = jnp.zeros((128, 128), F32)
    lanes = lax.broadcasted_iota(jnp.int32, (128, 128), 1)
    other = lanes != lax.broadcasted_iota(jnp.int32, (128, 128), 0)

    def target(t, _):
        cx, cy, cz = lax.div(t, 8), lax.rem(lax.div(t, 4), 2), lax.rem(t, 4)
        left = own_t[t]
        total = jnp.zeros((128, 128), F32)
        for dx in range(3):
            for dy in range(3):
                right = right_side(feat_b, ((cx + dx) * 4 + cy + dy) * 6 + cz)
                weight = jnp.dot(left, right, preferred_element_type=F32)
                weight = jnp.maximum(weight, 0.0)
                for dz in range(3):
                    part = weight[:, dz * 128:(dz + 1) * 128]
                    if dx == 1 and dy == 1 and dz == 1:
                        part = jnp.where(other, part, 0.0)
                    total = total + part * part * part
        sums = jnp.sum(total, axis=1, keepdims=True)
        mat[...] = jnp.where(lanes == t, sums, mat[...])
        return 0

    lax.fori_loop(0, 32, target, 0)
    density = mat[...].T[0:32] * cell_rows(own_ref, 7, 32)
    density_ref[...] = density
    slope_ref[...] = (cell_rows(own_ref, 6, 32) / jnp.sqrt(1.0 + density)).reshape(32, 1, 128)


def force_kernel(count_ref, own_ref, ext_ref, gain_ref, slope_ref, out_ref, feat_f, feat_b, own_f, own_t, coord, wide,
                 near, prod, mat, items):
    source_features(ext_ref, coord, feat_f, feat_b, 4)
    x, y, z = target_features(own_ref, own_f, own_t, (gain_ref[0], gain_ref[2]))
    select = sel_matrix()

    def spread(r, _):
        for q in range(3):
            wide[r, q] = jnp.broadcast_to(coord[q, pl.ds(r, 1), :], (8, 128))
        wide[r, 3] = jnp.broadcast_to(ext_ref[pl.ds(r * 8 + 5, 1), :], (8, 128))
        wide[r, 4] = jnp.broadcast_to(slope_ref[r], (8, 128))
        return 0

    lax.fori_loop(0, 144, spread, 0)
    mat[...] = jnp.zeros((128, 128), F32)

    def list_target(t, n):
        def list_rows(c, n):
            items[n] = t * 4 + c
            return n + 1

        return lax.fori_loop(0, lax.div(count_ref[t] + ROWS - 1, ROWS), list_rows, n)

    count = lax.fori_loop(0, 32, list_target, 0)
    items[count] = 0
    lane = lax.broadcasted_iota(jnp.int32, (ROWS, 128), 1)
    lane3 = lax.broadcasted_iota(jnp.int32, (ROWS // 8, 8, 128), 2)
    row3 = lax.broadcasted_iota(jnp.int32, (ROWS // 8, 8, 128), 0) * 8 + lax.broadcasted_iota(
        jnp.int32, (ROWS // 8, 8, 128), 1)

    def place(n):
        item = items[n]
        t, c = lax.div(item, 4), lax.rem(item, 4)
        return t, c, lax.div(t, 8), lax.rem(lax.div(t, 4), 2), lax.rem(t, 4)

    def multiply(n, slot):
        t, c, cx, cy, cz = place(n)
        left = own_t[t, pl.ds(pl.multiple_of(c * ROWS, ROWS), ROWS), :]
        near[slot, :, 3456:3712] = jnp.dot(left, select, preferred_element_type=F32)
        for q in range(9):
            right = right_side(feat_b, ((cx + q // 3) * 4 + cy + q % 3) * 6 + cz)
            near[slot, :, q * 384:(q + 1) * 384] = jnp.dot(left, right, preferred_element_type=F32)

    def reduce(n, slot):
        t, c, cx, cy, cz = place(n)
        rows = pl.ds(pl.multiple_of(c * ROWS, ROWS), ROWS)
        value = mat[rows, :]
        for m in range(4):
            value = jnp.where(lane == t * 4 + m, jnp.sum(prod[slot, m], axis=1, keepdims=True), value)
        mat[rows, :] = value

    multiply(0, 0)

    def step(n, _):
        slot = lax.rem(n, 2)
        multiply(n + 1, 1 - slot)
        t, c, cx, cy, cz = place(n)

        def block(offset):
            return near[slot, :, offset:offset + 128].reshape(ROWS // 8, 8, 128)

        gain, tilt = block(3456), block(3584)
        zero = jnp.zeros((ROWS // 8, 8, 128), F32)
        m0, mx, my, mz = zero, zero, zero, zero
        for q in range(9):
            for dz in range(3):
                r = ((cx + q // 3) * 4 + cy + q % 3) * 6 + cz + dz
                w = jnp.maximum(block(q * 384 + dz * 128), 0.0)
                if q == 4 and dz == 1:
                    w = jnp.where(lane3 != row3 + c * ROWS, w, 0.0)
                value = ((tilt * wide[r, 3] + wide[r, 4]) * w + gain) * w
                m0 = m0 + value
                mx = mx + value * wide[r, 0]
                my = my + value * wide[r, 1]
                mz = mz + value * wide[r, 2]
        for m, value in enumerate((m0, mx, my, mz)):
            prod[slot, m] = value.reshape(ROWS, 128)

        @pl.when(n > 0)
        def _():
            reduce(n - 1, 1 - slot)

        return 0

    lax.fori_loop(0, count, step, 0)
    reduce(count - 1, lax.rem(count - 1, 2))
    mat[...] = mat[...].T

    whole = mat[pl.ds(0, 32, stride=4), :]
    for m, place_own in enumerate((x, y, z)):
        out_ref[m] = gain_ref[1] * (mat[pl.ds(m + 1, 32, stride=4), :] - place_own * whole)


def sel_matrix():
    row = lax.broadcasted_iota(jnp.int32, (KF, 256), 0)
    lane = lax.broadcasted_iota(jnp.int32, (KF, 256), 1)
    first = (row >= 27) & (row < 29) & (lane < 128)
    second = (row >= 29) & (row < 31) & (lane >= 128)
    return jnp.where(first | second, 1.0, 0.0).astype(BF16)


def features_scratch():
    return [
        pltpu.VMEM((144 * KF, 128), F32),
        pltpu.VMEM((144 * KF, 128), BF16),
        pltpu.VMEM((32 * KF, 128), F32),
        pltpu.VMEM((32, 128, KF), BF16),
    ]


def density_pass(own, ext):
    return pl.pallas_call(
        density_kernel,
        out_shape=[jax.ShapeDtypeStruct((32, 128), F32), jax.ShapeDtypeStruct((32, 1, 128), F32)],
        in_specs=[VMEM_SPEC] * 2,
        out_specs=[VMEM_SPEC] * 2,
        scratch_shapes=features_scratch() + [pltpu.VMEM((128, 128), F32)],
        compiler_params=pltpu.CompilerParams(vmem_limit_bytes=32 << 20),
        cost_estimate=pl.CostEstimate(flops=10_000_000_000, bytes_accessed=1_000_000, transcendentals=0),
        name="density_pass",
    )(own, ext)


def force_pass(counts, own, ext, gain, slope):
    return pl.pallas_call(
        force_kernel,
        out_shape=jax.ShapeDtypeStruct((3, 32, 128), F32),
        in_specs=[SMEM_SPEC] + [VMEM_SPEC] * 4,
        out_specs=VMEM_SPEC,
        scratch_shapes=features_scratch() + [
            pltpu.VMEM((3, 144, 128), F32),
            pltpu.VMEM((144, 5, 8, 128), F32),
            pltpu.VMEM((2, ROWS, 3712), F32),
            pltpu.VMEM((2, 4, ROWS, 128), F32),
            pltpu.VMEM((128, 128), F32),
            pltpu.SMEM((136,), jnp.int32),
        ],
        compiler_params=pltpu.CompilerParams(vmem_limit_bytes=48 << 20),
        cost_estimate=pl.CostEstimate(flops=20_000_000_000, bytes_accessed=1_000_000, transcendentals=0),
        name="force_pass",
    )(counts, own, ext, gain, slope)


EWALD_SPLIT = 0.7


def tables():
    mode = np.arange(256)[:, None]
    point = np.arange(256)[None, :]
    cosine = np.cos(2 * np.pi * (mode * point % 256) / 256) * np.sqrt(2 / 256)
    cosine[0] /= np.sqrt(2)
    cosine[128] /= np.sqrt(2)
    sine = np.sin(2 * np.pi * ((mode - 128) * point % 256) / 256) * np.sqrt(2 / 256)
    table = np.where(mode <= 128, cosine, sine)
    row = np.arange(512)
    xr, cell, s = row // 128, row // 8 % 16, row % 8
    mixed = table[:, cell * 16 + s % 4 * 4 + xr]
    return table, mixed


def halves(array):
    high = array.astype(np.float32).astype(jnp.bfloat16)
    low = (array - high.astype(np.float64)).astype(np.float32).astype(jnp.bfloat16)
    return np.stack([high, low])


def split(value):
    high = value.astype(BF16)
    return high, (value - high.astype(F32)).astype(BF16)


def dot(a, b):
    return jnp.dot(a, b, preferred_element_type=F32)


def dot3(a, b):
    return dot(a[0], b[0]) + (dot(a[1], b[0]) + dot(a[0], b[1]))


def hat(count, lower, weight):
    point = lax.broadcasted_iota(jnp.int32, (count, lower.shape[1]), 0).astype(F32)
    return jnp.where(point == lower, 1.0 - weight, 0.0) + jnp.where(point == lower + 1.0, weight, 0.0)


def spread_kernel(atoms_ref, table_ref, out_ref, rho):
    def layer(cz, _):
        base = lax.div(cz, 4) * 8 + lax.rem(cz, 4)

        def row(f, shift=0.0):
            first = atoms_ref[pl.ds(base * 8 + f, 1), :]
            second = atoms_ref[pl.ds((base + 4) * 8 + f, 1), :] + shift
            return jnp.concatenate([first, second], axis=1)

        ox, oy, oz, fx, fy, fz, charge = row(0), row(1, 16.0), row(2), row(3), row(4), row(5), row(6)
        wy = hat(32, oy, fy)
        wz = split(hat(16, oz, fz) * charge)
        parts = []
        for x in range(16):
            wx = jnp.where(ox == x, 1.0 - fx, 0.0) + jnp.where(ox == x - 1, fx, 0.0)
            parts.append(wx * wy)
        plane = split(jnp.concatenate(parts, axis=0))
        dims = (((1,), (1,)), ((), ()))

        def against(a, b):
            return lax.dot_general(a, b, dims, preferred_element_type=F32)

        value = against(wz[0], plane[0]) + (against(wz[1], plane[0]) + against(wz[0], plane[1]))
        rho[pl.ds(pl.multiple_of(cz * 16, 16), 16), :] = value
        return 0

    lax.fori_loop(0, 16, layer, 0)
    lines = dot3((table_ref[0], table_ref[1]), split(rho[...]))
    for plane in range(2):
        for xq in range(4):
            out_ref[pl.ds(plane * 4 + xq, 128, stride=8), :] = lines[
                plane * 128:(plane + 1) * 128, xq * 128:(xq + 1) * 128]


def plane_kernel(device_ref, in_ref, table_ref, turned_ref, mixed_ref, mixed_turned_ref, out_ref):
    lane = lax.broadcasted_iota(jnp.int32, (16, 8, 128), 2)

    def pick(ref, half, g):
        return jnp.concatenate([ref[gx, half * 4 + g] for gx in range(4)], axis=0)

    rows = []
    for xr in range(4):
        pair = []
        for half in range(2):
            value = jnp.zeros((16, 8, 128), F32)
            for g in range(4):
                block = pick(in_ref, half, g)
                if g != xr:
                    block = pltpu.roll(block.reshape(128, 128), (g - xr) * 32 % 128, 1).reshape(16, 8, 128)
                value = jnp.where(lax.div(lane, 32) == g, block, value)
            pair.append(value.reshape(128, 128))
        rows.append(jnp.concatenate(pair, axis=1))
    plane = jnp.concatenate(rows, axis=0)
    turned = (turned_ref[0], turned_ref[1])
    along_y = split(dot3(split(plane), turned))

    me = device_ref[0]
    row = lax.broadcasted_iota(jnp.int32, (256, 256), 0)
    col = lax.broadcasted_iota(jnp.int32, (256, 256), 1)
    scale = 2.0 * math.pi / 256
    wave_x = jnp.where(row <= 128, row, row - 128).astype(F32) * scale
    wave_y = jnp.where(col <= 128, col, col - 128).astype(F32) * scale
    flat = wave_x * wave_x + wave_y * wave_y
    side = lax.div(lax.rem(lax.broadcasted_iota(jnp.int32, (256, 512), 1), 8), 4)
    side_turned = lax.div(lax.rem(lax.broadcasted_iota(jnp.int32, (512, 256), 0), 8), 4)
    total = None
    for p in range(2):
        mode = me if p == 0 else jnp.where(me == 0, 128, me)
        wave_z = jnp.full((256, 256), mode, jnp.int32).astype(F32) * scale
        squared = flat + wave_z * wave_z
        anchor = squared == 0.0
        green = jnp.where(anchor, 0.0, 4.0 * math.pi * jnp.exp(-squared / (4.0 * EWALD_SPLIT * EWALD_SPLIT))
                          / jnp.where(anchor, 1.0, squared))
        left = [jnp.where(side == p, mixed_ref[i].astype(F32), 0.0).astype(BF16) for i in range(2)]
        modes = split(dot3(left, along_y) * green)
        back = [jnp.where(side_turned == p, mixed_turned_ref[i].astype(F32), 0.0).astype(BF16) for i in range(2)]
        part = dot3(back, modes)
        total = part if total is None else total + part
    field = dot3(split(total), (table_ref[0], table_ref[1]))
    for half in range(2):
        block = [field[xr * 128:(xr + 1) * 128, half * 128:(half + 1) * 128] for xr in range(4)]
        for g in range(4):
            value = jnp.zeros((16, 8, 128), F32)
            for xr in range(4):
                moved = block[xr]
                if g != xr:
                    moved = pltpu.roll(moved, (xr - g) * 32 % 128, 1)
                value = jnp.where(lax.div(lane, 32) == xr, moved.reshape(16, 8, 128), value)
            for gx in range(4):
                out_ref[gx, half * 4 + g] = value[gx * 4:(gx + 1) * 4]


def sample_kernel(in_ref, atoms_ref, turned_ref, out_ref, field):
    columns = [
        jnp.concatenate([in_ref[pl.ds(plane * 4 + xq, 128, stride=8), :] for xq in range(4)], axis=1)
        for plane in range(2)
    ]
    modes = jnp.concatenate(columns, axis=0)
    lines = jnp.concatenate([modes[:, i * 128:(i + 1) * 128].T for i in range(4)], axis=0)
    high, low = split(dot3(split(lines), (turned_ref[0], turned_ref[1])))
    for group in range(2):
        field[group, :, 0:128] = high[:, group * 128:(group + 1) * 128]
        field[group, :, 128:256] = low[:, group * 128:(group + 1) * 128]
    point = lax.broadcasted_iota(jnp.int32, (128, 128), 0).astype(F32)

    def cell(n, _):
        cyl, cz = lax.rem(n, 2), lax.div(n, 2)
        source = lax.div(cz, 4) * 8 + cyl * 4 + lax.rem(cz, 4)

        def row(f):
            return atoms_ref[pl.ds(source * 8 + f, 1), :]

        ox, oy, oz, fx, fy, fz, charge = [row(f) for f in range(7)]
        lower_z = oz + (lax.rem(cz, 8) * 16).astype(F32)
        lower = jnp.where(point == lower_z, 1.0, 0.0)
        slope = jnp.where(point == lower_z + 1.0, 1.0, 0.0) - lower
        right = jnp.concatenate([lower, slope], axis=1).astype(BF16)
        right = jnp.concatenate([right, right], axis=0)
        left = field_rows(field, lax.div(cz, 8), cyl)
        both = dot(left, right)
        tilt = both[:, 128:256].reshape(16, 16, 128)
        plain = both[:, 0:128].reshape(16, 16, 128) + fz * tilt
        spot = lax.broadcasted_iota(jnp.int32, (16, 128), 0).astype(F32)
        low_y, high_y = spot == oy, spot == oy + 1.0
        wy = jnp.where(low_y, 1.0 - fy, 0.0) + jnp.where(high_y, fy, 0.0)
        sy = jnp.where(high_y, 1.0, 0.0) - jnp.where(low_y, 1.0, 0.0)

        def fold(value):
            return value[:, 0:8] + value[:, 8:16]

        plain_w, plain_s, tilt_w = fold(plain * wy), fold(plain * sy), fold(tilt * wy)
        x_sum = jnp.zeros((8, 128), F32)
        y_sum, z_sum = x_sum, x_sum
        for x in range(16):
            low_x, high_x = ox == x, ox == x - 1
            wx = jnp.where(low_x, 1.0 - fx, 0.0) + jnp.where(high_x, fx, 0.0)
            sx = jnp.where(high_x, 1.0, 0.0) - jnp.where(low_x, 1.0, 0.0)
            x_sum = x_sum + sx * plain_w[x]
            y_sum = y_sum + wx * plain_s[x]
            z_sum = z_sum + wx * tilt_w[x]
        for f, value in enumerate((x_sum, y_sum, z_sum)):
            out_ref[pl.ds(source * 8 + f, 1), :] = -charge * jnp.sum(value, axis=0, keepdims=True)
        return 0

    lax.fori_loop(0, 32, cell, 0)


def field_rows(field, group, cyl):
    start = pl.multiple_of(cyl * 16, 16)
    return jnp.concatenate([field[group, pl.ds(start + 32 * x, 16), :] for x in range(16)], axis=0)


TABLE, MIXED = tables()


def constants():
    return (halves(TABLE), halves(TABLE.T), halves(MIXED), halves(MIXED.T))


def params(mib=32):
    return pltpu.CompilerParams(vmem_limit_bytes=mib << 20)


def spread_pass(atoms, table):
    return pl.pallas_call(
        spread_kernel,
        out_shape=jax.ShapeDtypeStruct((1024, 128), F32),
        in_specs=[VMEM_SPEC] * 2,
        out_specs=VMEM_SPEC,
        scratch_shapes=[pltpu.VMEM((256, 512), F32)],
        compiler_params=params(),
        name="spread_pass",
    )(atoms, table)


def plane_pass(device, planes, table, turned, mixed, mixed_turned):
    return pl.pallas_call(
        plane_kernel,
        out_shape=jax.ShapeDtypeStruct((4, 8, 4, 8, 128), F32),
        in_specs=[SMEM_SPEC] + [VMEM_SPEC] * 5,
        out_specs=VMEM_SPEC,
        compiler_params=params(),
        name="plane_pass",
    )(device, planes, table, turned, mixed, mixed_turned)


def sample_pass(lines, atoms, turned):
    return pl.pallas_call(
        sample_kernel,
        out_shape=jax.ShapeDtypeStruct((256, 128), F32),
        in_specs=[VMEM_SPEC] * 3,
        out_specs=VMEM_SPEC,
        scratch_shapes=[pltpu.VMEM((2, 512, 256), BF16)],
        compiler_params=params(),
        name="sample_pass",
    )(lines, atoms, turned)


def species_value(species, lookup_table):
    result = jnp.zeros(species.shape, F32)
    for kind_index in range(NSPEC):
        result = result + jnp.where(species == kind_index, lookup_table[kind_index], 0.0)
    return result


def on_device(cell_counts, grid_offset, fraction, species, species_density, species_pair, species_embed, species_charge):
    slots = lax.broadcasted_iota(jnp.int32, species.shape, 3)
    alive = (slots < cell_counts[..., None]).astype(F32)
    offset = grid_offset.astype(F32)
    positions = (offset + 0.5 + fraction) / PPC
    pair = species_pair
    root = species_value(species, jnp.cbrt(species_density)) * alive
    repulsion = species_value(species, pair) * alive
    ratio = species_value(species, species_density / (pair * pair))
    tilt = species_value(species, 3.0 * species_embed / (pair * pair)) * alive
    charge = species_value(species, species_charge) * alive
    zero = jnp.zeros_like(alive)
    rows = [positions[:, :, :, d] for d in range(3)] + [root, repulsion, ratio, tilt, alive]
    own = jnp.stack(rows, axis=3)
    rows = [offset[:, :, :, d] for d in range(3)] + [fraction[:, :, :, d] for d in range(3)] + [charge, zero]
    atoms = jnp.stack(rows, axis=3).reshape(4, 8, 8, 128)
    extended, columns = halo_exchange(own, atoms)
    own = own.reshape(256, 128)
    extended = extended.reshape(1152, 128)
    columns = columns.reshape(256, 128)
    table, turned, mixed, mixed_turned = constants()

    lines = spread_pass(columns, table).reshape(128, 8, 128)
    planes = lax.all_to_all(lines, AXES, split_axis=0, concat_axis=0, tiled=True)
    density, slope = density_pass(own, extended)
    device = (lax.axis_index("gx") * 32 + lax.axis_index("gy") * 4 + lax.axis_index("gz")).reshape(1)
    planes = plane_pass(device, planes.reshape(4, 8, 4, 8, 128), table, turned, mixed, mixed_turned)
    lines = lax.all_to_all(planes.reshape(128, 8, 128), AXES, split_axis=0, concat_axis=0, tiled=True)

    wide_slope = slope_exchange(slope.reshape(4, 2, 4, 1, 128)).reshape(144, 1, 128)
    gain = jnp.stack([
        species_value(species, -4.0 * pair / species_density).reshape(32, 128),
        species_value(species, species_density).reshape(32, 128),
        slope.reshape(32, 128) / ratio.reshape(32, 128),
    ])
    eam = force_pass(cell_counts.reshape(32), own, extended, gain, wide_slope)
    electric = sample_pass(lines.reshape(1024, 128), columns, table)
    electric = return_exchange(electric.reshape(4, 8, 8, 128)).reshape(4, 2, 4, 8, 128)[:, :, :, 0:3]
    eam = eam.reshape(3, 4, 2, 4, 128).transpose(1, 2, 3, 0, 4)
    forces = (eam + COUPLING * electric) * alive[:, :, :, None, :]
    return forces, density.reshape(4, 2, 4, 128)


def solution(mesh):
    return jax.shard_map(
        on_device,
        mesh=mesh,
        in_specs=(
            P("gx", "gy", "gz"),
            P("gx", "gy", "gz", None, None),
            P("gx", "gy", "gz", None, None),
            P("gx", "gy", "gz", None),
            P(),
            P(),
            P(),
            P(),
        ),
        out_specs=(P("gx", "gy", "gz", None, None), P("gx", "gy", "gz", None)),
        check_vma=False,
    )
```

```python
import itertools
import math

import jax
import jax.numpy as jnp
import numpy as np
from jax import lax
from jax.experimental import pallas as pl
from jax.experimental.pallas import tpu as pltpu
from jax.sharding import PartitionSpec as P

PPC = 16
COUPLING = 8.0
F32, BF16 = jnp.float32, jnp.bfloat16
VMEM_SPEC = pl.BlockSpec(memory_space=pltpu.VMEM)
SMEM_SPEC = pl.BlockSpec(memory_space=pltpu.SMEM)


MESH = pl.DeviceIdType.MESH
AXES = ("gx", "gy", "gz")
SIZES = (4, 8, 4)
SIDES = [side for side in itertools.product((-1, 0, 1), repeat=3) if side != (0, 0, 0)]


def here():
    return [lax.axis_index(axis) for axis in AXES]


def toward(place, side):
    return tuple(lax.rem(p + s + n, n) for p, s, n in zip(place, side, SIZES))


def signal(devices):
    barrier = pltpu.get_barrier_semaphore()
    for device in devices:
        pl.semaphore_signal(barrier, inc=1, device_id=device, device_id_type=MESH)


def await_signals(count):
    pl.semaphore_wait(pltpu.get_barrier_semaphore(), count)


def send(src, dst, send_sem, recv_sem, device):
    copy = pltpu.make_async_remote_copy(
        src_ref=src, dst_ref=dst, send_sem=send_sem, recv_sem=recv_sem, device_id=device, device_id_type=MESH)
    copy.start()
    return copy


def halo_copies(own_ref, rim, ext_ref, place, send_sem, recv_sem):
    copies = []
    for n, side in enumerate(SIDES):
        src, dst = [], []
        for s, cells in zip(side, (4, 2, 4)):
            src.append(pl.ds(rim, cells) if s == 0 else pl.ds(rim + (cells - 1 if s == 1 else 0), 1))
            dst.append(pl.ds(1, cells) if s == 0 else pl.ds(0 if s == 1 else cells + 1, 1))
        copies.append(send(own_ref.at[tuple(src)], ext_ref.at[tuple(dst)], send_sem.at[n], recv_sem.at[n],
                           toward(place, side)))
    return copies


def column_copy(src_ref, dst_ref, place, send_sem, recv_sem, n):
    gx, gy, gz = place
    other = lax.rem(gz + n + 1, 4)
    return send(src_ref.at[other], dst_ref.at[gz], send_sem.at[n], recv_sem.at[n], (gx, gy, other))


def column_copies(src_ref, dst_ref, place, send_sem, recv_sem):
    return [column_copy(src_ref, dst_ref, place, send_sem, recv_sem, n) for n in range(3)]


def column_devices(place):
    gx, gy, gz = place
    return [(gx, gy, lax.rem(gz + n + 1, 4)) for n in range(3)]


DMA = pltpu.SemaphoreType.DMA


def comm_params(number):
    return pltpu.CompilerParams(collective_id=number, has_side_effects=True, vmem_limit_bytes=32 << 20)


ROWS = 16
KF = 32


def pieces(value):
    first = value.astype(BF16).astype(F32)
    rest = value - first
    second = rest.astype(BF16).astype(F32)
    third = (rest - second).astype(BF16).astype(F32)
    return first, second, third


def by_species(code, values):
    return jnp.where(code == 0.0, values[0], jnp.where(code == 1.0, values[1], 0.0))


def filled(ref, k):
    return jnp.full((8, 128), ref[k], F32)


def cube_root(value):
    guess = jnp.exp(jnp.log(value) * (1.0 / 3.0))
    return guess - (guess * guess * guess - value) / (3.0 * guess * guess)


def sublane():
    return lax.broadcasted_iota(jnp.int32, (8, 128), 0)


def assemble(blocks, ones, twos):
    rows = []
    for value, one, two in zip(blocks, ones, twos):
        first, second, third = pieces(value)
        rows.append(jnp.where(one, first, jnp.where(two, second, third)))
    return jnp.concatenate(rows, axis=0)


def patterns(first, second, last_first, last_second):
    ones, twos = [], []
    for block in range(4):
        one = two = None
        for k in range(block * 8, block * 8 + 8):
            here_one = (k % 6 in first) if k < 24 else k in last_first
            here_two = (k % 6 in second) if k < 24 else k in last_second
            if here_one:
                one = (sublane() == k % 8) if one is None else one | (sublane() == k % 8)
            if here_two:
                two = (sublane() == k % 8) if two is None else two | (sublane() == k % 8)
        ones.append(one)
        twos.append(two)
    return ones, twos


def source_features(ext_ref, slope_ref, wide, feat_b, scales, ratios):
    ones, twos = patterns((0, 2, 5), (1, 3), (24,), (25,))
    low_six, low_four, low_two, low_three = [sublane() < n for n in (6, 4, 2, 3)]

    def cell(r, _):
        def row(f):
            return jnp.broadcast_to(ext_ref[r, f:f + 1, :], (8, 128))

        x = row(0) + (lax.div(r, 24) - 3).astype(F32)
        y = row(1) + (lax.rem(lax.div(r, 6), 4) - 2).astype(F32)
        z = row(2) + (lax.rem(r, 6) - 3).astype(F32)
        code = row(3)
        scale = by_species(code, scales)
        if wide is not None:
            wide[r, 0], wide[r, 1], wide[r, 2] = x, y, z
            wide[r, 3] = jnp.where(code == 1.0, ratios[1], ratios[0])
            wide[r, 4] = jnp.broadcast_to(slope_ref[r], (8, 128))
        square = -scale * (x * x + y * y + z * z)
        double = scale + scale
        x, y, z = double * x, double * y, double * z
        blocks = [jnp.where(low_six, scale, x), jnp.where(low_four, x, y), jnp.where(low_two, y, z),
                  jnp.where(low_three, square, 0.0)]
        feat_b[pl.ds(pl.multiple_of(r * KF, KF), KF), :] = assemble(blocks, ones, twos).astype(BF16)
        return 0

    lax.fori_loop(0, 144, cell, 0, unroll=4)


def corner(t):
    return (lax.div(t, 8) * 4 + lax.rem(lax.div(t, 4), 2)) * 6 + lax.rem(t, 4)


def target_features(ext_ref, own_t, keep, slope_ref, gains, ratios):
    ones, twos = patterns((0, 1, 4), (2, 3), (24, 25, 26, 27, 29), (28, 30))
    low_six, low_four, low_two, low_three = [sublane() < n for n in (6, 4, 2, 3)]
    low_five, low_seven = sublane() < 5, sublane() < 7

    def cell(t, _):
        r = corner(t) + 31

        def row(f):
            return jnp.broadcast_to(ext_ref[r, f:f + 1, :], (8, 128))

        x = row(0) + (lax.div(t, 8) - 2).astype(F32)
        y = row(1) + (lax.rem(lax.div(t, 4), 2) - 1).astype(F32)
        z = row(2) + (lax.rem(t, 4) - 2).astype(F32)
        code = row(3)
        for n, value in enumerate((x, y, z, code)):
            keep[n, pl.ds(t, 1), :] = value[0:1]
        rest = 1.0 - (x * x + y * y + z * z)
        tail = jnp.zeros((8, 128), F32)
        if gains is not None:
            second = code == 1.0
            tilt = jnp.broadcast_to(slope_ref[r], (8, 128)) / jnp.where(second, ratios[1], ratios[0])
            tail = jnp.where(low_five, jnp.where(second, gains[1], gains[0]), jnp.where(low_seven, tilt, 0.0))
        blocks = [jnp.where(low_six, rest, x), jnp.where(low_four, x, y), jnp.where(low_two, y, z),
                  jnp.where(low_three, 1.0, tail)]
        own_t[t] = assemble(blocks, ones, twos).T.astype(BF16)
        return 0

    lax.fori_loop(0, 32, cell, 0, unroll=4)


def right_side(feat_b, cell):
    r = pl.multiple_of(cell * KF, KF)
    return jnp.concatenate([feat_b[pl.ds(r + KF * dz, KF), :] for dz in range(3)], axis=1)


def density_kernel(amplitude_ref, pair_ref, embed_ref, ext_ref, density_ref, slope_ref, feat_b, own_t, keep, mat):
    amplitudes, pairs, embeds = [[filled(ref, k) for k in range(2)] for ref in (amplitude_ref, pair_ref, embed_ref)]
    source_features(ext_ref, None, None, feat_b, [cube_root(value) for value in amplitudes], None)
    target_features(ext_ref, own_t, keep, None, None, None)
    mat[...] = jnp.zeros((128, 128), F32)
    lanes = lax.broadcasted_iota(jnp.int32, (128, 128), 1)
    other = lanes != lax.broadcasted_iota(jnp.int32, (128, 128), 0)

    def target(t):
        cx, cy, cz = lax.div(t, 8), lax.rem(lax.div(t, 4), 2), lax.rem(t, 4)
        left = own_t[t]
        total = jnp.zeros((128, 128), F32)
        for dx in range(3):
            for dy in range(3):
                right = right_side(feat_b, ((cx + dx) * 4 + cy + dy) * 6 + cz)
                weight = jnp.dot(left, right, preferred_element_type=F32)
                weight = jnp.maximum(weight, 0.0)
                for dz in range(3):
                    part = weight[:, dz * 128:(dz + 1) * 128]
                    if dx == 1 and dy == 1 and dz == 1:
                        part = jnp.where(other, part, 0.0)
                    total = total + part * part * part
        sums = jnp.sum(total, axis=1, keepdims=True)
        return sums

    def both(n, _):
        first, second = target(2 * n), target(2 * n + 1)
        mat[...] = jnp.where(lanes == 2 * n, first, jnp.where(lanes == 2 * n + 1, second, mat[...]))
        return 0

    lax.fori_loop(0, 16, both, 0)
    code = keep[3]
    alive = by_species(code, (1.0, 1.0))
    density = mat[...].T[0:32] * alive
    density_ref[...] = density.reshape(8, 4, 128)
    tilts = [jnp.concatenate([3.0 * embed / (pair * pair)] * 4, axis=0) for embed, pair in zip(embeds, pairs)]
    slope_ref[...] = (by_species(code, tilts) / jnp.sqrt(1.0 + density)).reshape(32, 1, 128)


def force_kernel(count_ref, amplitude_ref, pair_ref, ext_ref, slope_ref, out_ref, feat_b, own_t, keep, wide, near_a, near_b,
                 mat, table):
    amplitudes, pairs = [[filled(ref, k) for k in range(2)] for ref in (amplitude_ref, pair_ref)]
    ratios = [amplitude / (pair * pair) for amplitude, pair in zip(amplitudes, pairs)]
    gains = [-4.0 * pair / amplitude for amplitude, pair in zip(amplitudes, pairs)]
    source_features(ext_ref, slope_ref, wide, feat_b, pairs, ratios)
    target_features(ext_ref, own_t, keep, slope_ref, gains, ratios)
    feat_b[144 * KF:146 * KF, :] = jnp.concatenate([sel_matrix()[:, 0:128], sel_matrix()[:, 128:256]], axis=0)

    def fill(n, _):
        table[n] = jnp.where(n < 27, (lax.div(n, 9) * 4 + lax.rem(lax.div(n, 3), 3)) * 6 + lax.rem(n, 3),
                             jnp.where(n == 28, 145, 144))
        table[32 + n] = jnp.where(n < 27, 1, 0)
        return 0

    lax.fori_loop(0, 32, fill, 0)
    mat[...] = jnp.zeros((128, 128), F32)
    lane = lax.broadcasted_iota(jnp.int32, (ROWS, 128), 1)
    lane3 = lax.broadcasted_iota(jnp.int32, (ROWS // 8, 8, 128), 2)
    row3 = lax.broadcasted_iota(jnp.int32, (ROWS // 8, 8, 128), 0) * 8 + lax.broadcasted_iota(
        jnp.int32, (ROWS // 8, 8, 128), 1)

    def around(base, k):
        return base + (k // 9 * 4 + k // 3 % 3) * 6 + k % 3

    def multiply(t, near, part):
        left, base = own_t[t], corner(t)
        for k in range(0, 8, 2):
            right = []
            for n in (part * 8 + k, part * 8 + k + 1):
                start = pl.multiple_of((table[n] + table[32 + n] * base) * KF, KF)
                right.append(feat_b[pl.ds(start, KF), :])
            product = jnp.dot(left, jnp.concatenate(right, axis=1), preferred_element_type=F32)
            near[part * 8 + k] = product[:, 0:128]
            near[part * 8 + k + 1] = product[:, 128:256]

    def chunk(t, near, c):
        rows = pl.ds(pl.multiple_of(c * ROWS, ROWS), ROWS)
        base = corner(t)

        def block(k):
            return near[k, rows, :].reshape(ROWS // 8, 8, 128)

        gain, tilt = block(27), block(28)
        zero = jnp.zeros((ROWS // 8, 8, 128), F32)
        m0, mx, my, mz = zero, zero, zero, zero
        for k in range(27):
            r = around(base, k)
            w = jnp.maximum(block(k), 0.0)
            if k == 13:
                w = jnp.where(lane3 != row3 + c * ROWS, w, 0.0)
            value = ((tilt * wide[r, 3] + wide[r, 4]) * w + gain) * w
            m0 = m0 + value
            mx = mx + value * wide[r, 0]
            my = my + value * wide[r, 1]
            mz = mz + value * wide[r, 2]
        old = mat[rows, :]
        for m, value in enumerate((m0, mx, my, mz)):
            total = jnp.sum(value.reshape(ROWS, 128), axis=1, keepdims=True)
            old = jnp.where(lane == t * 4 + m, total, old)
        mat[rows, :] = old

    for part in range(4):
        multiply(0, near_a, part)

    def target(t, near, following):
        later = jnp.minimum(t + 1, 31)

        def rest(c, _):
            chunk(t, near, c)
            return 0

        for part in range(4):
            multiply(later, following, part)
            chunk(t, near, part)
        lax.fori_loop(4, lax.div(count_ref[t] + ROWS - 1, ROWS), rest, 0)

    def pair(n, _):
        target(2 * n, near_a, near_b)
        target(2 * n + 1, near_b, near_a)
        return 0

    lax.fori_loop(0, 16, pair, 0)
    mat[...] = mat[...].T

    whole = mat[pl.ds(0, 32, stride=4), :]
    amplitude = by_species(keep[3], [jnp.concatenate([value] * 4, axis=0) for value in amplitudes])
    for m in range(3):
        out_ref[m] = amplitude * (mat[pl.ds(m + 1, 32, stride=4), :] - keep[m] * whole)


def sel_matrix():
    row = lax.broadcasted_iota(jnp.int32, (KF, 256), 0)
    lane = lax.broadcasted_iota(jnp.int32, (KF, 256), 1)
    first = (row >= 27) & (row < 29) & (lane < 128)
    second = (row >= 29) & (row < 31) & (lane >= 128)
    return jnp.where(first | second, 1.0, 0.0).astype(BF16)


def features_scratch():
    return [pltpu.VMEM((146 * KF, 128), BF16), pltpu.VMEM((32, 128, KF), BF16), pltpu.VMEM((4, 32, 128), F32)]


def density_pass(amplitude, pair, embed, ext):
    return pl.pallas_call(
        density_kernel,
        out_shape=[jax.ShapeDtypeStruct((8, 4, 128), F32), jax.ShapeDtypeStruct((32, 1, 128), F32)],
        in_specs=[SMEM_SPEC] * 3 + [VMEM_SPEC],
        out_specs=[VMEM_SPEC] * 2,
        scratch_shapes=features_scratch() + [pltpu.VMEM((128, 128), F32)],
        compiler_params=pltpu.CompilerParams(vmem_limit_bytes=16 << 20),
        cost_estimate=pl.CostEstimate(flops=10_000_000_000, bytes_accessed=1_000_000, transcendentals=0),
        name="density_pass",
    )(amplitude, pair, embed, ext)


def force_pass(counts, amplitude, pair, ext, slope):
    return pl.pallas_call(
        force_kernel,
        out_shape=jax.ShapeDtypeStruct((3, 32, 128), F32),
        in_specs=[SMEM_SPEC] * 3 + [VMEM_SPEC] * 2,
        out_specs=VMEM_SPEC,
        scratch_shapes=features_scratch() + [
            pltpu.VMEM((144, 5, 8, 128), F32),
            pltpu.VMEM((32, 128, 128), F32),
            pltpu.VMEM((32, 128, 128), F32),
            pltpu.VMEM((128, 128), F32),
            pltpu.SMEM((64,), jnp.int32),
        ],
        compiler_params=pltpu.CompilerParams(vmem_limit_bytes=24 << 20),
        cost_estimate=pl.CostEstimate(flops=20_000_000_000, bytes_accessed=1_000_000, transcendentals=0),
        name="force_pass",
    )(counts, amplitude, pair, ext, slope)


EWALD_SPLIT = 0.7


def tables():
    mode = np.arange(256)[:, None]
    point = np.arange(256)[None, :]
    cosine = np.cos(2 * np.pi * (mode * point % 256) / 256) * np.sqrt(2 / 256)
    cosine[0] /= np.sqrt(2)
    cosine[128] /= np.sqrt(2)
    sine = np.sin(2 * np.pi * ((mode - 128) * point % 256) / 256) * np.sqrt(2 / 256)
    table = np.where(mode <= 128, cosine, sine)
    row = np.arange(512)
    xr, cell, s = row // 128, row // 8 % 16, row % 8
    mixed = table[:, cell * 16 + s % 4 * 4 + xr]
    return table, mixed


def parts_of(array):
    parts = []
    for _ in range(3):
        parts.append(array.astype(np.float32).astype(jnp.bfloat16))
        array = array - parts[-1].astype(np.float64)
    return np.stack(parts)


def split(value):
    high = value.astype(BF16)
    return high, (value - high.astype(F32)).astype(BF16)


def dot(a, b):
    return jnp.dot(a, b, preferred_element_type=F32)


def dot3(a, b):
    return dot(a[0], b[0]) + (dot(a[1], b[0]) + dot(a[0], b[1]))


def split3(value):
    first = value.astype(BF16)
    rest = value - first.astype(F32)
    second = rest.astype(BF16)
    return first, second, (rest - second.astype(F32)).astype(BF16)


def dot6(a, b):
    small = dot(a[1], b[1]) + (dot(a[2], b[0]) + dot(a[0], b[2]))
    return dot(a[0], b[0]) + (dot(a[1], b[0]) + dot(a[0], b[1]) + small)


def hat(count, lower, weight):
    point = lax.broadcasted_iota(jnp.int32, (count, lower.shape[1]), 0).astype(F32)
    return jnp.where(point == lower, 1.0 - weight, 0.0) + jnp.where(point == lower + 1.0, weight, 0.0)


def spread_and_transform(atoms_ref, charges, table_ref, out_ref, rho):
    def layer(cz, _):
        source, cell = lax.div(cz, 4), lax.rem(cz, 4)

        def row(f, shift=0.0):
            first = atoms_ref[source, cell, f:f + 1, :]
            second = atoms_ref[source, cell + 4, f:f + 1, :] + shift
            return jnp.concatenate([first, second], axis=1)

        ox, oy, oz, fx, fy, fz = row(0), row(1, 16.0), row(2), row(3), row(4), row(5)
        charge = by_species(row(6), charges)
        wy = hat(32, oy, fy)
        wz = split(hat(16, oz, fz) * charge)
        parts = []
        for x in range(16):
            wx = jnp.where(ox == x, 1.0 - fx, 0.0) + jnp.where(ox == x - 1, fx, 0.0)
            parts.append(wx * wy)
        plane = split(jnp.concatenate(parts, axis=0))
        dims = (((1,), (1,)), ((), ()))

        def against(a, b):
            return lax.dot_general(a, b, dims, preferred_element_type=F32)

        value = against(wz[0], plane[0]) + (against(wz[1], plane[0]) + against(wz[0], plane[1]))
        rho[pl.ds(pl.multiple_of(cz * 16, 16), 16), :] = value
        return 0

    lax.fori_loop(0, 16, layer, 0)
    lines = dot3((table_ref[0], table_ref[1]), split(rho[...]))
    for plane in range(2):
        for xq in range(4):
            out_ref[pl.ds(plane * 4 + xq, 128, stride=8), :] = lines[
                plane * 128:(plane + 1) * 128, xq * 128:(xq + 1) * 128]


def gather_kernel(charge_ref, count_ref, offset_ref, fraction_ref, species_ref, table_ref, ext_ref, got_ref, out_ref,
                  atoms, rho, send_sem, recv_sem, column_send, column_recv):
    place = here()
    signal([toward(place, side) for side in SIDES] + [column_devices(place)[1]])
    slot = lax.broadcasted_iota(jnp.int32, (1, 128), 1)

    def pack(t, _):
        x, y, z = lax.div(t, 8), lax.rem(lax.div(t, 4), 2), lax.rem(t, 4)
        offset, fraction = offset_ref[t].astype(F32), fraction_ref[t]
        kind = species_ref[lax.div(t, 4), pl.ds(z, 1), :].astype(F32)
        code = jnp.where(slot < count_ref[t], kind, -1.0)
        ext_ref[x + 1, y + 1, z + 1, 0:3, :] = (offset + 0.5 + fraction) * (1.0 / PPC)
        ext_ref[x + 1, y + 1, z + 1, 3:4, :] = code
        atoms[x, y * 4 + z, 0:3, :] = offset
        atoms[x, y * 4 + z, 3:6, :] = fraction
        atoms[x, y * 4 + z, 6:7, :] = code
        atoms[x, y * 4 + z, 7:8, :] = code
        return 0

    lax.fori_loop(0, 32, pack, 0)

    def keep(n, _):
        got_ref[place[2], n] = atoms[place[2], n]
        return 0

    lax.fori_loop(0, 8, keep, 0)
    await_signals(27)
    columns = column_copies(atoms, got_ref, place, column_send, column_recv)
    halo = halo_copies(ext_ref, 1, ext_ref, place, send_sem, recv_sem)
    for copy in columns:
        copy.wait()
    spread_and_transform(got_ref, [charge_ref[k] for k in range(2)], table_ref, out_ref, rho)
    for copy in halo:
        copy.wait()


def plane_kernel(in_ref, slope_ref, table_ref, turned_ref, mixed_ref, mixed_turned_ref, out_ref, wide_ref, send_sem,
                 recv_sem):
    place = here()
    devices = [toward(place, side) for side in SIDES]
    signal(devices)

    def keep(t, _):
        x, y, z = lax.div(t, 8), lax.rem(lax.div(t, 4), 2), lax.rem(t, 4)
        wide_ref[x + 1, y + 1, z + 1] = slope_ref[x, y, z]
        return 0

    lax.fori_loop(0, 32, keep, 0)
    await_signals(26)
    halo = halo_copies(slope_ref, 0, wide_ref, place, send_sem, recv_sem)
    transform_planes(place[0] * 32 + place[1] * 4 + place[2], in_ref, table_ref, turned_ref, mixed_ref, mixed_turned_ref,
                     out_ref)
    for copy in halo:
        copy.wait()


def transform_planes(me, in_ref, table_ref, turned_ref, mixed_ref, mixed_turned_ref, out_ref):
    lane = lax.broadcasted_iota(jnp.int32, (16, 8, 128), 2)

    def pick(ref, half, g):
        return jnp.concatenate([ref[gx, half * 4 + g] for gx in range(4)], axis=0)

    rows = []
    for xr in range(4):
        pair = []
        for half in range(2):
            value = jnp.zeros((16, 8, 128), F32)
            for g in range(4):
                block = pick(in_ref, half, g)
                if g != xr:
                    block = pltpu.roll(block.reshape(128, 128), (g - xr) * 32 % 128, 1).reshape(16, 8, 128)
                value = jnp.where(lax.div(lane, 32) == g, block, value)
            pair.append(value.reshape(128, 128))
        rows.append(jnp.concatenate(pair, axis=1))
    plane = jnp.concatenate(rows, axis=0)
    turned = (turned_ref[0], turned_ref[1])
    along_y = split(dot3(split(plane), turned))

    row = lax.broadcasted_iota(jnp.int32, (256, 256), 0)
    col = lax.broadcasted_iota(jnp.int32, (256, 256), 1)
    scale = 2.0 * math.pi / 256
    wave_x = jnp.where(row <= 128, row, row - 128).astype(F32) * scale
    wave_y = jnp.where(col <= 128, col, col - 128).astype(F32) * scale
    flat = wave_x * wave_x + wave_y * wave_y
    side = lax.div(lax.rem(lax.broadcasted_iota(jnp.int32, (256, 512), 1), 8), 4)
    side_turned = lax.div(lax.rem(lax.broadcasted_iota(jnp.int32, (512, 256), 0), 8), 4)
    total = None
    for p in range(2):
        mode = me if p == 0 else jnp.where(me == 0, 128, me)
        wave_z = jnp.full((256, 256), mode, jnp.int32).astype(F32) * scale
        squared = flat + wave_z * wave_z
        anchor = squared == 0.0
        green = jnp.where(anchor, 0.0, 4.0 * math.pi * jnp.exp(-squared / (4.0 * EWALD_SPLIT * EWALD_SPLIT))
                          / jnp.where(anchor, 1.0, squared))
        left = [jnp.where(side == p, mixed_ref[i].astype(F32), 0.0).astype(BF16) for i in range(2)]
        modes = split3(dot3(left, along_y) * green)
        back = [jnp.where(side_turned == p, mixed_turned_ref[i].astype(F32), 0.0).astype(BF16) for i in range(3)]
        part = dot6(back, modes)
        total = part if total is None else total + part
    field = dot6(split3(total), [table_ref[i] for i in range(3)])
    for half in range(2):
        block = [field[xr * 128:(xr + 1) * 128, half * 128:(half + 1) * 128] for xr in range(4)]
        for g in range(4):
            value = jnp.zeros((16, 8, 128), F32)
            for xr in range(4):
                moved = block[xr]
                if g != xr:
                    moved = pltpu.roll(moved, (xr - g) * 32 % 128, 1)
                value = jnp.where(lax.div(lane, 32) == xr, moved.reshape(16, 8, 128), value)
            for gx in range(4):
                out_ref[gx, half * 4 + g] = value[gx * 4:(gx + 1) * 4]


def sample_kernel(charge_ref, in_ref, atoms_ref, table_ref, back_ref, field, out, send_sem, recv_sem):
    place = here()
    signal(column_devices(place))
    charges = [charge_ref[k] for k in range(2)]
    columns = [
        jnp.concatenate([in_ref[pl.ds(plane * 4 + xq, 128, stride=8), :] for xq in range(4)], axis=1)
        for plane in range(2)
    ]
    modes = jnp.concatenate(columns, axis=0)
    lines = jnp.concatenate([modes[:, i * 128:(i + 1) * 128].T for i in range(4)], axis=0)
    pieces_of_field = split3(dot6(split3(lines), [table_ref[i] for i in range(3)]))
    for group in range(2):
        for i, piece in enumerate(pieces_of_field):
            field[group, :, i * 128:(i + 1) * 128] = piece[:, group * 128:(group + 1) * 128]
    await_signals(3)
    point = lax.broadcasted_iota(jnp.int32, (128, 128), 0).astype(F32)

    def cell(n):
        owner = lax.rem(place[2] + 1 + lax.div(n, 8), 4)
        own_cell = lax.rem(n, 8)
        cyl, cz = lax.div(own_cell, 4), owner * 4 + lax.rem(own_cell, 4)

        def row(f):
            return atoms_ref[owner, own_cell, f:f + 1, :]

        ox, oy, oz, fx, fy, fz = [row(f) for f in range(6)]
        charge = by_species(row(6), charges)
        lower_z = oz + (lax.rem(cz, 8) * 16).astype(F32)
        lower = jnp.where(point == lower_z, 1.0, 0.0)
        slope = jnp.where(point == lower_z + 1.0, 1.0, 0.0) - lower
        right = jnp.concatenate([lower, slope], axis=1).astype(BF16)
        right = jnp.concatenate([right, right, right], axis=0)
        left = field_rows(field, lax.div(cz, 8), cyl)
        both = dot(left, right)
        tilt = both[:, 128:256].reshape(16, 16, 128)
        plain = both[:, 0:128].reshape(16, 16, 128) + fz * tilt
        spot = lax.broadcasted_iota(jnp.int32, (16, 128), 0).astype(F32)
        low_y, high_y = spot == oy, spot == oy + 1.0
        wy = jnp.where(low_y, 1.0 - fy, 0.0) + jnp.where(high_y, fy, 0.0)
        sy = jnp.where(high_y, 1.0, 0.0) - jnp.where(low_y, 1.0, 0.0)

        def fold(value):
            return value[:, 0:8] + value[:, 8:16]

        plain_w, plain_s, tilt_w = fold(plain * wy), fold(plain * sy), fold(tilt * wy)
        x_sum = jnp.zeros((8, 128), F32)
        y_sum, z_sum = x_sum, x_sum
        for x in range(16):
            low_x, high_x = ox == x, ox == x - 1
            wx = jnp.where(low_x, 1.0 - fx, 0.0) + jnp.where(high_x, fx, 0.0)
            sx = jnp.where(high_x, 1.0, 0.0) - jnp.where(low_x, 1.0, 0.0)
            x_sum = x_sum + sx * plain_w[x]
            y_sum = y_sum + wx * plain_s[x]
            z_sum = z_sum + wx * tilt_w[x]
        for f, value in enumerate((x_sum, y_sum, z_sum)):
            out[owner, own_cell, f:f + 1, :] = -charge * jnp.sum(value, axis=0, keepdims=True)
        out[owner, own_cell, 3:4, :] = charge

    def group(g, _):
        def later(n, _):
            cell(n)
            return 0

        lax.fori_loop(g * 8 + 1, g * 8 + 8, later, 0)
        return 0

    copies = []
    for g in range(4):
        cell(g * 8)
        if g:
            copies.append(column_copy(out, back_ref, place, send_sem, recv_sem, g - 1))
        group(g, 0)

    def mine(n, _):
        back_ref[place[2], n] = out[place[2], n]
        return 0

    lax.fori_loop(0, 8, mine, 0)
    for copy in copies:
        copy.wait()


def field_rows(field, group, cyl):
    start = pl.multiple_of(cyl * 16, 16)
    return jnp.concatenate([field[group, pl.ds(start + 32 * x, 16), :] for x in range(16)], axis=0)


TABLE, MIXED = tables()


def constants():
    return (parts_of(TABLE), parts_of(TABLE.T)[:2], parts_of(MIXED)[:2], parts_of(MIXED.T))


def gather_pass(charge, counts, offset, fraction, species, table):
    return pl.pallas_call(
        gather_kernel,
        out_shape=[
            jax.ShapeDtypeStruct((6, 4, 6, 4, 128), F32),
            jax.ShapeDtypeStruct((4, 8, 8, 128), F32),
            jax.ShapeDtypeStruct((1024, 128), F32),
        ],
        in_specs=[SMEM_SPEC] * 2 + [VMEM_SPEC] * 4,
        out_specs=[VMEM_SPEC] * 3,
        scratch_shapes=[pltpu.VMEM((4, 8, 8, 128), F32), pltpu.VMEM((256, 512), F32), DMA((26,)), DMA((26,)), DMA((3,)),
                        DMA((3,))],
        compiler_params=comm_params(0),
        name="gather_pass",
    )(charge, counts, offset, fraction, species, table)


def plane_pass(planes, slope, table, turned, mixed, mixed_turned):
    return pl.pallas_call(
        plane_kernel,
        out_shape=[jax.ShapeDtypeStruct((4, 8, 4, 8, 128), F32), jax.ShapeDtypeStruct((6, 4, 6, 1, 128), F32)],
        in_specs=[VMEM_SPEC] * 6,
        out_specs=[VMEM_SPEC] * 2,
        scratch_shapes=[DMA((26,)), DMA((26,))],
        compiler_params=comm_params(1),
        name="plane_pass",
    )(planes, slope, table, turned, mixed, mixed_turned)


def sample_pass(charge, lines, atoms, table):
    return pl.pallas_call(
        sample_kernel,
        out_shape=jax.ShapeDtypeStruct((4, 8, 4, 128), F32),
        in_specs=[SMEM_SPEC] + [VMEM_SPEC] * 3,
        out_specs=VMEM_SPEC,
        scratch_shapes=[pltpu.VMEM((2, 512, 384), BF16), pltpu.VMEM((4, 8, 4, 128), F32), DMA((3,)), DMA((3,))],
        compiler_params=comm_params(2),
        name="sample_pass",
    )(charge, lines, atoms, table)


def on_device(cell_counts, grid_offset, fraction, species, species_density, species_pair, species_embed, species_charge):
    counts = cell_counts.reshape(32)
    table, turned, mixed, mixed_turned = constants()
    extended, columns, lines = gather_pass(
        species_charge, counts, grid_offset.reshape(32, 3, 128), fraction.reshape(32, 3, 128), species.reshape(8, 4, 128),
        table)
    extended = extended.reshape(144, 4, 128)
    planes = lax.all_to_all(lines.reshape(128, 8, 128), AXES, split_axis=0, concat_axis=0, tiled=True)
    density, slope = density_pass(species_density, species_pair, species_embed, extended)
    planes, wide_slope = plane_pass(
        planes.reshape(4, 8, 4, 8, 128), slope.reshape(4, 2, 4, 1, 128), table, turned, mixed, mixed_turned)
    lines = lax.all_to_all(planes.reshape(128, 8, 128), AXES, split_axis=0, concat_axis=0, tiled=True)
    eam = force_pass(counts, species_density, species_pair, extended, wide_slope.reshape(144, 1, 128))
    electric = sample_pass(species_charge, lines.reshape(1024, 128), columns, table)
    electric = electric.reshape(4, 2, 4, 4, 128)[:, :, :, 0:3]
    eam = eam.reshape(3, 4, 2, 4, 128).transpose(1, 2, 3, 0, 4)
    return eam + COUPLING * electric, density.reshape(4, 2, 4, 128)


def solution(mesh):
    return jax.shard_map(
        on_device,
        mesh=mesh,
        in_specs=(
            P("gx", "gy", "gz"),
            P("gx", "gy", "gz", None, None),
            P("gx", "gy", "gz", None, None),
            P("gx", "gy", "gz", None),
            P(),
            P(),
            P(),
            P(),
        ),
        out_specs=(P("gx", "gy", "gz", None, None), P("gx", "gy", "gz", None)),
        check_vma=False,
    )
```

```python
import itertools
import math

import jax
import jax.numpy as jnp
import numpy as np
from jax import lax
from jax.experimental import pallas as pl
from jax.experimental.pallas import tpu as pltpu
from jax.sharding import PartitionSpec as P

PPC = 16
COUPLING = 8.0
F32, BF16 = jnp.float32, jnp.bfloat16
VMEM_SPEC = pl.BlockSpec(memory_space=pltpu.VMEM)
SMEM_SPEC = pl.BlockSpec(memory_space=pltpu.SMEM)


MESH = pl.DeviceIdType.MESH
AXES = ("gx", "gy", "gz")
SIZES = (4, 8, 4)
SIDES = [side for side in itertools.product((-1, 0, 1), repeat=3) if side != (0, 0, 0)]


def here():
    return [lax.axis_index(axis) for axis in AXES]


def toward(place, side):
    return tuple(lax.rem(p + s + n, n) for p, s, n in zip(place, side, SIZES))


def signal(devices):
    barrier = pltpu.get_barrier_semaphore()
    for device in devices:
        pl.semaphore_signal(barrier, inc=1, device_id=device, device_id_type=MESH)


def await_signals(count):
    pl.semaphore_wait(pltpu.get_barrier_semaphore(), count)


def send(src, dst, send_sem, recv_sem, device):
    copy = pltpu.make_async_remote_copy(
        src_ref=src, dst_ref=dst, send_sem=send_sem, recv_sem=recv_sem, device_id=device, device_id_type=MESH)
    copy.start()
    return copy


def halo_copies(own_ref, rim, ext_ref, place, send_sem, recv_sem):
    copies = []
    for n, side in enumerate(SIDES):
        src, dst = [], []
        for s, cells in zip(side, (4, 2, 4)):
            src.append(pl.ds(rim, cells) if s == 0 else pl.ds(rim + (cells - 1 if s == 1 else 0), 1))
            dst.append(pl.ds(1, cells) if s == 0 else pl.ds(0 if s == 1 else cells + 1, 1))
        copies.append(send(own_ref.at[tuple(src)], ext_ref.at[tuple(dst)], send_sem.at[n], recv_sem.at[n],
                           toward(place, side)))
    return copies


def column_copy(src_ref, dst_ref, place, send_sem, recv_sem, n):
    gx, gy, gz = place
    other = lax.rem(gz + n + 1, 4)
    return send(src_ref.at[other], dst_ref.at[gz], send_sem.at[n], recv_sem.at[n], (gx, gy, other))


def column_copies(src_ref, dst_ref, place, send_sem, recv_sem):
    return [column_copy(src_ref, dst_ref, place, send_sem, recv_sem, n) for n in range(3)]


def column_devices(place):
    gx, gy, gz = place
    return [(gx, gy, lax.rem(gz + n + 1, 4)) for n in range(3)]


DMA = pltpu.SemaphoreType.DMA


def comm_params(number):
    return pltpu.CompilerParams(collective_id=number, has_side_effects=True, vmem_limit_bytes=32 << 20)


ROWS = 16
KF = 32


def pieces(value):
    first = value.astype(BF16).astype(F32)
    rest = value - first
    second = rest.astype(BF16).astype(F32)
    third = (rest - second).astype(BF16).astype(F32)
    return first, second, third


def by_species(code, values):
    return jnp.where(code == 0.0, values[0], jnp.where(code == 1.0, values[1], 0.0))


def filled(ref, k):
    return jnp.full((8, 128), ref[k], F32)


def cube_root(value):
    guess = jnp.exp(jnp.log(value) * (1.0 / 3.0))
    return guess - (guess * guess * guess - value) / (3.0 * guess * guess)


def sublane():
    return lax.broadcasted_iota(jnp.int32, (8, 128), 0)


def assemble(blocks, ones, twos):
    rows = []
    for value, one, two in zip(blocks, ones, twos):
        first, second, third = pieces(value)
        rows.append(jnp.where(one, first, jnp.where(two, second, third)))
    return jnp.concatenate(rows, axis=0)


def patterns(first, second, last_first, last_second):
    ones, twos = [], []
    for block in range(4):
        one = two = None
        for k in range(block * 8, block * 8 + 8):
            here_one = (k % 6 in first) if k < 24 else k in last_first
            here_two = (k % 6 in second) if k < 24 else k in last_second
            if here_one:
                one = (sublane() == k % 8) if one is None else one | (sublane() == k % 8)
            if here_two:
                two = (sublane() == k % 8) if two is None else two | (sublane() == k % 8)
        ones.append(one)
        twos.append(two)
    return ones, twos


def source_features(ext_ref, slope_ref, wide, feat_b, scales, ratios):
    ones, twos = patterns((0, 2, 5), (1, 3), (24,), (25,))
    low_six, low_four, low_two, low_three = [sublane() < n for n in (6, 4, 2, 3)]

    def cell(r, _):
        def row(f):
            return jnp.broadcast_to(ext_ref[r, f:f + 1, :], (8, 128))

        x = row(0) + (lax.div(r, 24) - 3).astype(F32)
        y = row(1) + (lax.rem(lax.div(r, 6), 4) - 2).astype(F32)
        z = row(2) + (lax.rem(r, 6) - 3).astype(F32)
        code = row(3)
        scale = by_species(code, scales)
        if wide is not None:
            wide[r, 0], wide[r, 1], wide[r, 2] = x, y, z
            wide[r, 3] = jnp.where(code == 1.0, ratios[1], ratios[0])
            wide[r, 4] = jnp.broadcast_to(slope_ref[r], (8, 128))
        square = -scale * (x * x + y * y + z * z)
        double = scale + scale
        x, y, z = double * x, double * y, double * z
        blocks = [jnp.where(low_six, scale, x), jnp.where(low_four, x, y), jnp.where(low_two, y, z),
                  jnp.where(low_three, square, 0.0)]
        feat_b[pl.ds(pl.multiple_of(r * KF, KF), KF), :] = assemble(blocks, ones, twos).astype(BF16)
        return 0

    lax.fori_loop(0, 144, cell, 0, unroll=4)


def corner(t):
    return (lax.div(t, 8) * 4 + lax.rem(lax.div(t, 4), 2)) * 6 + lax.rem(t, 4)


def target_features(ext_ref, own_t, keep, slope_ref, gains, ratios):
    ones, twos = patterns((0, 1, 4), (2, 3), (24, 25, 26, 27, 29), (28, 30))
    low_six, low_four, low_two, low_three = [sublane() < n for n in (6, 4, 2, 3)]
    low_five, low_seven = sublane() < 5, sublane() < 7

    def cell(t, _):
        r = corner(t) + 31

        def row(f):
            return jnp.broadcast_to(ext_ref[r, f:f + 1, :], (8, 128))

        x = row(0) + (lax.div(t, 8) - 2).astype(F32)
        y = row(1) + (lax.rem(lax.div(t, 4), 2) - 1).astype(F32)
        z = row(2) + (lax.rem(t, 4) - 2).astype(F32)
        code = row(3)
        for n, value in enumerate((x, y, z, code)):
            keep[n, pl.ds(t, 1), :] = value[0:1]
        rest = 1.0 - (x * x + y * y + z * z)
        tail = jnp.zeros((8, 128), F32)
        if gains is not None:
            second = code == 1.0
            tilt = jnp.broadcast_to(slope_ref[r], (8, 128)) / jnp.where(second, ratios[1], ratios[0])
            tail = jnp.where(low_five, jnp.where(second, gains[1], gains[0]), jnp.where(low_seven, tilt, 0.0))
        blocks = [jnp.where(low_six, rest, x), jnp.where(low_four, x, y), jnp.where(low_two, y, z),
                  jnp.where(low_three, 1.0, tail)]
        own_t[t] = assemble(blocks, ones, twos).T.astype(BF16)
        return 0

    lax.fori_loop(0, 32, cell, 0, unroll=4)


def split3(value):
    first = value.astype(BF16)
    rest = value - first.astype(F32)
    second = rest.astype(BF16)
    return first, second, (rest - second.astype(F32)).astype(BF16)


def lane_sums(rows):
    ones = jnp.ones((8, rows.shape[1]), BF16)
    return lax.dot_general(ones, rows, (((1,), (1,)), ((), ())), preferred_element_type=F32)


def right_side(feat_b, cell):
    r = pl.multiple_of(cell * KF, KF)
    return jnp.concatenate([feat_b[pl.ds(r + KF * dz, KF), :] for dz in range(3)], axis=1)


def density_kernel(amplitude_ref, pair_ref, embed_ref, ext_ref, density_ref, slope_ref, feat_b, own_t, keep, totals, mat):
    amplitudes, pairs, embeds = [[filled(ref, k) for k in range(2)] for ref in (amplitude_ref, pair_ref, embed_ref)]
    source_features(ext_ref, None, None, feat_b, [cube_root(value) for value in amplitudes], None)
    target_features(ext_ref, own_t, keep, None, None, None)
    lanes = lax.broadcasted_iota(jnp.int32, (128, 128), 1)
    other = lanes != lax.broadcasted_iota(jnp.int32, (128, 128), 0)

    def target(t):
        cx, cy, cz = lax.div(t, 8), lax.rem(lax.div(t, 4), 2), lax.rem(t, 4)
        left = own_t[t]
        total = jnp.zeros((128, 128), F32)
        for dx in range(3):
            for dy in range(3):
                right = right_side(feat_b, ((cx + dx) * 4 + cy + dy) * 6 + cz)
                weight = jnp.dot(left, right, preferred_element_type=F32)
                weight = jnp.maximum(weight, 0.0)
                for dz in range(3):
                    part = weight[:, dz * 128:(dz + 1) * 128]
                    if dx == 1 and dy == 1 and dz == 1:
                        part = jnp.where(other, part, 0.0)
                    total = total + part * part * part
        return total

    def settle(n):
        first, second, _ = split3(totals[...])
        sums = lane_sums(jnp.concatenate([first, second], axis=1))
        mat[pl.ds(2 * n, 1), :] = sums[0:1, 0:128]
        mat[pl.ds(2 * n + 1, 1), :] = sums[0:1, 128:256]

    totals[...] = jnp.zeros((256, 128), F32)

    def both(n, _):
        settle(jnp.maximum(n - 1, 0))
        totals[0:128, :] = target(2 * n)
        totals[128:256, :] = target(2 * n + 1)
        return 0

    lax.fori_loop(0, 16, both, 0)
    settle(15)
    code = keep[3]
    alive = by_species(code, (1.0, 1.0))
    density = mat[0:32, :] * alive
    density_ref[...] = density.reshape(8, 4, 128)
    tilts = [jnp.concatenate([3.0 * embed / (pair * pair)] * 4, axis=0) for embed, pair in zip(embeds, pairs)]
    slope_ref[...] = (by_species(code, tilts) / jnp.sqrt(1.0 + density)).reshape(32, 1, 128)


def force_kernel(count_ref, amplitude_ref, pair_ref, ext_ref, slope_ref, out_ref, feat_b, own_t, keep, wide, near_a, near_b,
                 part_a, part_b, mat, table):
    amplitudes, pairs = [[filled(ref, k) for k in range(2)] for ref in (amplitude_ref, pair_ref)]
    ratios = [amplitude / (pair * pair) for amplitude, pair in zip(amplitudes, pairs)]
    gains = [-4.0 * pair / amplitude for amplitude, pair in zip(amplitudes, pairs)]
    source_features(ext_ref, slope_ref, wide, feat_b, pairs, ratios)
    target_features(ext_ref, own_t, keep, slope_ref, gains, ratios)
    feat_b[144 * KF:146 * KF, :] = jnp.concatenate([sel_matrix()[:, 0:128], sel_matrix()[:, 128:256]], axis=0)

    def fill(n, _):
        table[n] = jnp.where(n < 27, (lax.div(n, 9) * 4 + lax.rem(lax.div(n, 3), 3)) * 6 + lax.rem(n, 3),
                             jnp.where(n == 28, 145, 144))
        table[32 + n] = jnp.where(n < 27, 1, 0)
        return 0

    lax.fori_loop(0, 32, fill, 0)
    part_a[...] = jnp.zeros((4, 128, 128), F32)
    part_b[...] = jnp.zeros((4, 128, 128), F32)
    lane = lax.broadcasted_iota(jnp.int32, (ROWS, 128), 1)
    lane3 = lax.broadcasted_iota(jnp.int32, (ROWS // 8, 8, 128), 2)
    row3 = lax.broadcasted_iota(jnp.int32, (ROWS // 8, 8, 128), 0) * 8 + lax.broadcasted_iota(
        jnp.int32, (ROWS // 8, 8, 128), 1)

    def around(base, k):
        return base + (k // 9 * 4 + k // 3 % 3) * 6 + k % 3

    def multiply(t, near, part):
        left, base = own_t[t], corner(t)
        for k in range(0, 8, 2):
            right = []
            for n in (part * 8 + k, part * 8 + k + 1):
                start = pl.multiple_of((table[n] + table[32 + n] * base) * KF, KF)
                right.append(feat_b[pl.ds(start, KF), :])
            product = jnp.dot(left, jnp.concatenate(right, axis=1), preferred_element_type=F32)
            near[part * 8 + k] = product[:, 0:128]
            near[part * 8 + k + 1] = product[:, 128:256]

    def chunk(t, near, part, c):
        rows = pl.ds(pl.multiple_of(c * ROWS, ROWS), ROWS)
        base = corner(t)

        def block(k):
            return near[k, rows, :].reshape(ROWS // 8, 8, 128)

        gain, tilt = block(27), block(28)
        zero = jnp.zeros((ROWS // 8, 8, 128), F32)
        m0, mx, my, mz = zero, zero, zero, zero
        for k in range(27):
            r = around(base, k)
            w = jnp.maximum(block(k), 0.0)
            if k == 13:
                w = jnp.where(lane3 != row3 + c * ROWS, w, 0.0)
            value = ((tilt * wide[r, 3] + wide[r, 4]) * w + gain) * w
            m0 = m0 + value
            mx = mx + value * wide[r, 0]
            my = my + value * wide[r, 1]
            mz = mz + value * wide[r, 2]
        for m, value in enumerate((m0, mx, my, mz)):
            part[m, rows, :] = value.reshape(ROWS, 128)

    def settle(t, part):
        for m in (0, 2):
            first, second, third = split3(jnp.concatenate([part[m], part[m + 1]], axis=0))
            sums = lane_sums(jnp.concatenate([first, second], axis=1)) + lane_sums(third)
            mat[pl.ds(t * 4 + m, 1), :] = sums[0:1, 0:128]
            mat[pl.ds(t * 4 + m + 1, 1), :] = sums[0:1, 128:256]

    for part in range(4):
        multiply(0, near_a, part)

    def target(t, near, following, part, before):
        later = jnp.minimum(t + 1, 31)

        def rest(c, _):
            chunk(t, near, part, c)
            return 0

        settle(jnp.maximum(t - 1, 0), before)
        for n in range(4):
            multiply(later, following, n)
            chunk(t, near, part, n)
        lax.fori_loop(4, lax.div(count_ref[lax.div(t, 8), lax.rem(lax.div(t, 4), 2), lax.rem(t, 4)] + ROWS - 1, ROWS), rest, 0)

    def pair(n, _):
        target(2 * n, near_a, near_b, part_a, part_b)
        target(2 * n + 1, near_b, near_a, part_b, part_a)
        return 0

    lax.fori_loop(0, 16, pair, 0)
    settle(31, part_b)
    whole = mat[pl.ds(0, 32, stride=4), :]
    amplitude = by_species(keep[3], [jnp.concatenate([value] * 4, axis=0) for value in amplitudes])
    for m in range(3):
        value = amplitude * (mat[pl.ds(m + 1, 32, stride=4), :] - keep[m] * whole)
        out_ref[:, m] = value.reshape(8, 4, 128)


def sel_matrix():
    row = lax.broadcasted_iota(jnp.int32, (KF, 256), 0)
    lane = lax.broadcasted_iota(jnp.int32, (KF, 256), 1)
    first = (row >= 27) & (row < 29) & (lane < 128)
    second = (row >= 29) & (row < 31) & (lane >= 128)
    return jnp.where(first | second, 1.0, 0.0).astype(BF16)


def features_scratch():
    return [pltpu.VMEM((146 * KF, 128), BF16), pltpu.VMEM((32, 128, KF), BF16), pltpu.VMEM((4, 32, 128), F32)]


def density_pass(amplitude, pair, embed, ext):
    return pl.pallas_call(
        density_kernel,
        out_shape=[jax.ShapeDtypeStruct((8, 4, 128), F32), jax.ShapeDtypeStruct((32, 1, 128), F32)],
        in_specs=[SMEM_SPEC] * 3 + [VMEM_SPEC],
        out_specs=[VMEM_SPEC] * 2,
        scratch_shapes=features_scratch() + [pltpu.VMEM((256, 128), F32), pltpu.VMEM((128, 128), F32)],
        compiler_params=pltpu.CompilerParams(vmem_limit_bytes=16 << 20),
        cost_estimate=pl.CostEstimate(flops=10_000_000_000, bytes_accessed=1_000_000, transcendentals=0),
        name="density_pass",
    )(amplitude, pair, embed, ext)


def force_pass(counts, amplitude, pair, ext, slope):
    return pl.pallas_call(
        force_kernel,
        out_shape=jax.ShapeDtypeStruct((8, 3, 4, 128), F32),
        in_specs=[SMEM_SPEC] * 3 + [VMEM_SPEC] * 2,
        out_specs=VMEM_SPEC,
        scratch_shapes=features_scratch() + [
            pltpu.VMEM((144, 5, 8, 128), F32),
            pltpu.VMEM((32, 128, 128), F32),
            pltpu.VMEM((32, 128, 128), F32),
            pltpu.VMEM((4, 128, 128), F32),
            pltpu.VMEM((4, 128, 128), F32),
            pltpu.VMEM((128, 128), F32),
            pltpu.SMEM((64,), jnp.int32),
        ],
        compiler_params=pltpu.CompilerParams(vmem_limit_bytes=24 << 20),
        cost_estimate=pl.CostEstimate(flops=20_000_000_000, bytes_accessed=1_000_000, transcendentals=0),
        name="force_pass",
    )(counts, amplitude, pair, ext, slope)


EWALD_SPLIT = 0.7


def tables():
    mode = np.arange(256)[:, None]
    point = np.arange(256)[None, :]
    cosine = np.cos(2 * np.pi * (mode * point % 256) / 256) * np.sqrt(2 / 256)
    cosine[0] /= np.sqrt(2)
    cosine[128] /= np.sqrt(2)
    sine = np.sin(2 * np.pi * ((mode - 128) * point % 256) / 256) * np.sqrt(2 / 256)
    table = np.where(mode <= 128, cosine, sine)
    row = np.arange(512)
    xr, cell, s = row // 128, row // 8 % 16, row % 8
    mixed = table[:, cell * 16 + s % 4 * 4 + xr]
    return table, mixed


def parts_of(array):
    parts = []
    for _ in range(3):
        parts.append(array.astype(np.float32).astype(jnp.bfloat16))
        array = array - parts[-1].astype(np.float64)
    return np.stack(parts)


def split(value):
    high = value.astype(BF16)
    return high, (value - high.astype(F32)).astype(BF16)


def dot(a, b):
    return jnp.dot(a, b, preferred_element_type=F32)


def dot3(a, b):
    return dot(a[0], b[0]) + (dot(a[1], b[0]) + dot(a[0], b[1]))


def dot6(a, b):
    small = dot(a[1], b[1]) + (dot(a[2], b[0]) + dot(a[0], b[2]))
    return dot(a[0], b[0]) + (dot(a[1], b[0]) + dot(a[0], b[1]) + small)


def hat(count, lower, weight):
    point = lax.broadcasted_iota(jnp.int32, (count, lower.shape[1]), 0).astype(F32)
    return jnp.where(point == lower, 1.0 - weight, 0.0) + jnp.where(point == lower + 1.0, weight, 0.0)


def spread_and_transform(atoms_ref, charges, table_ref, out_ref, rho):
    def layer(cz, _):
        source, cell = lax.div(cz, 4), lax.rem(cz, 4)

        def row(f, shift=0.0):
            first = atoms_ref[source, cell, f:f + 1, :]
            second = atoms_ref[source, cell + 4, f:f + 1, :] + shift
            return jnp.concatenate([first, second], axis=1)

        ox, oy, oz, fx, fy, fz = row(0), row(1, 16.0), row(2), row(3), row(4), row(5)
        charge = by_species(row(6), charges)
        wy = hat(32, oy, fy)
        wz = split(hat(16, oz, fz) * charge)
        parts = []
        for x in range(16):
            wx = jnp.where(ox == x, 1.0 - fx, 0.0) + jnp.where(ox == x - 1, fx, 0.0)
            parts.append(wx * wy)
        plane = split(jnp.concatenate(parts, axis=0))
        dims = (((1,), (1,)), ((), ()))

        def against(a, b):
            return lax.dot_general(a, b, dims, preferred_element_type=F32)

        value = against(wz[0], plane[0]) + (against(wz[1], plane[0]) + against(wz[0], plane[1]))
        rho[pl.ds(pl.multiple_of(cz * 16, 16), 16), :] = value
        return 0

    lax.fori_loop(0, 16, layer, 0, unroll=2)
    lines = dot3((table_ref[0], table_ref[1]), split(rho[...]))
    for plane in range(2):
        for xq in range(4):
            out_ref[pl.ds(plane * 4 + xq, 128, stride=8), :] = lines[
                plane * 128:(plane + 1) * 128, xq * 128:(xq + 1) * 128]


def gather_kernel(charge_ref, count_ref, offset_ref, fraction_ref, species_ref, table_ref, ext_ref, got_ref, out_ref,
                  atoms, rho, send_sem, recv_sem, column_send, column_recv):
    place = here()
    signal([toward(place, side) for side in SIDES] + [column_devices(place)[1]])
    slot = lax.broadcasted_iota(jnp.int32, (1, 128), 1)

    def pack(n, _):
        x, y = lax.div(n, 2), lax.rem(n, 2)
        for z in range(4):
            code = jnp.where(slot < count_ref[x, y, z], species_ref[x, y, z:z + 1, :].astype(F32), -1.0)
            for d in range(3):
                offset, fraction = offset_ref[x, y, d, z:z + 1, :].astype(F32), fraction_ref[x, y, d, z:z + 1, :]
                ext_ref[x + 1, y + 1, z + 1, d:d + 1, :] = (offset + 0.5 + fraction) * (1.0 / PPC)
                atoms[x, y * 4 + z, d:d + 1, :] = offset
                atoms[x, y * 4 + z, d + 3:d + 4, :] = fraction
            ext_ref[x + 1, y + 1, z + 1, 3:4, :] = code
            atoms[x, y * 4 + z, 6:7, :] = code
            atoms[x, y * 4 + z, 7:8, :] = code
        return 0

    lax.fori_loop(0, 8, pack, 0)

    def keep(n, _):
        got_ref[place[2], n] = atoms[place[2], n]
        return 0

    lax.fori_loop(0, 8, keep, 0)
    await_signals(27)
    columns = column_copies(atoms, got_ref, place, column_send, column_recv)
    halo = halo_copies(ext_ref, 1, ext_ref, place, send_sem, recv_sem)
    for copy in columns:
        copy.wait()
    spread_and_transform(got_ref, [charge_ref[k] for k in range(2)], table_ref, out_ref, rho)
    for copy in halo:
        copy.wait()


def plane_kernel(in_ref, slope_ref, table_ref, turned_ref, mixed_ref, mixed_turned_ref, out_ref, wide_ref, send_sem,
                 recv_sem):
    place = here()
    devices = [toward(place, side) for side in SIDES]
    signal(devices)

    def keep(t, _):
        x, y, z = lax.div(t, 8), lax.rem(lax.div(t, 4), 2), lax.rem(t, 4)
        wide_ref[x + 1, y + 1, z + 1] = slope_ref[x, y, z]
        return 0

    lax.fori_loop(0, 32, keep, 0)
    await_signals(26)
    halo = halo_copies(slope_ref, 0, wide_ref, place, send_sem, recv_sem)
    transform_planes(place[0] * 32 + place[1] * 4 + place[2], in_ref, table_ref, turned_ref, mixed_ref, mixed_turned_ref,
                     out_ref)
    for copy in halo:
        copy.wait()


def transform_planes(me, in_ref, table_ref, turned_ref, mixed_ref, mixed_turned_ref, out_ref):
    lane = lax.broadcasted_iota(jnp.int32, (16, 8, 128), 2)

    def pick(ref, half, g):
        return jnp.concatenate([ref[gx, half * 4 + g] for gx in range(4)], axis=0)

    rows = []
    for xr in range(4):
        pair = []
        for half in range(2):
            value = jnp.zeros((16, 8, 128), F32)
            for g in range(4):
                block = pick(in_ref, half, g)
                if g != xr:
                    block = pltpu.roll(block.reshape(128, 128), (g - xr) * 32 % 128, 1).reshape(16, 8, 128)
                value = jnp.where(lax.div(lane, 32) == g, block, value)
            pair.append(value.reshape(128, 128))
        rows.append(jnp.concatenate(pair, axis=1))
    plane = jnp.concatenate(rows, axis=0)
    turned = (turned_ref[0], turned_ref[1])
    along_y = split(dot3(split(plane), turned))

    row = lax.broadcasted_iota(jnp.int32, (256, 256), 0)
    col = lax.broadcasted_iota(jnp.int32, (256, 256), 1)
    scale = 2.0 * math.pi / 256
    wave_x = jnp.where(row <= 128, row, row - 128).astype(F32) * scale
    wave_y = jnp.where(col <= 128, col, col - 128).astype(F32) * scale
    flat = wave_x * wave_x + wave_y * wave_y
    side = lax.div(lax.rem(lax.broadcasted_iota(jnp.int32, (256, 512), 1), 8), 4)
    side_turned = lax.div(lax.rem(lax.broadcasted_iota(jnp.int32, (512, 256), 0), 8), 4)
    total = None
    for p in range(2):
        mode = me if p == 0 else jnp.where(me == 0, 128, me)
        wave_z = jnp.full((256, 256), mode, jnp.int32).astype(F32) * scale
        squared = flat + wave_z * wave_z
        anchor = squared == 0.0
        green = jnp.where(anchor, 0.0, 4.0 * math.pi * jnp.exp(-squared / (4.0 * EWALD_SPLIT * EWALD_SPLIT))
                          / jnp.where(anchor, 1.0, squared))
        left = [jnp.where(side == p, mixed_ref[i].astype(F32), 0.0).astype(BF16) for i in range(2)]
        modes = split3(dot3(left, along_y) * green)
        back = [jnp.where(side_turned == p, mixed_turned_ref[i].astype(F32), 0.0).astype(BF16) for i in range(3)]
        part = dot6(back, modes)
        total = part if total is None else total + part
    field = dot6(split3(total), [table_ref[i] for i in range(3)])
    for half in range(2):
        block = [field[xr * 128:(xr + 1) * 128, half * 128:(half + 1) * 128] for xr in range(4)]
        for g in range(4):
            value = jnp.zeros((16, 8, 128), F32)
            for xr in range(4):
                moved = block[xr]
                if g != xr:
                    moved = pltpu.roll(moved, (xr - g) * 32 % 128, 1)
                value = jnp.where(lax.div(lane, 32) == xr, moved.reshape(16, 8, 128), value)
            for gx in range(4):
                out_ref[gx, half * 4 + g] = value[gx * 4:(gx + 1) * 4]


def sample_kernel(charge_ref, in_ref, atoms_ref, table_ref, back_ref, field, out, send_sem, recv_sem):
    place = here()
    signal(column_devices(place))
    charges = [charge_ref[k] for k in range(2)]
    columns = [
        jnp.concatenate([in_ref[pl.ds(plane * 4 + xq, 128, stride=8), :] for xq in range(4)], axis=1)
        for plane in range(2)
    ]
    modes = jnp.concatenate(columns, axis=0)
    lines = jnp.concatenate([modes[:, i * 128:(i + 1) * 128].T for i in range(4)], axis=0)
    pieces_of_field = split3(dot6(split3(lines), [table_ref[i] for i in range(3)]))
    for group in range(2):
        for i, piece in enumerate(pieces_of_field):
            field[group, :, i * 128:(i + 1) * 128] = piece[:, group * 128:(group + 1) * 128]
    await_signals(3)
    point = lax.broadcasted_iota(jnp.int32, (128, 128), 0).astype(F32)

    def cell(n):
        owner = lax.rem(place[2] + 1 + lax.div(n, 8), 4)
        own_cell = lax.rem(n, 8)
        cyl, cz = lax.div(own_cell, 4), owner * 4 + lax.rem(own_cell, 4)

        def row(f):
            return atoms_ref[owner, own_cell, f:f + 1, :]

        ox, oy, oz, fx, fy, fz = [row(f) for f in range(6)]
        charge = by_species(row(6), charges)
        lower_z = oz + (lax.rem(cz, 8) * 16).astype(F32)
        lower = jnp.where(point == lower_z, 1.0, 0.0)
        slope = jnp.where(point == lower_z + 1.0, 1.0, 0.0) - lower
        right = jnp.concatenate([lower, slope], axis=1).astype(BF16)
        right = jnp.concatenate([right, right, right], axis=0)
        left = field_rows(field, lax.div(cz, 8), cyl)
        both = dot(left, right)
        tilt = both[:, 128:256].reshape(16, 16, 128)
        plain = both[:, 0:128].reshape(16, 16, 128) + fz * tilt
        spot = lax.broadcasted_iota(jnp.int32, (16, 128), 0).astype(F32)
        low_y, high_y = spot == oy, spot == oy + 1.0
        wy = jnp.where(low_y, 1.0 - fy, 0.0) + jnp.where(high_y, fy, 0.0)
        sy = jnp.where(high_y, 1.0, 0.0) - jnp.where(low_y, 1.0, 0.0)

        def fold(value):
            return value[:, 0:8] + value[:, 8:16]

        plain_w, plain_s, tilt_w = fold(plain * wy), fold(plain * sy), fold(tilt * wy)
        x_sum = jnp.zeros((8, 128), F32)
        y_sum, z_sum = x_sum, x_sum
        for x in range(16):
            low_x, high_x = ox == x, ox == x - 1
            wx = jnp.where(low_x, 1.0 - fx, 0.0) + jnp.where(high_x, fx, 0.0)
            sx = jnp.where(high_x, 1.0, 0.0) - jnp.where(low_x, 1.0, 0.0)
            x_sum = x_sum + sx * plain_w[x]
            y_sum = y_sum + wx * plain_s[x]
            z_sum = z_sum + wx * tilt_w[x]
        for f, value in enumerate((x_sum, y_sum, z_sum)):
            out[owner, cyl, f, pl.ds(lax.rem(own_cell, 4), 1), :] = -charge * jnp.sum(value, axis=0, keepdims=True)

    def group(g, _):
        def later(n, _):
            cell(n)
            return 0

        lax.fori_loop(g * 8 + 2, g * 8 + 8, later, 0, unroll=2)
        return 0

    copies = []
    for g in range(4):
        cell(g * 8)
        cell(g * 8 + 1)
        if g:
            copies.append(column_copy(out, back_ref, place, send_sem, recv_sem, g - 1))
        group(g, 0)

    back_ref[place[2]] = out[place[2]]
    for copy in copies:
        copy.wait()


def field_rows(field, group, cyl):
    start = pl.multiple_of(cyl * 16, 16)
    return jnp.concatenate([field[group, pl.ds(start + 32 * x, 16), :] for x in range(16)], axis=0)


TABLE, MIXED = tables()


def constants():
    return (parts_of(TABLE), parts_of(TABLE.T)[:2], parts_of(MIXED)[:2], parts_of(MIXED.T))


def gather_pass(charge, counts, offset, fraction, species, table):
    return pl.pallas_call(
        gather_kernel,
        out_shape=[
            jax.ShapeDtypeStruct((6, 4, 6, 4, 128), F32),
            jax.ShapeDtypeStruct((4, 8, 8, 128), F32),
            jax.ShapeDtypeStruct((1024, 128), F32),
        ],
        in_specs=[SMEM_SPEC] * 2 + [VMEM_SPEC] * 4,
        out_specs=[VMEM_SPEC] * 3,
        scratch_shapes=[pltpu.VMEM((4, 8, 8, 128), F32), pltpu.VMEM((256, 512), F32), DMA((26,)), DMA((26,)), DMA((3,)),
                        DMA((3,))],
        compiler_params=comm_params(0),
        name="gather_pass",
    )(charge, counts, offset, fraction, species, table)


def plane_pass(planes, slope, table, turned, mixed, mixed_turned):
    return pl.pallas_call(
        plane_kernel,
        out_shape=[jax.ShapeDtypeStruct((4, 8, 4, 8, 128), F32), jax.ShapeDtypeStruct((6, 4, 6, 1, 128), F32)],
        in_specs=[VMEM_SPEC] * 6,
        out_specs=[VMEM_SPEC] * 2,
        scratch_shapes=[DMA((26,)), DMA((26,))],
        compiler_params=comm_params(1),
        name="plane_pass",
    )(planes, slope, table, turned, mixed, mixed_turned)


def sample_pass(charge, lines, atoms, table):
    return pl.pallas_call(
        sample_kernel,
        out_shape=jax.ShapeDtypeStruct((4, 2, 3, 4, 128), F32),
        in_specs=[SMEM_SPEC] + [VMEM_SPEC] * 3,
        out_specs=VMEM_SPEC,
        scratch_shapes=[pltpu.VMEM((2, 512, 384), BF16), pltpu.VMEM((4, 2, 3, 4, 128), F32), DMA((3,)), DMA((3,))],
        compiler_params=comm_params(2),
        name="sample_pass",
    )(charge, lines, atoms, table)


def on_device(cell_counts, grid_offset, fraction, species, species_density, species_pair, species_embed, species_charge):
    table, turned, mixed, mixed_turned = constants()
    order = (0, 1, 3, 2, 4)
    extended, columns, lines = gather_pass(
        species_charge, cell_counts, grid_offset.transpose(order), fraction.transpose(order), species, table)
    extended = extended.reshape(144, 4, 128)
    planes = lax.all_to_all(lines.reshape(128, 8, 128), AXES, split_axis=0, concat_axis=0, tiled=True)
    density, slope = density_pass(species_density, species_pair, species_embed, extended)
    planes, wide_slope = plane_pass(
        planes.reshape(4, 8, 4, 8, 128), slope.reshape(4, 2, 4, 1, 128), table, turned, mixed, mixed_turned)
    lines = lax.all_to_all(planes.reshape(128, 8, 128), AXES, split_axis=0, concat_axis=0, tiled=True)
    eam = force_pass(cell_counts, species_density, species_pair, extended, wide_slope.reshape(144, 1, 128))
    electric = sample_pass(species_charge, lines.reshape(1024, 128), columns, table)
    forces = eam.reshape(4, 2, 3, 4, 128) + COUPLING * electric
    return forces.transpose(order), density.reshape(4, 2, 4, 128)


def solution(mesh):
    return jax.shard_map(
        on_device,
        mesh=mesh,
        in_specs=(
            P("gx", "gy", "gz"),
            P("gx", "gy", "gz", None, None),
            P("gx", "gy", "gz", None, None),
            P("gx", "gy", "gz", None),
            P(),
            P(),
            P(),
            P(),
        ),
        out_specs=(P("gx", "gy", "gz", None, None), P("gx", "gy", "gz", None)),
        check_vma=False,
    )
```

```python
import itertools
import math

import jax
import jax.numpy as jnp
import numpy as np
from jax import lax
from jax.experimental import pallas as pl
from jax.experimental.pallas import tpu as pltpu
from jax.sharding import PartitionSpec as P

PPC = 16
COUPLING = 8.0
F32, BF16 = jnp.float32, jnp.bfloat16
VMEM_SPEC = pl.BlockSpec(memory_space=pltpu.VMEM)
SMEM_SPEC = pl.BlockSpec(memory_space=pltpu.SMEM)


MESH = pl.DeviceIdType.MESH
AXES = ("gx", "gy", "gz")
SIZES = (4, 8, 4)
SIDES = [side for side in itertools.product((-1, 0, 1), repeat=3) if side != (0, 0, 0)]


def here():
    return [lax.axis_index(axis) for axis in AXES]


def toward(place, side):
    return tuple(lax.rem(p + s + n, n) for p, s, n in zip(place, side, SIZES))


def signal(devices):
    barrier = pltpu.get_barrier_semaphore()
    for device in devices:
        pl.semaphore_signal(barrier, inc=1, device_id=device, device_id_type=MESH)


def await_signals(count):
    pl.semaphore_wait(pltpu.get_barrier_semaphore(), count)


def send(src, dst, send_sem, recv_sem, device):
    copy = pltpu.make_async_remote_copy(
        src_ref=src, dst_ref=dst, send_sem=send_sem, recv_sem=recv_sem, device_id=device, device_id_type=MESH)
    copy.start()
    return copy


def halo_copies(own_ref, rim, ext_ref, place, send_sem, recv_sem):
    copies = []
    for n, side in enumerate(SIDES):
        src, dst = [], []
        for s, cells in zip(side, (4, 2, 4)):
            src.append(pl.ds(rim, cells) if s == 0 else pl.ds(rim + (cells - 1 if s == 1 else 0), 1))
            dst.append(pl.ds(1, cells) if s == 0 else pl.ds(0 if s == 1 else cells + 1, 1))
        copies.append(send(own_ref.at[tuple(src)], ext_ref.at[tuple(dst)], send_sem.at[n], recv_sem.at[n],
                           toward(place, side)))
    return copies


def column_copy(src_ref, dst_ref, place, send_sem, recv_sem, n):
    gx, gy, gz = place
    other = lax.rem(gz + n + 1, 4)
    return send(src_ref.at[other], dst_ref.at[gz], send_sem.at[n], recv_sem.at[n], (gx, gy, other))


def column_copies(src_ref, dst_ref, place, send_sem, recv_sem):
    return [column_copy(src_ref, dst_ref, place, send_sem, recv_sem, n) for n in range(3)]


def column_devices(place):
    gx, gy, gz = place
    return [(gx, gy, lax.rem(gz + n + 1, 4)) for n in range(3)]


DMA = pltpu.SemaphoreType.DMA


def comm_params(number):
    return pltpu.CompilerParams(collective_id=number, has_side_effects=True, vmem_limit_bytes=32 << 20)


ROWS = 16
KF = 32


def pieces(value):
    first = value.astype(BF16).astype(F32)
    rest = value - first
    second = rest.astype(BF16).astype(F32)
    third = (rest - second).astype(BF16).astype(F32)
    return first, second, third


def by_species(code, values):
    return jnp.where(code == 0.0, values[0], jnp.where(code == 1.0, values[1], 0.0))


def filled(ref, k):
    return jnp.full((8, 128), ref[k], F32)


def cube_root(value):
    guess = jnp.exp(jnp.log(value) * (1.0 / 3.0))
    return guess - (guess * guess * guess - value) / (3.0 * guess * guess)


def sublane():
    return lax.broadcasted_iota(jnp.int32, (8, 128), 0)


def assemble(blocks, ones, twos):
    rows = []
    for value, one, two in zip(blocks, ones, twos):
        first, second, third = pieces(value)
        rows.append(jnp.where(one, first, jnp.where(two, second, third)))
    return jnp.concatenate(rows, axis=0)


def patterns(first, second, last_first, last_second):
    ones, twos = [], []
    for block in range(4):
        one = two = None
        for k in range(block * 8, block * 8 + 8):
            here_one = (k % 6 in first) if k < 24 else k in last_first
            here_two = (k % 6 in second) if k < 24 else k in last_second
            if here_one:
                one = (sublane() == k % 8) if one is None else one | (sublane() == k % 8)
            if here_two:
                two = (sublane() == k % 8) if two is None else two | (sublane() == k % 8)
        ones.append(one)
        twos.append(two)
    return ones, twos


def cell_at(r):
    return lax.div(r, 24), lax.rem(lax.div(r, 6), 4), lax.rem(r, 6)


def source_features(ext_ref, slope_ref, wide, feat_b, scales, ratios):
    ones, twos = patterns((0, 2, 5), (1, 3), (24,), (25,))
    low_six, low_four, low_two, low_three = [sublane() < n for n in (6, 4, 2, 3)]

    def cell(r, _):
        def row(f):
            x, y, z = cell_at(r)
            return jnp.broadcast_to(ext_ref[x, y, z, f:f + 1, :], (8, 128))

        x = row(0) + (lax.div(r, 24) - 3).astype(F32)
        y = row(1) + (lax.rem(lax.div(r, 6), 4) - 2).astype(F32)
        z = row(2) + (lax.rem(r, 6) - 3).astype(F32)
        code = row(3)
        scale = by_species(code, scales)
        if wide is not None:
            wide[r, 0], wide[r, 1], wide[r, 2] = x, y, z
            wide[r, 3] = jnp.where(code == 1.0, ratios[1], ratios[0])
            wide[r, 4] = jnp.broadcast_to(slope_ref[cell_at(r)], (8, 128))
        square = -scale * (x * x + y * y + z * z)
        double = scale + scale
        x, y, z = double * x, double * y, double * z
        blocks = [jnp.where(low_six, scale, x), jnp.where(low_four, x, y), jnp.where(low_two, y, z),
                  jnp.where(low_three, square, 0.0)]
        feat_b[pl.ds(pl.multiple_of(r * KF, KF), KF), :] = assemble(blocks, ones, twos).astype(BF16)
        return 0

    lax.fori_loop(0, 144, cell, 0, unroll=4)


def corner(t):
    return (lax.div(t, 8) * 4 + lax.rem(lax.div(t, 4), 2)) * 6 + lax.rem(t, 4)


def target_features(ext_ref, own_t, keep, slope_ref, gains, ratios):
    ones, twos = patterns((0, 1, 4), (2, 3), (24, 25, 26, 27, 29), (28, 30))
    low_six, low_four, low_two, low_three = [sublane() < n for n in (6, 4, 2, 3)]
    low_five, low_seven = sublane() < 5, sublane() < 7

    def cell(t, _):
        r = corner(t) + 31

        def row(f):
            x, y, z = cell_at(r)
            return jnp.broadcast_to(ext_ref[x, y, z, f:f + 1, :], (8, 128))

        x = row(0) + (lax.div(t, 8) - 2).astype(F32)
        y = row(1) + (lax.rem(lax.div(t, 4), 2) - 1).astype(F32)
        z = row(2) + (lax.rem(t, 4) - 2).astype(F32)
        code = row(3)
        for n, value in enumerate((x, y, z, code)):
            keep[n, pl.ds(t, 1), :] = value[0:1]
        rest = 1.0 - (x * x + y * y + z * z)
        tail = jnp.zeros((8, 128), F32)
        if gains is not None:
            second = code == 1.0
            tilt = jnp.broadcast_to(slope_ref[cell_at(r)], (8, 128)) / jnp.where(second, ratios[1], ratios[0])
            tail = jnp.where(low_five, jnp.where(second, gains[1], gains[0]), jnp.where(low_seven, tilt, 0.0))
        blocks = [jnp.where(low_six, rest, x), jnp.where(low_four, x, y), jnp.where(low_two, y, z),
                  jnp.where(low_three, 1.0, tail)]
        own_t[t] = assemble(blocks, ones, twos).T.astype(BF16)
        return 0

    lax.fori_loop(0, 32, cell, 0, unroll=4)


def split3(value):
    first = value.astype(BF16)
    rest = value - first.astype(F32)
    second = rest.astype(BF16)
    return first, second, (rest - second.astype(F32)).astype(BF16)


def lane_sums(rows):
    ones = jnp.ones((8, rows.shape[1]), BF16)
    return lax.dot_general(ones, rows, (((1,), (1,)), ((), ())), preferred_element_type=F32)


def right_side(feat_b, cell):
    r = pl.multiple_of(cell * KF, KF)
    return jnp.concatenate([feat_b[pl.ds(r + KF * dz, KF), :] for dz in range(3)], axis=1)


def density_features(ext_ref, amplitudes, feat_b, own_t, keep):
    source_features(ext_ref, None, None, feat_b, [cube_root(value) for value in amplitudes], None)
    target_features(ext_ref, own_t, keep, None, None, None)


def densities(pairs, embeds, density_ref, slope_ref, feat_b, own_t, keep, totals, mat):
    lanes = lax.broadcasted_iota(jnp.int32, (128, 128), 1)
    other = lanes != lax.broadcasted_iota(jnp.int32, (128, 128), 0)

    def target(t):
        cx, cy, cz = lax.div(t, 8), lax.rem(lax.div(t, 4), 2), lax.rem(t, 4)
        left = own_t[t]
        total = jnp.zeros((128, 128), F32)
        for dx in range(3):
            for dy in range(3):
                right = right_side(feat_b, ((cx + dx) * 4 + cy + dy) * 6 + cz)
                weight = jnp.dot(left, right, preferred_element_type=F32)
                weight = jnp.maximum(weight, 0.0)
                for dz in range(3):
                    part = weight[:, dz * 128:(dz + 1) * 128]
                    if dx == 1 and dy == 1 and dz == 1:
                        part = jnp.where(other, part, 0.0)
                    total = total + part * part * part
        return total

    def settle(n):
        first, second, _ = split3(totals[...])
        sums = lane_sums(jnp.concatenate([first, second], axis=1))
        mat[pl.ds(2 * n, 1), :] = sums[0:1, 0:128]
        mat[pl.ds(2 * n + 1, 1), :] = sums[0:1, 128:256]

    totals[...] = jnp.zeros((256, 128), F32)

    def both(n, _):
        settle(jnp.maximum(n - 1, 0))
        totals[0:128, :] = target(2 * n)
        totals[128:256, :] = target(2 * n + 1)
        return 0

    lax.fori_loop(0, 16, both, 0)
    settle(15)
    code = keep[3]
    alive = by_species(code, (1.0, 1.0))
    density = mat[0:32, :] * alive
    density_ref[...] = density.reshape(8, 4, 128)
    tilts = [jnp.concatenate([3.0 * embed / (pair * pair)] * 4, axis=0) for embed, pair in zip(embeds, pairs)]
    slope_ref[...] = (by_species(code, tilts) / jnp.sqrt(1.0 + density)).reshape(4, 2, 4, 1, 128)


def force_kernel(count_ref, amplitude_ref, pair_ref, ext_ref, slope_ref, given_ref, out_ref, density_ref, feat_b, own_t, keep, wide, near_a, near_b,
                 part_a, part_b, mat, table):
    amplitudes, pairs = [[filled(ref, k) for k in range(2)] for ref in (amplitude_ref, pair_ref)]
    ratios = [amplitude / (pair * pair) for amplitude, pair in zip(amplitudes, pairs)]
    density_ref[...] = given_ref[...]
    gains = [-4.0 * pair / amplitude for amplitude, pair in zip(amplitudes, pairs)]
    source_features(ext_ref, slope_ref, wide, feat_b, pairs, ratios)
    target_features(ext_ref, own_t, keep, slope_ref, gains, ratios)
    feat_b[144 * KF:146 * KF, :] = jnp.concatenate([sel_matrix()[:, 0:128], sel_matrix()[:, 128:256]], axis=0)

    def fill(n, _):
        table[n] = jnp.where(n < 27, (lax.div(n, 9) * 4 + lax.rem(lax.div(n, 3), 3)) * 6 + lax.rem(n, 3),
                             jnp.where(n == 28, 145, 144))
        table[32 + n] = jnp.where(n < 27, 1, 0)
        return 0

    lax.fori_loop(0, 32, fill, 0)
    part_a[...] = jnp.zeros((4, 128, 128), F32)
    part_b[...] = jnp.zeros((4, 128, 128), F32)
    lane = lax.broadcasted_iota(jnp.int32, (ROWS, 128), 1)
    lane3 = lax.broadcasted_iota(jnp.int32, (ROWS // 8, 8, 128), 2)
    row3 = lax.broadcasted_iota(jnp.int32, (ROWS // 8, 8, 128), 0) * 8 + lax.broadcasted_iota(
        jnp.int32, (ROWS // 8, 8, 128), 1)

    def around(base, k):
        return base + (k // 9 * 4 + k // 3 % 3) * 6 + k % 3

    def multiply(t, near, part):
        left, base = own_t[t], corner(t)
        for k in range(0, 8, 2):
            right = []
            for n in (part * 8 + k, part * 8 + k + 1):
                start = pl.multiple_of((table[n] + table[32 + n] * base) * KF, KF)
                right.append(feat_b[pl.ds(start, KF), :])
            product = jnp.dot(left, jnp.concatenate(right, axis=1), preferred_element_type=F32)
            near[part * 8 + k] = product[:, 0:128]
            near[part * 8 + k + 1] = product[:, 128:256]

    def chunk(t, near, part, c):
        rows = pl.ds(pl.multiple_of(c * ROWS, ROWS), ROWS)
        base = corner(t)

        def block(k):
            return near[k, rows, :].reshape(ROWS // 8, 8, 128)

        gain, tilt = block(27), block(28)
        zero = jnp.zeros((ROWS // 8, 8, 128), F32)
        m0, mx, my, mz = zero, zero, zero, zero
        for k in range(27):
            r = around(base, k)
            w = jnp.maximum(block(k), 0.0)
            if k == 13:
                w = jnp.where(lane3 != row3 + c * ROWS, w, 0.0)
            value = ((tilt * wide[r, 3] + wide[r, 4]) * w + gain) * w
            m0 = m0 + value
            mx = mx + value * wide[r, 0]
            my = my + value * wide[r, 1]
            mz = mz + value * wide[r, 2]
        for m, value in enumerate((m0, mx, my, mz)):
            part[m, rows, :] = value.reshape(ROWS, 128)

    def settle(t, part):
        for m in (0, 2):
            first, second, third = split3(jnp.concatenate([part[m], part[m + 1]], axis=0))
            sums = lane_sums(jnp.concatenate([first, second], axis=1)) + lane_sums(third)
            mat[pl.ds(t * 4 + m, 1), :] = sums[0:1, 0:128]
            mat[pl.ds(t * 4 + m + 1, 1), :] = sums[0:1, 128:256]

    for part in range(4):
        multiply(0, near_a, part)

    def target(t, near, following, part, before):
        later = jnp.minimum(t + 1, 31)

        def rest(c, _):
            chunk(t, near, part, c)
            return 0

        settle(jnp.maximum(t - 1, 0), before)
        for n in range(4):
            multiply(later, following, n)
            chunk(t, near, part, n)
        lax.fori_loop(4, lax.div(count_ref[lax.div(t, 8), lax.rem(lax.div(t, 4), 2), lax.rem(t, 4)] + ROWS - 1, ROWS), rest, 0)

    def pair(n, _):
        target(2 * n, near_a, near_b, part_a, part_b)
        target(2 * n + 1, near_b, near_a, part_b, part_a)
        return 0

    lax.fori_loop(0, 16, pair, 0)
    settle(31, part_b)
    whole = mat[pl.ds(0, 32, stride=4), :]
    amplitude = by_species(keep[3], [jnp.concatenate([value] * 4, axis=0) for value in amplitudes])
    for m in range(3):
        value = amplitude * (mat[pl.ds(m + 1, 32, stride=4), :] - keep[m] * whole)
        out_ref[:, m] = value.reshape(8, 4, 128)


def sel_matrix():
    row = lax.broadcasted_iota(jnp.int32, (KF, 256), 0)
    lane = lax.broadcasted_iota(jnp.int32, (KF, 256), 1)
    first = (row >= 27) & (row < 29) & (lane < 128)
    second = (row >= 29) & (row < 31) & (lane >= 128)
    return jnp.where(first | second, 1.0, 0.0).astype(BF16)


def features_scratch():
    return [pltpu.VMEM((146 * KF, 128), BF16), pltpu.VMEM((32, 128, KF), BF16), pltpu.VMEM((4, 32, 128), F32)]


def force_pass(counts, amplitude, pair, ext, slope, density):
    return pl.pallas_call(
        force_kernel,
        out_shape=[jax.ShapeDtypeStruct((8, 3, 4, 128), F32), jax.ShapeDtypeStruct((8, 4, 128), F32)],
        in_specs=[SMEM_SPEC] * 3 + [VMEM_SPEC] * 3,
        out_specs=[VMEM_SPEC] * 2,
        scratch_shapes=features_scratch() + [
            pltpu.VMEM((144, 5, 8, 128), F32),
            pltpu.VMEM((32, 128, 128), F32),
            pltpu.VMEM((32, 128, 128), F32),
            pltpu.VMEM((4, 128, 128), F32),
            pltpu.VMEM((4, 128, 128), F32),
            pltpu.VMEM((128, 128), F32),
            pltpu.SMEM((64,), jnp.int32),
        ],
        compiler_params=pltpu.CompilerParams(vmem_limit_bytes=24 << 20),
        cost_estimate=pl.CostEstimate(flops=20_000_000_000, bytes_accessed=1_000_000, transcendentals=0),
        name="force_pass",
    )(counts, amplitude, pair, ext, slope, density)


EWALD_SPLIT = 0.7


def tables():
    mode = np.arange(256)[:, None]
    point = np.arange(256)[None, :]
    cosine = np.cos(2 * np.pi * (mode * point % 256) / 256) * np.sqrt(2 / 256)
    cosine[0] /= np.sqrt(2)
    cosine[128] /= np.sqrt(2)
    sine = np.sin(2 * np.pi * ((mode - 128) * point % 256) / 256) * np.sqrt(2 / 256)
    table = np.where(mode <= 128, cosine, sine)
    row = np.arange(512)
    xr, cell, s = row // 128, row // 8 % 16, row % 8
    mixed = table[:, cell * 16 + s % 4 * 4 + xr]
    return table, mixed


def parts_of(array):
    parts = []
    for _ in range(3):
        parts.append(array.astype(np.float32).astype(jnp.bfloat16))
        array = array - parts[-1].astype(np.float64)
    return np.stack(parts)


def split(value):
    high = value.astype(BF16)
    return high, (value - high.astype(F32)).astype(BF16)


def dot(a, b):
    return jnp.dot(a, b, preferred_element_type=F32)


def dot3(a, b):
    return dot(a[0], b[0]) + (dot(a[1], b[0]) + dot(a[0], b[1]))


def dot6(a, b):
    small = dot(a[1], b[1]) + (dot(a[2], b[0]) + dot(a[0], b[2]))
    return dot(a[0], b[0]) + (dot(a[1], b[0]) + dot(a[0], b[1]) + small)


def hat(count, lower, weight):
    point = lax.broadcasted_iota(jnp.int32, (count, lower.shape[1]), 0).astype(F32)
    return jnp.where(point == lower, 1.0 - weight, 0.0) + jnp.where(point == lower + 1.0, weight, 0.0)


def spread_and_transform(atoms_ref, charges, table_ref, out_ref, rho):
    def layer(cz, _):
        source, cell = lax.div(cz, 4), lax.rem(cz, 4)

        def row(f, shift=0.0):
            first = atoms_ref[source, cell, f:f + 1, :]
            second = atoms_ref[source, cell + 4, f:f + 1, :] + shift
            return jnp.concatenate([first, second], axis=1)

        ox, oy, oz, fx, fy, fz = row(0), row(1, 16.0), row(2), row(3), row(4), row(5)
        charge = by_species(row(6), charges)
        wy = hat(32, oy, fy)
        wz = split(hat(16, oz, fz) * charge)
        parts = []
        for x in range(16):
            wx = jnp.where(ox == x, 1.0 - fx, 0.0) + jnp.where(ox == x - 1, fx, 0.0)
            parts.append(wx * wy)
        plane = split(jnp.concatenate(parts, axis=0))
        dims = (((1,), (1,)), ((), ()))

        def against(a, b):
            return lax.dot_general(a, b, dims, preferred_element_type=F32)

        value = against(wz[0], plane[0]) + (against(wz[1], plane[0]) + against(wz[0], plane[1]))
        rho[pl.ds(pl.multiple_of(cz * 16, 16), 16), :] = value
        return 0

    lax.fori_loop(0, 16, layer, 0, unroll=2)
    lines = dot3((table_ref[0], table_ref[1]), split(rho[...]))
    for plane in range(2):
        for xq in range(4):
            out_ref[pl.ds(plane * 4 + xq, 128, stride=8), :] = lines[
                plane * 128:(plane + 1) * 128, xq * 128:(xq + 1) * 128]


def device_at(d):
    return lax.div(d, 32), lax.rem(lax.div(d, 4), 8), lax.rem(d, 4)


def front_kernel(charge_hbm, amplitude_hbm, pair_hbm, embed_hbm, count_hbm, offset_hbm, fraction_hbm, species_hbm, table_hbm,
                 turned_hbm, mixed_hbm, mixed_turned_hbm, ext_ref, got_ref, density_ref, wide_ref, out_ref,
                 charge_ref, amplitude_ref, pair_ref, embed_ref, count_ref, offset_ref, fraction_ref, species_ref, table_ref,
                 turned_ref, mixed_ref, mixed_turned_ref, atoms, rho, lines, planes, slopes, feat_b, own_t, rows, totals, mat,
                 load_sem, halo_send, halo_recv, column_send, column_recv, slope_send, slope_recv, line_send, line_recv):
    place = here()
    me = place[0] * 32 + place[1] * 4 + place[2]
    loads = [
        pltpu.make_async_copy(src, dst, load_sem.at[n])
        for n, (src, dst) in enumerate((
            (count_hbm, count_ref), (species_hbm, species_ref), (offset_hbm, offset_ref), (fraction_hbm, fraction_ref),
            (charge_hbm, charge_ref), (amplitude_hbm, amplitude_ref), (pair_hbm, pair_ref), (embed_hbm, embed_ref),
            (table_hbm, table_ref), (turned_hbm, turned_ref), (mixed_hbm, mixed_ref), (mixed_turned_hbm, mixed_turned_ref)))
    ]
    for load in loads:
        load.start()
    barrier = pltpu.get_barrier_semaphore()

    def greet(i, _):
        pl.semaphore_signal(barrier, inc=1, device_id=device_at(lax.rem(me + i, 128)), device_id_type=MESH)
        return 0

    lax.fori_loop(1, 128, greet, 0)
    for load in loads[:4]:
        load.wait()
    slot = lax.broadcasted_iota(jnp.int32, (1, 128), 1)

    def pack(n, _):
        x, y = lax.div(n, 2), lax.rem(n, 2)
        for z in range(4):
            code = jnp.where(slot < count_ref[x, y, z], species_ref[x, y, z:z + 1, :].astype(F32), -1.0)
            for d in range(3):
                offset, fraction = offset_ref[x, y, d, z:z + 1, :].astype(F32), fraction_ref[x, y, d, z:z + 1, :]
                ext_ref[x + 1, y + 1, z + 1, d:d + 1, :] = (offset + 0.5 + fraction) * (1.0 / PPC)
                atoms[x, y * 4 + z, d:d + 1, :] = offset
                atoms[x, y * 4 + z, d + 3:d + 4, :] = fraction
            ext_ref[x + 1, y + 1, z + 1, 3:4, :] = code
            atoms[x, y * 4 + z, 6:7, :] = code
            atoms[x, y * 4 + z, 7:8, :] = code
        return 0

    lax.fori_loop(0, 8, pack, 0)

    def keep_own(n, _):
        got_ref[place[2], n] = atoms[place[2], n]
        return 0

    lax.fori_loop(0, 8, keep_own, 0)
    for load in loads[4:]:
        load.wait()
    pl.semaphore_wait(barrier, 127)
    columns = column_copies(atoms, got_ref, place, column_send, column_recv)
    halo = halo_copies(ext_ref, 1, ext_ref, place, halo_send, halo_recv)
    for copy in columns:
        copy.wait()
    spread_and_transform(got_ref, [charge_ref[k] for k in range(2)], table_ref, lines, rho)
    for copy in halo:
        copy.wait()
    amplitudes, pairs, embeds = [[filled(ref, k) for k in range(2)] for ref in (amplitude_ref, pair_ref, embed_ref)]
    density_features(ext_ref, amplitudes, feat_b, own_t, rows)

    def line_copy(i):
        other = lax.rem(me + i, 128)
        return pltpu.make_async_remote_copy(
            src_ref=lines.at[pl.ds(pl.multiple_of(other * 8, 8), 8), :],
            dst_ref=planes.at[pl.ds(pl.multiple_of(me * 8, 8), 8), :],
            send_sem=line_send.at[i],
            recv_sem=line_recv.at[i],
            device_id=device_at(other),
            device_id_type=MESH,
        )

    def send_line(i, _):
        line_copy(i).start()
        return 0

    def wait_line(i, _):
        line_copy(i).wait()
        return 0

    lax.fori_loop(1, 128, send_line, 0)
    mine = pl.ds(pl.multiple_of(me * 8, 8), 8)
    planes[mine, :] = lines[mine, :]
    densities(pairs, embeds, density_ref, slopes, feat_b, own_t, rows, totals, mat)

    def keep_slope(t, _):
        x, y, z = lax.div(t, 8), lax.rem(lax.div(t, 4), 2), lax.rem(t, 4)
        wide_ref[x + 1, y + 1, z + 1] = slopes[x, y, z]
        return 0

    lax.fori_loop(0, 32, keep_slope, 0)
    halo = halo_copies(slopes, 0, wide_ref, place, slope_send, slope_recv)
    lax.fori_loop(1, 128, wait_line, 0)
    transform_planes(me, planes, table_ref, turned_ref, mixed_ref, mixed_turned_ref, out_ref)
    for copy in halo:
        copy.wait()


def transform_planes(me, in_ref, table_ref, turned_ref, mixed_ref, mixed_turned_ref, out_ref):
    lane = lax.broadcasted_iota(jnp.int32, (16, 8, 128), 2)

    def pick(ref, half, g):
        starts = [(gx * 32 + (half * 4 + g) * 4) * 8 for gx in range(4)]
        return jnp.concatenate([ref[start:start + 32, :] for start in starts], axis=0).reshape(16, 8, 128)

    rows = []
    for xr in range(4):
        pair = []
        for half in range(2):
            value = jnp.zeros((16, 8, 128), F32)
            for g in range(4):
                block = pick(in_ref, half, g)
                if g != xr:
                    block = pltpu.roll(block.reshape(128, 128), (g - xr) * 32 % 128, 1).reshape(16, 8, 128)
                value = jnp.where(lax.div(lane, 32) == g, block, value)
            pair.append(value.reshape(128, 128))
        rows.append(jnp.concatenate(pair, axis=1))
    plane = jnp.concatenate(rows, axis=0)
    turned = (turned_ref[0], turned_ref[1])
    along_y = split(dot3(split(plane), turned))

    row = lax.broadcasted_iota(jnp.int32, (256, 256), 0)
    col = lax.broadcasted_iota(jnp.int32, (256, 256), 1)
    scale = 2.0 * math.pi / 256
    wave_x = jnp.where(row <= 128, row, row - 128).astype(F32) * scale
    wave_y = jnp.where(col <= 128, col, col - 128).astype(F32) * scale
    flat = wave_x * wave_x + wave_y * wave_y
    side = lax.div(lax.rem(lax.broadcasted_iota(jnp.int32, (256, 512), 1), 8), 4)
    side_turned = lax.div(lax.rem(lax.broadcasted_iota(jnp.int32, (512, 256), 0), 8), 4)
    total = None
    for p in range(2):
        mode = me if p == 0 else jnp.where(me == 0, 128, me)
        wave_z = jnp.full((256, 256), mode, jnp.int32).astype(F32) * scale
        squared = flat + wave_z * wave_z
        anchor = squared == 0.0
        green = jnp.where(anchor, 0.0, 4.0 * math.pi * jnp.exp(-squared / (4.0 * EWALD_SPLIT * EWALD_SPLIT))
                          / jnp.where(anchor, 1.0, squared))
        left = [jnp.where(side == p, mixed_ref[i].astype(F32), 0.0).astype(BF16) for i in range(2)]
        modes = split3(dot3(left, along_y) * green)
        back = [jnp.where(side_turned == p, mixed_turned_ref[i].astype(F32), 0.0).astype(BF16) for i in range(3)]
        part = dot6(back, modes)
        total = part if total is None else total + part
    field = dot6(split3(total), [table_ref[i] for i in range(3)])
    for half in range(2):
        block = [field[xr * 128:(xr + 1) * 128, half * 128:(half + 1) * 128] for xr in range(4)]
        for g in range(4):
            value = jnp.zeros((16, 8, 128), F32)
            for xr in range(4):
                moved = block[xr]
                if g != xr:
                    moved = pltpu.roll(moved, (xr - g) * 32 % 128, 1)
                value = jnp.where(lax.div(lane, 32) == xr, moved.reshape(16, 8, 128), value)
            for gx in range(4):
                start = (gx * 32 + (half * 4 + g) * 4) * 8
                out_ref[start:start + 32, :] = value[gx * 4:(gx + 1) * 4].reshape(32, 128)


def sample_kernel(charge_ref, in_ref, atoms_ref, table_ref, back_ref, field, out, send_sem, recv_sem):
    place = here()
    signal(column_devices(place))
    charges = [charge_ref[k] for k in range(2)]
    columns = [
        jnp.concatenate([in_ref[pl.ds(plane * 4 + xq, 128, stride=8), :] for xq in range(4)], axis=1)
        for plane in range(2)
    ]
    modes = jnp.concatenate(columns, axis=0)
    lines = jnp.concatenate([modes[:, i * 128:(i + 1) * 128].T for i in range(4)], axis=0)
    pieces_of_field = split3(dot6(split3(lines), [table_ref[i] for i in range(3)]))
    for group in range(2):
        for i, piece in enumerate(pieces_of_field):
            field[group, :, i * 128:(i + 1) * 128] = piece[:, group * 128:(group + 1) * 128]
    await_signals(3)
    point = lax.broadcasted_iota(jnp.int32, (128, 128), 0).astype(F32)

    def cell(n):
        owner = lax.rem(place[2] + 1 + lax.div(n, 8), 4)
        own_cell = lax.rem(n, 8)
        cyl, cz = lax.div(own_cell, 4), owner * 4 + lax.rem(own_cell, 4)

        def row(f):
            return atoms_ref[owner, own_cell, f:f + 1, :]

        ox, oy, oz, fx, fy, fz = [row(f) for f in range(6)]
        charge = by_species(row(6), charges)
        lower_z = oz + (lax.rem(cz, 8) * 16).astype(F32)
        lower = jnp.where(point == lower_z, 1.0, 0.0)
        slope = jnp.where(point == lower_z + 1.0, 1.0, 0.0) - lower
        right = jnp.concatenate([lower, slope], axis=1).astype(BF16)
        right = jnp.concatenate([right, right, right], axis=0)
        left = field_rows(field, lax.div(cz, 8), cyl)
        both = dot(left, right)
        tilt = both[:, 128:256].reshape(16, 16, 128)
        plain = both[:, 0:128].reshape(16, 16, 128) + fz * tilt
        spot = lax.broadcasted_iota(jnp.int32, (16, 128), 0).astype(F32)
        low_y, high_y = spot == oy, spot == oy + 1.0
        wy = jnp.where(low_y, 1.0 - fy, 0.0) + jnp.where(high_y, fy, 0.0)
        sy = jnp.where(high_y, 1.0, 0.0) - jnp.where(low_y, 1.0, 0.0)

        def fold(value):
            return value[:, 0:8] + value[:, 8:16]

        plain_w, plain_s, tilt_w = fold(plain * wy), fold(plain * sy), fold(tilt * wy)
        x_sum = jnp.zeros((8, 128), F32)
        y_sum, z_sum = x_sum, x_sum
        for x in range(16):
            low_x, high_x = ox == x, ox == x - 1
            wx = jnp.where(low_x, 1.0 - fx, 0.0) + jnp.where(high_x, fx, 0.0)
            sx = jnp.where(high_x, 1.0, 0.0) - jnp.where(low_x, 1.0, 0.0)
            x_sum = x_sum + sx * plain_w[x]
            y_sum = y_sum + wx * plain_s[x]
            z_sum = z_sum + wx * tilt_w[x]
        for f, value in enumerate((x_sum, y_sum, z_sum)):
            out[owner, cyl, f, pl.ds(lax.rem(own_cell, 4), 1), :] = -charge * jnp.sum(value, axis=0, keepdims=True)

    def group(g, _):
        def later(n, _):
            cell(n)
            return 0

        lax.fori_loop(g * 8 + 2, g * 8 + 8, later, 0, unroll=2)
        return 0

    copies = []
    for g in range(4):
        cell(g * 8)
        cell(g * 8 + 1)
        if g:
            copies.append(column_copy(out, back_ref, place, send_sem, recv_sem, g - 1))
        group(g, 0)

    back_ref[place[2]] = out[place[2]]
    for copy in copies:
        copy.wait()


def field_rows(field, group, cyl):
    start = pl.multiple_of(cyl * 16, 16)
    return jnp.concatenate([field[group, pl.ds(start + 32 * x, 16), :] for x in range(16)], axis=0)


TABLE, MIXED = tables()


def constants():
    return (parts_of(TABLE), parts_of(TABLE.T)[:2], parts_of(MIXED)[:2], parts_of(MIXED.T))


def front_pass(*arrays):
    hbm = pl.BlockSpec(memory_space=pltpu.HBM)
    small = [pltpu.SMEM((2,), F32)] * 4 + [pltpu.SMEM((4, 2, 4), jnp.int32)]
    return pl.pallas_call(
        front_kernel,
        out_shape=[
            jax.ShapeDtypeStruct((6, 4, 6, 4, 128), F32),
            jax.ShapeDtypeStruct((4, 8, 8, 128), F32),
            jax.ShapeDtypeStruct((8, 4, 128), F32),
            jax.ShapeDtypeStruct((6, 4, 6, 1, 128), F32),
            jax.ShapeDtypeStruct((1024, 128), F32),
        ],
        in_specs=[hbm] * 12,
        out_specs=[VMEM_SPEC] * 5,
        scratch_shapes=small + [
            pltpu.VMEM((4, 2, 3, 4, 128), jnp.int32),
            pltpu.VMEM((4, 2, 3, 4, 128), F32),
            pltpu.VMEM((4, 2, 4, 128), jnp.int32),
            pltpu.VMEM((3, 256, 256), BF16),
            pltpu.VMEM((2, 256, 256), BF16),
            pltpu.VMEM((2, 256, 512), BF16),
            pltpu.VMEM((3, 512, 256), BF16),
            pltpu.VMEM((4, 8, 8, 128), F32),
            pltpu.VMEM((256, 512), F32),
            pltpu.VMEM((1024, 128), F32),
            pltpu.VMEM((1024, 128), F32),
            pltpu.VMEM((4, 2, 4, 1, 128), F32),
        ] + features_scratch() + [
            pltpu.VMEM((256, 128), F32),
            pltpu.VMEM((128, 128), F32),
            DMA((12,)),
            DMA((26,)), DMA((26,)), DMA((3,)), DMA((3,)), DMA((26,)), DMA((26,)), DMA((128,)), DMA((128,)),
        ],
        compiler_params=comm_params(0),
        name="front_pass",
    )(*arrays)


def sample_pass(charge, lines, atoms, table):
    return pl.pallas_call(
        sample_kernel,
        out_shape=jax.ShapeDtypeStruct((4, 2, 3, 4, 128), F32),
        in_specs=[SMEM_SPEC] + [VMEM_SPEC] * 3,
        out_specs=VMEM_SPEC,
        scratch_shapes=[pltpu.VMEM((2, 512, 384), BF16), pltpu.VMEM((4, 2, 3, 4, 128), F32), DMA((3,)), DMA((3,))],
        compiler_params=comm_params(2),
        name="sample_pass",
    )(charge, lines, atoms, table)


def on_device(cell_counts, grid_offset, fraction, species, species_density, species_pair, species_embed, species_charge):
    table, turned, mixed, mixed_turned = constants()
    order = (0, 1, 3, 2, 4)
    extended, columns, density, wide_slope, planes = front_pass(
        species_charge, species_density, species_pair, species_embed, cell_counts, grid_offset.transpose(order),
        fraction.transpose(order), species, table, turned, mixed, mixed_turned)
    lines = lax.all_to_all(planes.reshape(128, 8, 128), AXES, split_axis=0, concat_axis=0, tiled=True)
    eam, density = force_pass(cell_counts, species_density, species_pair, extended, wide_slope, density)
    electric = sample_pass(species_charge, lines.reshape(1024, 128), columns, table)
    forces = eam.reshape(4, 2, 3, 4, 128) + COUPLING * electric
    return forces.transpose(order), density.reshape(4, 2, 4, 128)


def solution(mesh):
    return jax.shard_map(
        on_device,
        mesh=mesh,
        in_specs=(
            P("gx", "gy", "gz"),
            P("gx", "gy", "gz", None, None),
            P("gx", "gy", "gz", None, None),
            P("gx", "gy", "gz", None),
            P(),
            P(),
            P(),
            P(),
        ),
        out_specs=(P("gx", "gy", "gz", None, None), P("gx", "gy", "gz", None)),
        check_vma=False,
    )
```

```python
import itertools
import math

import jax
import jax.numpy as jnp
import numpy as np
from jax import lax
from jax.experimental import pallas as pl
from jax.experimental.pallas import tpu as pltpu
from jax.sharding import PartitionSpec as P

PPC = 16
COUPLING = 8.0
F32, BF16 = jnp.float32, jnp.bfloat16
VMEM_SPEC = pl.BlockSpec(memory_space=pltpu.VMEM)
SMEM_SPEC = pl.BlockSpec(memory_space=pltpu.SMEM)


MESH = pl.DeviceIdType.MESH
AXES = ("gx", "gy", "gz")
SIZES = (4, 8, 4)
SIDES = [side for side in itertools.product((-1, 0, 1), repeat=3) if side != (0, 0, 0)]


def here():
    return [lax.axis_index(axis) for axis in AXES]


def toward(place, side):
    return tuple(lax.rem(p + s + n, n) for p, s, n in zip(place, side, SIZES))


def signal(devices):
    barrier = pltpu.get_barrier_semaphore()
    for device in devices:
        pl.semaphore_signal(barrier, inc=1, device_id=device, device_id_type=MESH)


def await_signals(count):
    pl.semaphore_wait(pltpu.get_barrier_semaphore(), count)


def send(src, dst, send_sem, recv_sem, device):
    copy = pltpu.make_async_remote_copy(
        src_ref=src, dst_ref=dst, send_sem=send_sem, recv_sem=recv_sem, device_id=device, device_id_type=MESH)
    copy.start()
    return copy


def halo_copies(own_ref, rim, ext_ref, place, send_sem, recv_sem):
    copies = []
    for n, side in enumerate(SIDES):
        src, dst = [], []
        for s, cells in zip(side, (4, 2, 4)):
            src.append(pl.ds(rim, cells) if s == 0 else pl.ds(rim + (cells - 1 if s == 1 else 0), 1))
            dst.append(pl.ds(1, cells) if s == 0 else pl.ds(0 if s == 1 else cells + 1, 1))
        copies.append(send(own_ref.at[tuple(src)], ext_ref.at[tuple(dst)], send_sem.at[n], recv_sem.at[n],
                           toward(place, side)))
    return copies


def column_copy(src_ref, dst_ref, place, send_sem, recv_sem, n):
    gx, gy, gz = place
    other = lax.rem(gz + n + 1, 4)
    return send(src_ref.at[other], dst_ref.at[gz], send_sem.at[n], recv_sem.at[n], (gx, gy, other))


def column_copies(src_ref, dst_ref, place, send_sem, recv_sem):
    return [column_copy(src_ref, dst_ref, place, send_sem, recv_sem, n) for n in range(3)]


def column_devices(place):
    gx, gy, gz = place
    return [(gx, gy, lax.rem(gz + n + 1, 4)) for n in range(3)]


DMA = pltpu.SemaphoreType.DMA


def comm_params(number):
    return pltpu.CompilerParams(collective_id=number, has_side_effects=True, vmem_limit_bytes=32 << 20)


ROWS = 16
KF = 32


def pieces(value):
    first = value.astype(BF16).astype(F32)
    rest = value - first
    second = rest.astype(BF16).astype(F32)
    third = (rest - second).astype(BF16).astype(F32)
    return first, second, third


def by_species(code, values):
    return jnp.where(code == 0.0, values[0], jnp.where(code == 1.0, values[1], 0.0))


def filled(ref, k):
    return jnp.full((8, 128), ref[k], F32)


def cube_root(value):
    guess = jnp.exp(jnp.log(value) * (1.0 / 3.0))
    return guess - (guess * guess * guess - value) / (3.0 * guess * guess)


def sublane():
    return lax.broadcasted_iota(jnp.int32, (8, 128), 0)


def assemble(blocks, ones, twos):
    rows = []
    for value, one, two in zip(blocks, ones, twos):
        first, second, third = pieces(value)
        rows.append(jnp.where(one, first, jnp.where(two, second, third)))
    return jnp.concatenate(rows, axis=0)


def patterns(first, second, last_first, last_second):
    ones, twos = [], []
    for block in range(4):
        one = two = None
        for k in range(block * 8, block * 8 + 8):
            here_one = (k % 6 in first) if k < 24 else k in last_first
            here_two = (k % 6 in second) if k < 24 else k in last_second
            if here_one:
                one = (sublane() == k % 8) if one is None else one | (sublane() == k % 8)
            if here_two:
                two = (sublane() == k % 8) if two is None else two | (sublane() == k % 8)
        ones.append(one)
        twos.append(two)
    return ones, twos


def cell_at(r):
    return lax.div(r, 24), lax.rem(lax.div(r, 6), 4), lax.rem(r, 6)


def source_features(ext_ref, slope_ref, wide, feat_b, scales, ratios):
    ones, twos = patterns((0, 2, 5), (1, 3), (24,), (25,))
    low_six, low_four, low_two, low_three = [sublane() < n for n in (6, 4, 2, 3)]

    def cell(r, _):
        def row(f):
            x, y, z = cell_at(r)
            return jnp.broadcast_to(ext_ref[x, y, z, f:f + 1, :], (8, 128))

        x = row(0) + (lax.div(r, 24) - 3).astype(F32)
        y = row(1) + (lax.rem(lax.div(r, 6), 4) - 2).astype(F32)
        z = row(2) + (lax.rem(r, 6) - 3).astype(F32)
        code = row(3)
        scale = by_species(code, scales)
        if wide is not None:
            wide[r, 0], wide[r, 1], wide[r, 2] = x, y, z
            wide[r, 3] = jnp.where(code == 1.0, ratios[1], ratios[0])
            wide[r, 4] = jnp.broadcast_to(slope_ref[cell_at(r)], (8, 128))
        square = -scale * (x * x + y * y + z * z)
        double = scale + scale
        x, y, z = double * x, double * y, double * z
        blocks = [jnp.where(low_six, scale, x), jnp.where(low_four, x, y), jnp.where(low_two, y, z),
                  jnp.where(low_three, square, 0.0)]
        feat_b[pl.ds(pl.multiple_of(r * KF, KF), KF), :] = assemble(blocks, ones, twos).astype(BF16)
        return 0

    lax.fori_loop(0, 144, cell, 0, unroll=4)


def corner(t):
    return (lax.div(t, 8) * 4 + lax.rem(lax.div(t, 4), 2)) * 6 + lax.rem(t, 4)


def target_features(ext_ref, own_t, keep, slope_ref, gains, ratios):
    ones, twos = patterns((0, 1, 4), (2, 3), (24, 25, 26, 27, 29), (28, 30))
    low_six, low_four, low_two, low_three = [sublane() < n for n in (6, 4, 2, 3)]
    low_five, low_seven = sublane() < 5, sublane() < 7

    def cell(t, _):
        r = corner(t) + 31

        def row(f):
            x, y, z = cell_at(r)
            return jnp.broadcast_to(ext_ref[x, y, z, f:f + 1, :], (8, 128))

        x = row(0) + (lax.div(t, 8) - 2).astype(F32)
        y = row(1) + (lax.rem(lax.div(t, 4), 2) - 1).astype(F32)
        z = row(2) + (lax.rem(t, 4) - 2).astype(F32)
        code = row(3)
        for n, value in enumerate((x, y, z, code)):
            keep[n, pl.ds(t, 1), :] = value[0:1]
        rest = 1.0 - (x * x + y * y + z * z)
        tail = jnp.zeros((8, 128), F32)
        if gains is not None:
            second = code == 1.0
            tilt = jnp.broadcast_to(slope_ref[cell_at(r)], (8, 128)) / jnp.where(second, ratios[1], ratios[0])
            tail = jnp.where(low_five, jnp.where(second, gains[1], gains[0]), jnp.where(low_seven, tilt, 0.0))
        blocks = [jnp.where(low_six, rest, x), jnp.where(low_four, x, y), jnp.where(low_two, y, z),
                  jnp.where(low_three, 1.0, tail)]
        own_t[t] = assemble(blocks, ones, twos).T.astype(BF16)
        return 0

    lax.fori_loop(0, 32, cell, 0, unroll=4)


def split3(value):
    first = value.astype(BF16)
    rest = value - first.astype(F32)
    second = rest.astype(BF16)
    return first, second, (rest - second.astype(F32)).astype(BF16)


def lane_sums(rows):
    ones = jnp.ones((8, rows.shape[1]), BF16)
    return lax.dot_general(ones, rows, (((1,), (1,)), ((), ())), preferred_element_type=F32)


def right_side(feat_b, cell):
    r = pl.multiple_of(cell * KF, KF)
    return jnp.concatenate([feat_b[pl.ds(r + KF * dz, KF), :] for dz in range(3)], axis=1)


def density_steps(feat_b, own_t, totals, mat):
    lanes = lax.broadcasted_iota(jnp.int32, (128, 128), 1)
    other = lanes != lax.broadcasted_iota(jnp.int32, (128, 128), 0)

    def target(t):
        cx, cy, cz = lax.div(t, 8), lax.rem(lax.div(t, 4), 2), lax.rem(t, 4)
        left = own_t[t]
        total = jnp.zeros((128, 128), F32)
        for dx in range(3):
            for dy in range(3):
                right = right_side(feat_b, ((cx + dx) * 4 + cy + dy) * 6 + cz)
                weight = jnp.dot(left, right, preferred_element_type=F32)
                weight = jnp.maximum(weight, 0.0)
                for dz in range(3):
                    part = weight[:, dz * 128:(dz + 1) * 128]
                    if dx == 1 and dy == 1 and dz == 1:
                        part = jnp.where(other, part, 0.0)
                    total = total + part * part * part
        return total

    def settle(n):
        first, second, _ = split3(totals[...])
        sums = lane_sums(jnp.concatenate([first, second], axis=1))
        mat[pl.ds(2 * n, 1), :] = sums[0:1, 0:128]
        mat[pl.ds(2 * n + 1, 1), :] = sums[0:1, 128:256]

    def both(n, _):
        settle(jnp.maximum(n - 1, 0))
        totals[0:128, :] = target(2 * n)
        totals[128:256, :] = target(2 * n + 1)
        return 0

    def run(first, last):
        lax.fori_loop(first, last, both, 0)

    return run, lambda: settle(15)


def densities(pairs, embeds, density_ref, slope_ref, keep, mat):
    code = keep[3]
    alive = by_species(code, (1.0, 1.0))
    density = mat[0:32, :] * alive
    density_ref[...] = density.reshape(8, 4, 128)
    tilts = [jnp.concatenate([3.0 * embed / (pair * pair)] * 4, axis=0) for embed, pair in zip(embeds, pairs)]
    slope_ref[...] = (by_species(code, tilts) / jnp.sqrt(1.0 + density)).reshape(4, 2, 4, 1, 128)


def force_kernel(count_hbm, amplitude_hbm, pair_hbm, ext_hbm, slope_hbm, given_hbm, electric_hbm, out_ref, density_ref,
                 count_ref, amplitude_ref, pair_ref, ext_ref, slope_ref, given_ref, electric_ref, feat_b, own_t, keep, wide,
                 near_a, near_b, part_a, part_b, mat, table, load_sem):
    loads = [
        pltpu.make_async_copy(src, dst, load_sem.at[n])
        for n, (src, dst) in enumerate((
            (amplitude_hbm, amplitude_ref), (pair_hbm, pair_ref), (ext_hbm, ext_ref), (slope_hbm, slope_ref),
            (count_hbm, count_ref), (given_hbm, given_ref), (electric_hbm, electric_ref)))
    ]
    for load in loads:
        load.start()
    part_a[...] = jnp.zeros((4, 128, 128), F32)
    part_b[...] = jnp.zeros((4, 128, 128), F32)
    for load in loads:
        load.wait()
    amplitudes, pairs = [[filled(ref, k) for k in range(2)] for ref in (amplitude_ref, pair_ref)]
    ratios = [amplitude / (pair * pair) for amplitude, pair in zip(amplitudes, pairs)]
    density_ref[...] = given_ref[...]
    gains = [-4.0 * pair / amplitude for amplitude, pair in zip(amplitudes, pairs)]
    source_features(ext_ref, slope_ref, wide, feat_b, pairs, ratios)
    target_features(ext_ref, own_t, keep, slope_ref, gains, ratios)
    feat_b[144 * KF:146 * KF, :] = jnp.concatenate([sel_matrix()[:, 0:128], sel_matrix()[:, 128:256]], axis=0)

    def fill(n, _):
        table[n] = jnp.where(n < 27, (lax.div(n, 9) * 4 + lax.rem(lax.div(n, 3), 3)) * 6 + lax.rem(n, 3),
                             jnp.where(n == 28, 145, 144))
        table[32 + n] = jnp.where(n < 27, 1, 0)
        return 0

    lax.fori_loop(0, 32, fill, 0)
    lane = lax.broadcasted_iota(jnp.int32, (ROWS, 128), 1)
    lane3 = lax.broadcasted_iota(jnp.int32, (ROWS // 8, 8, 128), 2)
    row3 = lax.broadcasted_iota(jnp.int32, (ROWS // 8, 8, 128), 0) * 8 + lax.broadcasted_iota(
        jnp.int32, (ROWS // 8, 8, 128), 1)

    def around(base, k):
        return base + (k // 9 * 4 + k // 3 % 3) * 6 + k % 3

    def multiply(t, near, part):
        left, base = own_t[t], corner(t)
        for k in range(0, 8, 2):
            right = []
            for n in (part * 8 + k, part * 8 + k + 1):
                start = pl.multiple_of((table[n] + table[32 + n] * base) * KF, KF)
                right.append(feat_b[pl.ds(start, KF), :])
            product = jnp.dot(left, jnp.concatenate(right, axis=1), preferred_element_type=F32)
            near[part * 8 + k] = product[:, 0:128]
            near[part * 8 + k + 1] = product[:, 128:256]

    def chunk(t, near, part, c):
        rows = pl.ds(pl.multiple_of(c * ROWS, ROWS), ROWS)
        base = corner(t)

        def block(k):
            return near[k, rows, :].reshape(ROWS // 8, 8, 128)

        gain, tilt = block(27), block(28)
        zero = jnp.zeros((ROWS // 8, 8, 128), F32)
        m0, mx, my, mz = zero, zero, zero, zero
        for k in range(27):
            r = around(base, k)
            w = jnp.maximum(block(k), 0.0)
            if k == 13:
                w = jnp.where(lane3 != row3 + c * ROWS, w, 0.0)
            value = ((tilt * wide[r, 3] + wide[r, 4]) * w + gain) * w
            m0 = m0 + value
            mx = mx + value * wide[r, 0]
            my = my + value * wide[r, 1]
            mz = mz + value * wide[r, 2]
        for m, value in enumerate((m0, mx, my, mz)):
            part[m, rows, :] = value.reshape(ROWS, 128)

    def settle(t, part):
        for m in (0, 2):
            first, second, third = split3(jnp.concatenate([part[m], part[m + 1]], axis=0))
            sums = lane_sums(jnp.concatenate([first, second], axis=1)) + lane_sums(third)
            mat[pl.ds(t * 4 + m, 1), :] = sums[0:1, 0:128]
            mat[pl.ds(t * 4 + m + 1, 1), :] = sums[0:1, 128:256]

    for part in range(4):
        multiply(0, near_a, part)

    def target(t, near, following, part, before):
        later = jnp.minimum(t + 1, 31)

        def rest(c, _):
            chunk(t, near, part, c)
            return 0

        settle(jnp.maximum(t - 1, 0), before)
        for n in range(4):
            multiply(later, following, n)
            chunk(t, near, part, n)
        lax.fori_loop(4, lax.div(count_ref[lax.div(t, 8), lax.rem(lax.div(t, 4), 2), lax.rem(t, 4)] + ROWS - 1, ROWS), rest, 0)

    def pair(n, _):
        target(2 * n, near_a, near_b, part_a, part_b)
        target(2 * n + 1, near_b, near_a, part_b, part_a)
        return 0

    lax.fori_loop(0, 16, pair, 0)
    settle(31, part_b)
    whole = mat[pl.ds(0, 32, stride=4), :]
    amplitude = by_species(keep[3], [jnp.concatenate([value] * 4, axis=0) for value in amplitudes])
    for m in range(3):
        value = amplitude * (mat[pl.ds(m + 1, 32, stride=4), :] - keep[m] * whole)
        out_ref[:, m] = value.reshape(8, 4, 128) + COUPLING * electric_ref[:, m]


def sel_matrix():
    row = lax.broadcasted_iota(jnp.int32, (KF, 256), 0)
    lane = lax.broadcasted_iota(jnp.int32, (KF, 256), 1)
    first = (row >= 27) & (row < 29) & (lane < 128)
    second = (row >= 29) & (row < 31) & (lane >= 128)
    return jnp.where(first | second, 1.0, 0.0).astype(BF16)


def features_scratch():
    return [pltpu.VMEM((146 * KF, 128), BF16), pltpu.VMEM((32, 128, KF), BF16), pltpu.VMEM((4, 32, 128), F32)]


def force_pass(*arrays):
    return pl.pallas_call(
        force_kernel,
        out_shape=[jax.ShapeDtypeStruct((8, 3, 4, 128), F32), jax.ShapeDtypeStruct((8, 4, 128), F32)],
        in_specs=[pl.BlockSpec(memory_space=pltpu.HBM)] * 7,
        out_specs=[VMEM_SPEC] * 2,
        scratch_shapes=[
            pltpu.SMEM((4, 2, 4), jnp.int32),
            pltpu.SMEM((2,), F32),
            pltpu.SMEM((2,), F32),
            pltpu.VMEM((6, 4, 6, 4, 128), F32),
            pltpu.VMEM((6, 4, 6, 1, 128), F32),
            pltpu.VMEM((8, 4, 128), F32),
            pltpu.VMEM((8, 3, 4, 128), F32),
        ] + features_scratch() + [
            pltpu.VMEM((144, 5, 8, 128), F32),
            pltpu.VMEM((32, 128, 128), F32),
            pltpu.VMEM((32, 128, 128), F32),
            pltpu.VMEM((4, 128, 128), F32),
            pltpu.VMEM((4, 128, 128), F32),
            pltpu.VMEM((128, 128), F32),
            pltpu.SMEM((64,), jnp.int32),
            pltpu.SemaphoreType.DMA((7,)),
        ],
        compiler_params=pltpu.CompilerParams(vmem_limit_bytes=67043328),
        cost_estimate=pl.CostEstimate(flops=20_000_000_000, bytes_accessed=1_000_000, transcendentals=0),
        name="force_pass",
    )(*arrays)


EWALD_SPLIT = 0.7


def tables():
    mode = np.arange(256)[:, None]
    point = np.arange(256)[None, :]
    cosine = np.cos(2 * np.pi * (mode * point % 256) / 256) * np.sqrt(2 / 256)
    cosine[0] /= np.sqrt(2)
    cosine[128] /= np.sqrt(2)
    sine = np.sin(2 * np.pi * ((mode - 128) * point % 256) / 256) * np.sqrt(2 / 256)
    table = np.where(mode <= 128, cosine, sine)
    row = np.arange(512)
    xr, cell, s = row // 128, row // 8 % 16, row % 8
    mixed = table[:, cell * 16 + s % 4 * 4 + xr]
    return table, mixed


def parts_of(array):
    parts = []
    for _ in range(3):
        parts.append(array.astype(np.float32).astype(jnp.bfloat16))
        array = array - parts[-1].astype(np.float64)
    return np.stack(parts)


def split(value):
    high = value.astype(BF16)
    return high, (value - high.astype(F32)).astype(BF16)


def dot(a, b):
    return jnp.dot(a, b, preferred_element_type=F32)


def dot3(a, b):
    return dot(a[0], b[0]) + (dot(a[1], b[0]) + dot(a[0], b[1]))


def dot6(a, b):
    small = dot(a[1], b[1]) + (dot(a[2], b[0]) + dot(a[0], b[2]))
    return dot(a[0], b[0]) + (dot(a[1], b[0]) + dot(a[0], b[1]) + small)


def hat(count, lower, weight):
    point = lax.broadcasted_iota(jnp.int32, (count, lower.shape[1]), 0).astype(F32)
    return jnp.where(point == lower, 1.0 - weight, 0.0) + jnp.where(point == lower + 1.0, weight, 0.0)


def spread_and_transform(atoms_ref, charges, table_ref, out_ref, rho, gz, arrivals):
    def layer(cz, _):
        source, cell = lax.div(cz, 4), lax.rem(cz, 4)

        def row(f, shift=0.0):
            first = atoms_ref[source, cell, f:f + 1, :]
            second = atoms_ref[source, cell + 4, f:f + 1, :] + shift
            return jnp.concatenate([first, second], axis=1)

        ox, oy, oz, fx, fy, fz = row(0), row(1, 16.0), row(2), row(3), row(4), row(5)
        charge = by_species(row(6), charges)
        wy = hat(32, oy, fy)
        wz = split(hat(16, oz, fz) * charge)
        parts = []
        for x in range(16):
            wx = jnp.where(ox == x, 1.0 - fx, 0.0) + jnp.where(ox == x - 1, fx, 0.0)
            parts.append(wx * wy)
        plane = split(jnp.concatenate(parts, axis=0))
        dims = (((1,), (1,)), ((), ()))

        def against(a, b):
            return lax.dot_general(a, b, dims, preferred_element_type=F32)

        value = against(wz[0], plane[0]) + (against(wz[1], plane[0]) + against(wz[0], plane[1]))
        rho[pl.ds(pl.multiple_of(cz * 16, 16), 16), :] = value
        return 0

    for n, arrival in enumerate([None] + arrivals):
        if arrival is not None:
            arrival.wait()
        start = lax.rem(gz + 4 - n, 4) * 4
        lax.fori_loop(start, start + 4, layer, 0, unroll=False)
    lines = dot3((table_ref[0], table_ref[1]), split(rho[...]))
    for plane in range(2):
        for xq in range(4):
            out_ref[pl.ds(plane * 4 + xq, 128, stride=8), :] = lines[
                plane * 128:(plane + 1) * 128, xq * 128:(xq + 1) * 128]


def device_at(d):
    return lax.div(d, 32), lax.rem(lax.div(d, 4), 8), lax.rem(d, 4)


def front_kernel(charge_hbm, amplitude_hbm, pair_hbm, embed_hbm, count_hbm, offset_hbm, fraction_hbm, species_hbm, table_hbm,
                 turned_hbm, mixed_hbm, mixed_turned_hbm, ext_ref, density_ref, wide_ref, electric_ref,
                 charge_ref, amplitude_ref, pair_ref, embed_ref, count_ref, offset_ref, fraction_ref, species_ref, table_ref,
                 turned_ref, mixed_ref, mixed_turned_ref, atoms, got_ref, rho, lines, planes, fields, back, slopes, feat_b, own_t, rows, totals, mat, field, out,
                 load_sem, halo_send, halo_recv, column_send, column_recv, slope_send, slope_recv, line_send, line_recv,
                 field_send, field_recv, return_send, return_recv):
    place = here()
    me = place[0] * 32 + place[1] * 4 + place[2]
    loads = [
        pltpu.make_async_copy(src, dst, load_sem.at[n])
        for n, (src, dst) in enumerate((
            (count_hbm, count_ref), (species_hbm, species_ref), (offset_hbm, offset_ref), (fraction_hbm, fraction_ref),
            (charge_hbm, charge_ref), (amplitude_hbm, amplitude_ref), (pair_hbm, pair_ref), (embed_hbm, embed_ref),
            (table_hbm, table_ref), (turned_hbm, turned_ref), (mixed_hbm, mixed_ref), (mixed_turned_hbm, mixed_turned_ref)))
    ]
    for load in loads:
        load.start()
    barrier = pltpu.get_barrier_semaphore()

    def greet(i, _):
        pl.semaphore_signal(barrier, inc=1, device_id=device_at(lax.rem(me + i, 128)), device_id_type=MESH)
        return 0

    lax.fori_loop(1, 128, greet, 0)
    for load in loads[:4]:
        load.wait()
    slot = lax.broadcasted_iota(jnp.int32, (1, 128), 1)

    def pack(n, _):
        x, y = lax.div(n, 2), lax.rem(n, 2)
        for z in range(4):
            code = jnp.where(slot < count_ref[x, y, z], species_ref[x, y, z:z + 1, :].astype(F32), -1.0)
            for d in range(3):
                offset, fraction = offset_ref[x, y, d, z:z + 1, :].astype(F32), fraction_ref[x, y, d, z:z + 1, :]
                ext_ref[x + 1, y + 1, z + 1, d:d + 1, :] = (offset + 0.5 + fraction) * (1.0 / PPC)
                atoms[x, y * 4 + z, d:d + 1, :] = offset
                atoms[x, y * 4 + z, d + 3:d + 4, :] = fraction
            ext_ref[x + 1, y + 1, z + 1, 3:4, :] = code
            atoms[x, y * 4 + z, 6:7, :] = code
            atoms[x, y * 4 + z, 7:8, :] = code
        return 0

    lax.fori_loop(0, 8, pack, 0)

    def keep_own(n, _):
        got_ref[place[2], n] = atoms[place[2], n]
        return 0

    lax.fori_loop(0, 8, keep_own, 0)
    for load in loads[4:]:
        load.wait()
    pl.semaphore_wait(barrier, 127)
    columns = column_copies(atoms, got_ref, place, column_send, column_recv)
    halo = halo_copies(ext_ref, 1, ext_ref, place, halo_send, halo_recv)
    charges = [charge_ref[k] for k in range(2)]
    spread_and_transform(got_ref, charges, table_ref, lines, rho, place[2], columns)
    for copy in halo:
        copy.wait()
    amplitudes, pairs, embeds = [[filled(ref, k) for k in range(2)] for ref in (amplitude_ref, pair_ref, embed_ref)]

    def exchange(src, dst, send_sem, recv_sem):
        def tile_copy(i):
            other = lax.rem(me + i, 128)
            return pltpu.make_async_remote_copy(
                src_ref=src.at[pl.ds(pl.multiple_of(other * 8, 8), 8), :],
                dst_ref=dst.at[pl.ds(pl.multiple_of(me * 8, 8), 8), :],
                send_sem=send_sem.at[i],
                recv_sem=recv_sem.at[i],
                device_id=device_at(other),
                device_id_type=MESH,
            )

        def start(i, _):
            tile_copy(i).start()
            return 0

        def finish(i, _):
            tile_copy(i).wait()
            return 0

        lax.fori_loop(1, 128, start, 0)
        mine = pl.ds(pl.multiple_of(me * 8, 8), 8)
        dst[mine, :] = src[mine, :]
        return lambda: lax.fori_loop(1, 128, finish, 0)

    target_features(ext_ref, own_t, rows, None, None, None)
    finish_lines = exchange(lines, planes, line_send, line_recv)
    source_features(ext_ref, None, None, feat_b, [cube_root(value) for value in amplitudes], None)
    run, end = density_steps(feat_b, own_t, totals, mat)
    totals[...] = jnp.zeros((256, 128), F32)
    run(0, 7)
    finish_lines()
    transform_planes(me, planes, table_ref, turned_ref, mixed_ref, mixed_turned_ref, fields)
    run(7, 8)
    finish_fields = exchange(fields, back, field_send, field_recv)
    run(8, 16)
    end()
    densities(pairs, embeds, density_ref, slopes, rows, mat)

    def keep_slope(t, _):
        x, y, z = lax.div(t, 8), lax.rem(lax.div(t, 4), 2), lax.rem(t, 4)
        wide_ref[x + 1, y + 1, z + 1] = slopes[x, y, z]
        return 0

    lax.fori_loop(0, 32, keep_slope, 0)
    halo = halo_copies(slopes, 0, wide_ref, place, slope_send, slope_recv)
    finish_fields()
    sample(place, charges, back, got_ref, table_ref, electric_ref, field, out, return_send, return_recv)
    for copy in halo:
        copy.wait()


def transform_planes(me, in_ref, table_ref, turned_ref, mixed_ref, mixed_turned_ref, out_ref):
    lane = lax.broadcasted_iota(jnp.int32, (16, 8, 128), 2)

    def pick(ref, half, g):
        starts = [(gx * 32 + (half * 4 + g) * 4) * 8 for gx in range(4)]
        return jnp.concatenate([ref[start:start + 32, :] for start in starts], axis=0).reshape(16, 8, 128)

    rows = []
    for xr in range(4):
        pair = []
        for half in range(2):
            value = jnp.zeros((16, 8, 128), F32)
            for g in range(4):
                block = pick(in_ref, half, g)
                if g != xr:
                    block = pltpu.roll(block.reshape(128, 128), (g - xr) * 32 % 128, 1).reshape(16, 8, 128)
                value = jnp.where(lax.div(lane, 32) == g, block, value)
            pair.append(value.reshape(128, 128))
        rows.append(jnp.concatenate(pair, axis=1))
    plane = jnp.concatenate(rows, axis=0)
    turned = (turned_ref[0], turned_ref[1])
    along_y = split(dot3(split(plane), turned))

    row = lax.broadcasted_iota(jnp.int32, (256, 256), 0)
    col = lax.broadcasted_iota(jnp.int32, (256, 256), 1)
    scale = 2.0 * math.pi / 256
    wave_x = jnp.where(row <= 128, row, row - 128).astype(F32) * scale
    wave_y = jnp.where(col <= 128, col, col - 128).astype(F32) * scale
    flat = wave_x * wave_x + wave_y * wave_y
    side = lax.div(lax.rem(lax.broadcasted_iota(jnp.int32, (256, 512), 1), 8), 4)
    side_turned = lax.div(lax.rem(lax.broadcasted_iota(jnp.int32, (512, 256), 0), 8), 4)
    total = None
    for p in range(2):
        mode = me if p == 0 else jnp.where(me == 0, 128, me)
        wave_z = jnp.full((256, 256), mode, jnp.int32).astype(F32) * scale
        squared = flat + wave_z * wave_z
        anchor = squared == 0.0
        green = jnp.where(anchor, 0.0, 4.0 * math.pi * jnp.exp(-squared / (4.0 * EWALD_SPLIT * EWALD_SPLIT))
                          / jnp.where(anchor, 1.0, squared))
        left = [jnp.where(side == p, mixed_ref[i].astype(F32), 0.0).astype(BF16) for i in range(2)]
        modes = split3(dot3(left, along_y) * green)
        back = [jnp.where(side_turned == p, mixed_turned_ref[i].astype(F32), 0.0).astype(BF16) for i in range(3)]
        part = dot6(back, modes)
        total = part if total is None else total + part
    field = dot6(split3(total), [table_ref[i] for i in range(3)])
    for half in range(2):
        block = [field[xr * 128:(xr + 1) * 128, half * 128:(half + 1) * 128] for xr in range(4)]
        for g in range(4):
            value = jnp.zeros((16, 8, 128), F32)
            for xr in range(4):
                moved = block[xr]
                if g != xr:
                    moved = pltpu.roll(moved, (xr - g) * 32 % 128, 1)
                value = jnp.where(lax.div(lane, 32) == xr, moved.reshape(16, 8, 128), value)
            for gx in range(4):
                start = (gx * 32 + (half * 4 + g) * 4) * 8
                out_ref[start:start + 32, :] = value[gx * 4:(gx + 1) * 4].reshape(32, 128)


def sample(place, charges, in_ref, atoms_ref, table_ref, back_ref, field, out, send_sem, recv_sem):
    columns = [
        jnp.concatenate([in_ref[pl.ds(plane * 4 + xq, 128, stride=8), :] for xq in range(4)], axis=1)
        for plane in range(2)
    ]
    modes = jnp.concatenate(columns, axis=0)
    lines = jnp.concatenate([modes[:, i * 128:(i + 1) * 128].T for i in range(4)], axis=0)
    pieces_of_field = split3(dot6(split3(lines), [table_ref[i] for i in range(3)]))
    for group in range(2):
        for i, piece in enumerate(pieces_of_field):
            field[group, :, i * 128:(i + 1) * 128] = piece[:, group * 128:(group + 1) * 128]
    point = lax.broadcasted_iota(jnp.int32, (128, 128), 0).astype(F32)

    def cell(n):
        owner = lax.rem(place[2] + 1 + lax.div(n, 8), 4)
        own_cell = lax.rem(n, 8)
        cyl, cz = lax.div(own_cell, 4), owner * 4 + lax.rem(own_cell, 4)

        def row(f):
            return atoms_ref[owner, own_cell, f:f + 1, :]

        ox, oy, oz, fx, fy, fz = [row(f) for f in range(6)]
        charge = by_species(row(6), charges)
        lower_z = oz + (lax.rem(cz, 8) * 16).astype(F32)
        lower = jnp.where(point == lower_z, 1.0, 0.0)
        slope = jnp.where(point == lower_z + 1.0, 1.0, 0.0) - lower
        right = jnp.concatenate([lower, slope], axis=1).astype(BF16)
        right = jnp.concatenate([right, right, right], axis=0)
        left = field_rows(field, lax.div(cz, 8), cyl)
        both = dot(left, right)
        tilt = both[:, 128:256].reshape(16, 16, 128)
        plain = both[:, 0:128].reshape(16, 16, 128) + fz * tilt
        spot = lax.broadcasted_iota(jnp.int32, (16, 128), 0).astype(F32)
        low_y, high_y = spot == oy, spot == oy + 1.0
        wy = jnp.where(low_y, 1.0 - fy, 0.0) + jnp.where(high_y, fy, 0.0)
        sy = jnp.where(high_y, 1.0, 0.0) - jnp.where(low_y, 1.0, 0.0)

        def fold(value):
            return value[:, 0:8] + value[:, 8:16]

        plain_w, plain_s, tilt_w = fold(plain * wy), fold(plain * sy), fold(tilt * wy)
        x_sum = jnp.zeros((8, 128), F32)
        y_sum, z_sum = x_sum, x_sum
        for x in range(16):
            low_x, high_x = ox == x, ox == x - 1
            wx = jnp.where(low_x, 1.0 - fx, 0.0) + jnp.where(high_x, fx, 0.0)
            sx = jnp.where(high_x, 1.0, 0.0) - jnp.where(low_x, 1.0, 0.0)
            x_sum = x_sum + sx * plain_w[x]
            y_sum = y_sum + wx * plain_s[x]
            z_sum = z_sum + wx * tilt_w[x]
        for f, value in enumerate((x_sum, y_sum, z_sum)):
            out[owner, cyl, f, pl.ds(lax.rem(own_cell, 4), 1), :] = -charge * jnp.sum(value, axis=0, keepdims=True)

    def group(g, _):
        def later(n, _):
            cell(n)
            return 0

        lax.fori_loop(g * 8 + 2, g * 8 + 8, later, 0, unroll=2)
        return 0

    copies = []
    for g in range(4):
        cell(g * 8)
        cell(g * 8 + 1)
        if g:
            copies.append(column_copy(out, back_ref, place, send_sem, recv_sem, g - 1))
        group(g, 0)

    back_ref[place[2]] = out[place[2]]
    for copy in copies:
        copy.wait()


def field_rows(field, group, cyl):
    start = pl.multiple_of(cyl * 16, 16)
    return jnp.concatenate([field[group, pl.ds(start + 32 * x, 16), :] for x in range(16)], axis=0)


TABLE, MIXED = tables()


def constants():
    return (parts_of(TABLE), parts_of(TABLE.T)[:2], parts_of(MIXED)[:2], parts_of(MIXED.T))


def front_pass(*arrays):
    hbm = pl.BlockSpec(memory_space=pltpu.HBM)
    small = [pltpu.SMEM((2,), F32)] * 4 + [pltpu.SMEM((4, 2, 4), jnp.int32)]
    return pl.pallas_call(
        front_kernel,
        out_shape=[
            jax.ShapeDtypeStruct((6, 4, 6, 4, 128), F32),
            jax.ShapeDtypeStruct((8, 4, 128), F32),
            jax.ShapeDtypeStruct((6, 4, 6, 1, 128), F32),
            jax.ShapeDtypeStruct((4, 2, 3, 4, 128), F32),
        ],
        in_specs=[hbm] * 12,
        out_specs=[VMEM_SPEC] * 4,
        scratch_shapes=small + [
            pltpu.VMEM((4, 2, 3, 4, 128), jnp.int32),
            pltpu.VMEM((4, 2, 3, 4, 128), F32),
            pltpu.VMEM((4, 2, 4, 128), jnp.int32),
            pltpu.VMEM((3, 256, 256), BF16),
            pltpu.VMEM((2, 256, 256), BF16),
            pltpu.VMEM((2, 256, 512), BF16),
            pltpu.VMEM((3, 512, 256), BF16),
            pltpu.VMEM((4, 8, 8, 128), F32),
            pltpu.VMEM((4, 8, 8, 128), F32),
            pltpu.VMEM((256, 512), F32),
            pltpu.VMEM((1024, 128), F32),
            pltpu.VMEM((1024, 128), F32),
            pltpu.VMEM((1024, 128), F32),
            pltpu.VMEM((1024, 128), F32),
            pltpu.VMEM((4, 2, 4, 1, 128), F32),
        ] + features_scratch() + [
            pltpu.VMEM((256, 128), F32),
            pltpu.VMEM((128, 128), F32),
            pltpu.VMEM((2, 512, 384), BF16),
            pltpu.VMEM((4, 2, 3, 4, 128), F32),
            DMA((12,)),
            DMA((26,)), DMA((26,)), DMA((3,)), DMA((3,)), DMA((26,)), DMA((26,)), DMA((128,)), DMA((128,)),
            DMA((128,)), DMA((128,)), DMA((3,)), DMA((3,)),
        ],
        compiler_params=pltpu.CompilerParams(collective_id=0, has_side_effects=True, vmem_limit_bytes=67043328),
        name="front_pass",
    )(*arrays)


def on_device(cell_counts, grid_offset, fraction, species, species_density, species_pair, species_embed, species_charge):
    table, turned, mixed, mixed_turned = constants()
    order = (0, 1, 3, 2, 4)
    extended, density, wide_slope, electric = front_pass(
        species_charge, species_density, species_pair, species_embed, cell_counts, grid_offset.transpose(order),
        fraction.transpose(order), species, table, turned, mixed, mixed_turned)
    forces, density = force_pass(
        cell_counts, species_density, species_pair, extended, wide_slope, density, electric.reshape(8, 3, 4, 128))
    return forces.reshape(4, 2, 3, 4, 128).transpose(order), density.reshape(4, 2, 4, 128)


def solution(mesh):
    return jax.shard_map(
        on_device,
        mesh=mesh,
        in_specs=(
            P("gx", "gy", "gz"),
            P("gx", "gy", "gz", None, None),
            P("gx", "gy", "gz", None, None),
            P("gx", "gy", "gz", None),
            P(),
            P(),
            P(),
            P(),
        ),
        out_specs=(P("gx", "gy", "gz", None, None), P("gx", "gy", "gz", None)),
        check_vma=False,
    )
```

```python
import itertools
import math

import jax
import jax.numpy as jnp
import numpy as np
from jax import lax
from jax.experimental import pallas as pl
from jax.experimental.pallas import tpu as pltpu
from jax.sharding import PartitionSpec as P

PPC = 16
COUPLING = 8.0
F32, BF16 = jnp.float32, jnp.bfloat16
VMEM_SPEC = pl.BlockSpec(memory_space=pltpu.VMEM)
SMEM_SPEC = pl.BlockSpec(memory_space=pltpu.SMEM)


MESH = pl.DeviceIdType.MESH
AXES = ("gx", "gy", "gz")
SIZES = (4, 8, 4)
SIDES = [side for side in itertools.product((-1, 0, 1), repeat=3) if side != (0, 0, 0)]


def here():
    return [lax.axis_index(axis) for axis in AXES]


def toward(place, side):
    return tuple(lax.rem(p + s + n, n) for p, s, n in zip(place, side, SIZES))


def send(src, dst, send_sem, recv_sem, device):
    copy = pltpu.make_async_remote_copy(
        src_ref=src, dst_ref=dst, send_sem=send_sem, recv_sem=recv_sem, device_id=device, device_id_type=MESH)
    return copy


def halo_copies(own_ref, rim, ext_ref, place, send_sem, recv_sem):
    copies = []
    for n, side in enumerate(SIDES):
        src, dst = [], []
        for s, cells in zip(side, (4, 2, 4)):
            src.append(pl.ds(rim, cells) if s == 0 else pl.ds(rim + (cells - 1 if s == 1 else 0), 1))
            dst.append(pl.ds(1, cells) if s == 0 else pl.ds(0 if s == 1 else cells + 1, 1))
        copies.append(send(own_ref.at[tuple(src)], ext_ref.at[tuple(dst)], send_sem.at[n], recv_sem.at[n],
                           toward(place, side)))
    for copy in copies:
        copy.start()
    return copies


def column_copy(src_ref, dst_ref, place, send_sem, recv_sem, n):
    gx, gy, gz = place
    other = lax.rem(gz + n + 1, 4)
    return send(src_ref.at[other], dst_ref.at[gz], send_sem.at[n], recv_sem.at[n], (gx, gy, other))


def column_copies(src_ref, dst_ref, place, send_sem, recv_sem):
    copies = [column_copy(src_ref, dst_ref, place, send_sem, recv_sem, n) for n in range(3)]
    for copy in copies:
        copy.start()
    return copies


DMA = pltpu.SemaphoreType.DMA


ROWS = 16
KF = 32


def pieces(value):
    first = value.astype(BF16).astype(F32)
    rest = value - first
    second = rest.astype(BF16).astype(F32)
    third = (rest - second).astype(BF16).astype(F32)
    return first, second, third


def by_species(code, values):
    return jnp.where(code == 0.0, values[0], jnp.where(code == 1.0, values[1], 0.0))


def filled(ref, k):
    return jnp.full((8, 128), ref[k], F32)


def cube_root(value):
    guess = jnp.exp(jnp.log(value) * (1.0 / 3.0))
    return guess - (guess * guess * guess - value) / (3.0 * guess * guess)


def sublane():
    return lax.broadcasted_iota(jnp.int32, (8, 128), 0)


def assemble(blocks, ones, twos):
    rows = []
    for value, one, two in zip(blocks, ones, twos):
        first, second, third = pieces(value)
        rows.append(jnp.where(one, first, jnp.where(two, second, third)))
    return jnp.concatenate(rows, axis=0)


def patterns(first, second, last_first, last_second):
    ones, twos = [], []
    for block in range(4):
        one = two = None
        for k in range(block * 8, block * 8 + 8):
            here_one = (k % 6 in first) if k < 24 else k in last_first
            here_two = (k % 6 in second) if k < 24 else k in last_second
            if here_one:
                one = (sublane() == k % 8) if one is None else one | (sublane() == k % 8)
            if here_two:
                two = (sublane() == k % 8) if two is None else two | (sublane() == k % 8)
        ones.append(one)
        twos.append(two)
    return ones, twos


def cell_at(r):
    return lax.div(r, 24), lax.rem(lax.div(r, 6), 4), lax.rem(r, 6)


def source_features(ext_ref, slope_ref, wide, feat_b, scales, ratios):
    ones, twos = patterns((0, 2, 5), (1, 3), (24,), (25,))
    low_six, low_four, low_two, low_three = [sublane() < n for n in (6, 4, 2, 3)]

    def cell(r, _):
        def row(f):
            x, y, z = cell_at(r)
            return jnp.broadcast_to(ext_ref[x, y, z, f:f + 1, :], (8, 128))

        x = row(0) + (lax.div(r, 24) - 3).astype(F32)
        y = row(1) + (lax.rem(lax.div(r, 6), 4) - 2).astype(F32)
        z = row(2) + (lax.rem(r, 6) - 3).astype(F32)
        code = row(3)
        scale = by_species(code, scales)
        if wide is not None:
            wide[r, 0], wide[r, 1], wide[r, 2] = x, y, z
            wide[r, 3] = jnp.where(code == 1.0, ratios[1], ratios[0])
            wide[r, 4] = jnp.broadcast_to(slope_ref[cell_at(r)], (8, 128))
        square = -scale * (x * x + y * y + z * z)
        double = scale + scale
        x, y, z = double * x, double * y, double * z
        blocks = [jnp.where(low_six, scale, x), jnp.where(low_four, x, y), jnp.where(low_two, y, z),
                  jnp.where(low_three, square, 0.0)]
        feat_b[pl.ds(pl.multiple_of(r * KF, KF), KF), :] = assemble(blocks, ones, twos).astype(BF16)
        return 0

    lax.fori_loop(0, 144, cell, 0, unroll=4)


def corner(t):
    return (lax.div(t, 8) * 4 + lax.rem(lax.div(t, 4), 2)) * 6 + lax.rem(t, 4)


def target_features(ext_ref, own_t, keep, slope_ref, gains, ratios):
    ones, twos = patterns((0, 1, 4), (2, 3), (24, 25, 26, 27, 29), (28, 30))
    low_six, low_four, low_two, low_three = [sublane() < n for n in (6, 4, 2, 3)]
    low_five, low_seven = sublane() < 5, sublane() < 7

    def cell(t, _):
        r = corner(t) + 31

        def row(f):
            x, y, z = cell_at(r)
            return jnp.broadcast_to(ext_ref[x, y, z, f:f + 1, :], (8, 128))

        x = row(0) + (lax.div(t, 8) - 2).astype(F32)
        y = row(1) + (lax.rem(lax.div(t, 4), 2) - 1).astype(F32)
        z = row(2) + (lax.rem(t, 4) - 2).astype(F32)
        code = row(3)
        for n, value in enumerate((x, y, z, code)):
            keep[n, pl.ds(t, 1), :] = value[0:1]
        rest = 1.0 - (x * x + y * y + z * z)
        tail = jnp.zeros((8, 128), F32)
        if gains is not None:
            second = code == 1.0
            tilt = jnp.broadcast_to(slope_ref[cell_at(r)], (8, 128)) / jnp.where(second, ratios[1], ratios[0])
            tail = jnp.where(low_five, jnp.where(second, gains[1], gains[0]), jnp.where(low_seven, tilt, 0.0))
        blocks = [jnp.where(low_six, rest, x), jnp.where(low_four, x, y), jnp.where(low_two, y, z),
                  jnp.where(low_three, 1.0, tail)]
        own_t[t] = assemble(blocks, ones, twos).T.astype(BF16)
        return 0

    lax.fori_loop(0, 32, cell, 0, unroll=4)


def split3(value):
    first = value.astype(BF16)
    rest = value - first.astype(F32)
    second = rest.astype(BF16)
    return first, second, (rest - second.astype(F32)).astype(BF16)


def lane_sums(rows):
    ones = jnp.ones((8, rows.shape[1]), BF16)
    return lax.dot_general(ones, rows, (((1,), (1,)), ((), ())), preferred_element_type=F32)


def right_side(feat_b, cell):
    r = pl.multiple_of(cell * KF, KF)
    return jnp.concatenate([feat_b[pl.ds(r + KF * dz, KF), :] for dz in range(3)], axis=1)


def density_steps(feat_b, own_t, totals, mat):
    lanes = lax.broadcasted_iota(jnp.int32, (128, 128), 1)
    other = lanes != lax.broadcasted_iota(jnp.int32, (128, 128), 0)

    def target(t):
        cx, cy, cz = lax.div(t, 8), lax.rem(lax.div(t, 4), 2), lax.rem(t, 4)
        left = own_t[t]
        total = jnp.zeros((128, 128), F32)
        for dx in range(3):
            for dy in range(3):
                right = right_side(feat_b, ((cx + dx) * 4 + cy + dy) * 6 + cz)
                weight = jnp.dot(left, right, preferred_element_type=F32)
                weight = jnp.maximum(weight, 0.0)
                for dz in range(3):
                    part = weight[:, dz * 128:(dz + 1) * 128]
                    if dx == 1 and dy == 1 and dz == 1:
                        part = jnp.where(other, part, 0.0)
                    total = total + part * part * part
        return total

    def settle(n):
        first, second, _ = split3(totals[...])
        sums = lane_sums(jnp.concatenate([first, second], axis=1))
        mat[pl.ds(2 * n, 1), :] = sums[0:1, 0:128]
        mat[pl.ds(2 * n + 1, 1), :] = sums[0:1, 128:256]

    def both(n, _):
        settle(jnp.maximum(n - 1, 0))
        totals[0:128, :] = target(2 * n)
        totals[128:256, :] = target(2 * n + 1)
        return 0

    def run(first, last):
        lax.fori_loop(first, last, both, 0)

    return run, lambda: settle(15)


def densities(pairs, embeds, density_ref, slope_ref, keep, mat):
    code = keep[3]
    alive = by_species(code, (1.0, 1.0))
    density = mat[0:32, :] * alive
    density_ref[...] = density.reshape(8, 4, 128)
    tilts = [jnp.concatenate([3.0 * embed / (pair * pair)] * 4, axis=0) for embed, pair in zip(embeds, pairs)]
    slope_ref[...] = (by_species(code, tilts) / jnp.sqrt(1.0 + density)).reshape(4, 2, 4, 1, 128)


def force_kernel(count_hbm, amplitude_hbm, pair_hbm, ext_hbm, slope_hbm, given_hbm, electric_hbm, out_ref, density_ref,
                 count_ref, amplitude_ref, pair_ref, ext_ref, slope_ref, given_ref, electric_ref, feat_b, own_t, keep, wide,
                 near_a, near_b, part_a, part_b, mat, table, load_sem):
    loads = [
        pltpu.make_async_copy(src, dst, load_sem.at[n])
        for n, (src, dst) in enumerate((
            (amplitude_hbm, amplitude_ref), (pair_hbm, pair_ref), (ext_hbm, ext_ref), (slope_hbm, slope_ref),
            (count_hbm, count_ref), (given_hbm, given_ref), (electric_hbm, electric_ref)))
    ]
    for load in loads:
        load.start()
    part_a[...] = jnp.zeros((4, 128, 128), F32)
    part_b[...] = jnp.zeros((4, 128, 128), F32)
    for load in loads:
        load.wait()
    amplitudes, pairs = [[filled(ref, k) for k in range(2)] for ref in (amplitude_ref, pair_ref)]
    ratios = [amplitude / (pair * pair) for amplitude, pair in zip(amplitudes, pairs)]
    density_ref[...] = given_ref[...]
    gains = [-4.0 * pair / amplitude for amplitude, pair in zip(amplitudes, pairs)]
    source_features(ext_ref, slope_ref, wide, feat_b, pairs, ratios)
    target_features(ext_ref, own_t, keep, slope_ref, gains, ratios)
    feat_b[144 * KF:146 * KF, :] = jnp.concatenate([sel_matrix()[:, 0:128], sel_matrix()[:, 128:256]], axis=0)

    def fill(n, _):
        table[n] = jnp.where(n < 27, (lax.div(n, 9) * 4 + lax.rem(lax.div(n, 3), 3)) * 6 + lax.rem(n, 3),
                             jnp.where(n == 28, 145, 144))
        table[32 + n] = jnp.where(n < 27, 1, 0)
        return 0

    lax.fori_loop(0, 32, fill, 0)
    lane = lax.broadcasted_iota(jnp.int32, (ROWS, 128), 1)
    lane3 = lax.broadcasted_iota(jnp.int32, (ROWS // 8, 8, 128), 2)
    row3 = lax.broadcasted_iota(jnp.int32, (ROWS // 8, 8, 128), 0) * 8 + lax.broadcasted_iota(
        jnp.int32, (ROWS // 8, 8, 128), 1)

    def around(base, k):
        return base + (k // 9 * 4 + k // 3 % 3) * 6 + k % 3

    def multiply(t, near, part):
        left, base = own_t[t], corner(t)
        for k in range(0, 8, 2):
            right = []
            for n in (part * 8 + k, part * 8 + k + 1):
                start = pl.multiple_of((table[n] + table[32 + n] * base) * KF, KF)
                right.append(feat_b[pl.ds(start, KF), :])
            product = jnp.dot(left, jnp.concatenate(right, axis=1), preferred_element_type=F32)
            near[part * 8 + k] = product[:, 0:128]
            near[part * 8 + k + 1] = product[:, 128:256]

    def chunk(t, near, part, c):
        rows = pl.ds(pl.multiple_of(c * ROWS, ROWS), ROWS)
        base = corner(t)

        def block(k):
            return near[k, rows, :].reshape(ROWS // 8, 8, 128)

        gain, tilt = block(27), block(28)
        zero = jnp.zeros((ROWS // 8, 8, 128), F32)
        m0, mx, my, mz = zero, zero, zero, zero
        for k in range(27):
            r = around(base, k)
            w = jnp.maximum(block(k), 0.0)
            if k == 13:
                w = jnp.where(lane3 != row3 + c * ROWS, w, 0.0)
            value = ((tilt * wide[r, 3] + wide[r, 4]) * w + gain) * w
            m0 = m0 + value
            mx = mx + value * wide[r, 0]
            my = my + value * wide[r, 1]
            mz = mz + value * wide[r, 2]
        for m, value in enumerate((m0, mx, my, mz)):
            part[m, rows, :] = value.reshape(ROWS, 128)

    def settle(t, part):
        for m in (0, 2):
            first, second, third = split3(jnp.concatenate([part[m], part[m + 1]], axis=0))
            sums = lane_sums(jnp.concatenate([first, second], axis=1)) + lane_sums(third)
            mat[pl.ds(t * 4 + m, 1), :] = sums[0:1, 0:128]
            mat[pl.ds(t * 4 + m + 1, 1), :] = sums[0:1, 128:256]

    for part in range(4):
        multiply(0, near_a, part)

    def target(t, near, following, part, before):
        later = jnp.minimum(t + 1, 31)

        def rest(c, _):
            chunk(t, near, part, c)
            return 0

        settle(jnp.maximum(t - 1, 0), before)
        for n in range(4):
            multiply(later, following, n)
            chunk(t, near, part, n)
        lax.fori_loop(4, lax.div(count_ref[lax.div(t, 8), lax.rem(lax.div(t, 4), 2), lax.rem(t, 4)] + ROWS - 1, ROWS), rest, 0)

    def pair(n, _):
        target(2 * n, near_a, near_b, part_a, part_b)
        target(2 * n + 1, near_b, near_a, part_b, part_a)
        return 0

    lax.fori_loop(0, 16, pair, 0)
    settle(31, part_b)
    whole = mat[pl.ds(0, 32, stride=4), :]
    amplitude = by_species(keep[3], [jnp.concatenate([value] * 4, axis=0) for value in amplitudes])
    for m in range(3):
        value = amplitude * (mat[pl.ds(m + 1, 32, stride=4), :] - keep[m] * whole)
        out_ref[:, m] = value.reshape(8, 4, 128) + COUPLING * electric_ref[:, m]


def sel_matrix():
    row = lax.broadcasted_iota(jnp.int32, (KF, 256), 0)
    lane = lax.broadcasted_iota(jnp.int32, (KF, 256), 1)
    first = (row >= 27) & (row < 29) & (lane < 128)
    second = (row >= 29) & (row < 31) & (lane >= 128)
    return jnp.where(first | second, 1.0, 0.0).astype(BF16)


def features_scratch():
    return [pltpu.VMEM((146 * KF, 128), BF16), pltpu.VMEM((32, 128, KF), BF16), pltpu.VMEM((4, 32, 128), F32)]


def force_pass(*arrays):
    return pl.pallas_call(
        force_kernel,
        out_shape=[jax.ShapeDtypeStruct((8, 3, 4, 128), F32), jax.ShapeDtypeStruct((8, 4, 128), F32)],
        in_specs=[pl.BlockSpec(memory_space=pltpu.HBM)] * 7,
        out_specs=[VMEM_SPEC] * 2,
        scratch_shapes=[
            pltpu.SMEM((4, 2, 4), jnp.int32),
            pltpu.SMEM((2,), F32),
            pltpu.SMEM((2,), F32),
            pltpu.VMEM((6, 4, 6, 4, 128), F32),
            pltpu.VMEM((6, 4, 6, 1, 128), F32),
            pltpu.VMEM((8, 4, 128), F32),
            pltpu.VMEM((8, 3, 4, 128), F32),
        ] + features_scratch() + [
            pltpu.VMEM((144, 5, 8, 128), F32),
            pltpu.VMEM((32, 128, 128), F32),
            pltpu.VMEM((32, 128, 128), F32),
            pltpu.VMEM((4, 128, 128), F32),
            pltpu.VMEM((4, 128, 128), F32),
            pltpu.VMEM((128, 128), F32),
            pltpu.SMEM((64,), jnp.int32),
            pltpu.SemaphoreType.DMA((7,)),
        ],
        compiler_params=pltpu.CompilerParams(vmem_limit_bytes=67043328),
        cost_estimate=pl.CostEstimate(flops=20_000_000_000, bytes_accessed=1_000_000, transcendentals=0),
        name="force_pass",
    )(*arrays)


EWALD_SPLIT = 0.7


def tables():
    mode = np.arange(256)[:, None]
    point = np.arange(256)[None, :]
    cosine = np.cos(2 * np.pi * (mode * point % 256) / 256) * np.sqrt(2 / 256)
    cosine[0] /= np.sqrt(2)
    cosine[128] /= np.sqrt(2)
    sine = np.sin(2 * np.pi * ((mode - 128) * point % 256) / 256) * np.sqrt(2 / 256)
    table = np.where(mode <= 128, cosine, sine)
    row = np.arange(512)
    xr, cell, s = row // 128, row // 8 % 16, row % 8
    mixed = table[:, cell * 16 + s % 4 * 4 + xr]
    return table, mixed


def parts_of(array):
    parts = []
    for _ in range(3):
        parts.append(array.astype(np.float32).astype(jnp.bfloat16))
        array = array - parts[-1].astype(np.float64)
    return np.stack(parts)


def split(value):
    high = value.astype(BF16)
    return high, (value - high.astype(F32)).astype(BF16)


def dot(a, b):
    return jnp.dot(a, b, preferred_element_type=F32)


def dot3(a, b):
    return dot(a[0], b[0]) + (dot(a[1], b[0]) + dot(a[0], b[1]))


def dot6(a, b):
    small = dot(a[1], b[1]) + (dot(a[2], b[0]) + dot(a[0], b[2]))
    return dot(a[0], b[0]) + (dot(a[1], b[0]) + dot(a[0], b[1]) + small)


def hat(count, lower, weight):
    point = lax.broadcasted_iota(jnp.int32, (count, lower.shape[1]), 0).astype(F32)
    return jnp.where(point == lower, 1.0 - weight, 0.0) + jnp.where(point == lower + 1.0, weight, 0.0)


def spread_and_transform(atoms_ref, charges, table_ref, out_ref, rho, gz, arrivals):
    def layer(cz, _):
        source, cell = lax.div(cz, 4), lax.rem(cz, 4)

        def row(f, shift=0.0):
            first = atoms_ref[source, cell, f:f + 1, :]
            second = atoms_ref[source, cell + 4, f:f + 1, :] + shift
            return jnp.concatenate([first, second], axis=1)

        ox, oy, oz, fx, fy, fz = row(0), row(1, 16.0), row(2), row(3), row(4), row(5)
        charge = by_species(row(6), charges)
        wy = hat(32, oy, fy)
        wz = split(hat(16, oz, fz) * charge)
        parts = []
        for x in range(16):
            wx = jnp.where(ox == x, 1.0 - fx, 0.0) + jnp.where(ox == x - 1, fx, 0.0)
            parts.append(wx * wy)
        plane = split(jnp.concatenate(parts, axis=0))
        dims = (((1,), (1,)), ((), ()))

        def against(a, b):
            return lax.dot_general(a, b, dims, preferred_element_type=F32)

        value = against(wz[0], plane[0]) + (against(wz[1], plane[0]) + against(wz[0], plane[1]))
        rho[pl.ds(pl.multiple_of(cz * 16, 16), 16), :] = value
        return 0

    for n, arrival in enumerate([None] + arrivals):
        if arrival is not None:
            arrival.wait()
        start = lax.rem(gz + 4 - n, 4) * 4
        lax.fori_loop(start, start + 4, layer, 0, unroll=False)
    lines = dot3((table_ref[0], table_ref[1]), split(rho[...]))
    for plane in range(2):
        for xq in range(4):
            out_ref[pl.ds(plane * 4 + xq, 128, stride=8), :] = lines[
                plane * 128:(plane + 1) * 128, xq * 128:(xq + 1) * 128]


def front_kernel(charge_hbm, amplitude_hbm, pair_hbm, embed_hbm, count_hbm, offset_hbm, fraction_hbm, species_hbm, table_hbm,
                 turned_hbm, mixed_hbm, mixed_turned_hbm, ext_ref, density_ref, wide_ref, electric_ref,
                 charge_ref, amplitude_ref, pair_ref, embed_ref, count_ref, offset_ref, fraction_ref, species_ref, table_ref,
                 turned_ref, mixed_ref, mixed_turned_ref, atoms, got_ref, rho, lines, planes, fields, back, slopes, feat_b, own_t, rows, totals, mat, field, out,
                 load_sem, halo_send, halo_recv, column_send, column_recv, slope_send, slope_recv, line_send, line_recv,
                 field_send, field_recv, return_send, return_recv):
    place = here()
    me = place[0] * 32 + place[1] * 4 + place[2]
    loads = [
        pltpu.make_async_copy(src, dst, load_sem.at[n])
        for n, (src, dst) in enumerate((
            (count_hbm, count_ref), (species_hbm, species_ref), (offset_hbm, offset_ref), (fraction_hbm, fraction_ref),
            (charge_hbm, charge_ref), (amplitude_hbm, amplitude_ref), (pair_hbm, pair_ref), (embed_hbm, embed_ref),
            (table_hbm, table_ref), (turned_hbm, turned_ref), (mixed_hbm, mixed_ref), (mixed_turned_hbm, mixed_turned_ref)))
    ]
    for load in loads:
        load.start()
    barrier = pltpu.get_barrier_semaphore()

    def greet(other, _):
        pl.semaphore_signal(barrier, inc=1, device_id=other, device_id_type=pl.DeviceIdType.LOGICAL)
        return 0

    lax.fori_loop(me + 1, 128, greet, 0)
    lax.fori_loop(0, me, greet, 0)
    for load in loads[:4]:
        load.wait()
    slot = lax.broadcasted_iota(jnp.int32, (1, 128), 1)

    def pack(n, _):
        x, y = lax.div(n, 2), lax.rem(n, 2)
        for z in range(4):
            code = jnp.where(slot < count_ref[x, y, z], species_ref[x, y, z:z + 1, :].astype(F32), -1.0)
            for d in range(3):
                offset, fraction = offset_ref[x, y, d, z:z + 1, :].astype(F32), fraction_ref[x, y, d, z:z + 1, :]
                ext_ref[x + 1, y + 1, z + 1, d:d + 1, :] = (offset + 0.5 + fraction) * (1.0 / PPC)
                atoms[x, y * 4 + z, d:d + 1, :] = offset
                atoms[x, y * 4 + z, d + 3:d + 4, :] = fraction
            ext_ref[x + 1, y + 1, z + 1, 3:4, :] = code
            atoms[x, y * 4 + z, 6:7, :] = code
            atoms[x, y * 4 + z, 7:8, :] = code
        return 0

    lax.fori_loop(0, 8, pack, 0)

    def keep_own(n, _):
        got_ref[place[2], n] = atoms[place[2], n]
        return 0

    lax.fori_loop(0, 8, keep_own, 0)
    for load in loads[4:]:
        load.wait()
    pl.semaphore_wait(barrier, 127)
    columns = column_copies(atoms, got_ref, place, column_send, column_recv)
    halo = halo_copies(ext_ref, 1, ext_ref, place, halo_send, halo_recv)
    charges = [charge_ref[k] for k in range(2)]
    spread_and_transform(got_ref, charges, table_ref, lines, rho, place[2], columns)
    for copy in halo:
        copy.wait()
    amplitudes, pairs, embeds = [[filled(ref, k) for k in range(2)] for ref in (amplitude_ref, pair_ref, embed_ref)]

    def exchange(src, dst, send_sem, recv_sem):
        mine = pl.ds(pl.multiple_of(me * 8, 8), 8)

        def start(other, _):
            pltpu.make_async_remote_copy(
                src_ref=src.at[pl.ds(pl.multiple_of(other * 8, 8), 8), :],
                dst_ref=dst.at[mine, :],
                send_sem=send_sem.at[0],
                recv_sem=recv_sem.at[0],
                device_id=other,
                device_id_type=pl.DeviceIdType.LOGICAL,
            ).start()
            return 0

        lax.fori_loop(me + 1, 128, start, 0)
        lax.fori_loop(0, me, start, 0)
        dst[mine, :] = src[mine, :]

        def finish():
            pltpu.make_async_copy(src.at[0:1016, :], dst.at[0:1016, :], recv_sem.at[0]).wait()
            pltpu.make_async_copy(src.at[0:1016, :], dst.at[0:1016, :], send_sem.at[0]).wait()

        return finish

    target_features(ext_ref, own_t, rows, None, None, None)
    finish_lines = exchange(lines, planes, line_send, line_recv)
    source_features(ext_ref, None, None, feat_b, [cube_root(value) for value in amplitudes], None)
    run, end = density_steps(feat_b, own_t, totals, mat)
    totals[...] = jnp.zeros((256, 128), F32)
    run(0, 7)
    finish_lines()
    transform_planes(me, planes, table_ref, turned_ref, mixed_ref, mixed_turned_ref, fields)
    run(7, 8)
    finish_fields = exchange(fields, back, field_send, field_recv)
    run(8, 16)
    end()
    densities(pairs, embeds, density_ref, slopes, rows, mat)

    def keep_slope(t, _):
        x, y, z = lax.div(t, 8), lax.rem(lax.div(t, 4), 2), lax.rem(t, 4)
        wide_ref[x + 1, y + 1, z + 1] = slopes[x, y, z]
        return 0

    lax.fori_loop(0, 32, keep_slope, 0)
    halo = halo_copies(slopes, 0, wide_ref, place, slope_send, slope_recv)
    finish_fields()
    sample(place, charges, back, got_ref, table_ref, electric_ref, field, out, return_send, return_recv)
    for copy in halo:
        copy.wait()


def transform_planes(me, in_ref, table_ref, turned_ref, mixed_ref, mixed_turned_ref, out_ref):
    lane = lax.broadcasted_iota(jnp.int32, (16, 8, 128), 2)

    def pick(ref, half, g):
        starts = [(gx * 32 + (half * 4 + g) * 4) * 8 for gx in range(4)]
        return jnp.concatenate([ref[start:start + 32, :] for start in starts], axis=0).reshape(16, 8, 128)

    rows = []
    for xr in range(4):
        pair = []
        for half in range(2):
            value = jnp.zeros((16, 8, 128), F32)
            for g in range(4):
                block = pick(in_ref, half, g)
                if g != xr:
                    block = pltpu.roll(block.reshape(128, 128), (g - xr) * 32 % 128, 1).reshape(16, 8, 128)
                value = jnp.where(lax.div(lane, 32) == g, block, value)
            pair.append(value.reshape(128, 128))
        rows.append(jnp.concatenate(pair, axis=1))
    plane = jnp.concatenate(rows, axis=0)
    turned = (turned_ref[0], turned_ref[1])
    along_y = dot3(split(plane), turned)

    row = lax.broadcasted_iota(jnp.int32, (256, 256), 0)
    col = lax.broadcasted_iota(jnp.int32, (256, 256), 1)
    scale = 2.0 * math.pi / 256
    wave_x = jnp.where(row <= 128, row, row - 128).astype(F32) * scale
    wave_y = jnp.where(col <= 128, col, col - 128).astype(F32) * scale
    flat = wave_x * wave_x + wave_y * wave_y
    side = lax.div(lax.rem(lax.broadcasted_iota(jnp.int32, (512, 256), 0), 8), 4)
    total = None
    for p in range(2):
        mode = me if p == 0 else jnp.where(me == 0, 128, me)
        wave_z = jnp.full((256, 256), mode, jnp.int32).astype(F32) * scale
        squared = flat + wave_z * wave_z
        anchor = squared == 0.0
        green = jnp.where(anchor, 0.0, 4.0 * math.pi * jnp.exp(-squared / (4.0 * EWALD_SPLIT * EWALD_SPLIT))
                          / jnp.where(anchor, 1.0, squared))
        modes = split3(dot3((mixed_ref[0], mixed_ref[1]), split(jnp.where(side == p, along_y, 0.0))) * green)
        part = dot6([mixed_turned_ref[i] for i in range(3)], modes)
        total = part if total is None else jnp.where(side == 0, total, part)
    field = dot6(split3(total), [table_ref[i] for i in range(3)])
    for half in range(2):
        block = [field[xr * 128:(xr + 1) * 128, half * 128:(half + 1) * 128] for xr in range(4)]
        for g in range(4):
            value = jnp.zeros((16, 8, 128), F32)
            for xr in range(4):
                moved = block[xr]
                if g != xr:
                    moved = pltpu.roll(moved, (xr - g) * 32 % 128, 1)
                value = jnp.where(lax.div(lane, 32) == xr, moved.reshape(16, 8, 128), value)
            for gx in range(4):
                start = (gx * 32 + (half * 4 + g) * 4) * 8
                out_ref[start:start + 32, :] = value[gx * 4:(gx + 1) * 4].reshape(32, 128)


def sample(place, charges, in_ref, atoms_ref, table_ref, back_ref, field, out, send_sem, recv_sem):
    columns = [
        jnp.concatenate([in_ref[pl.ds(plane * 4 + xq, 128, stride=8), :] for xq in range(4)], axis=1)
        for plane in range(2)
    ]
    modes = jnp.concatenate(columns, axis=0)
    lines = jnp.concatenate([modes[:, i * 128:(i + 1) * 128].T for i in range(4)], axis=0)
    pieces_of_field = split3(dot6(split3(lines), [table_ref[i] for i in range(3)]))
    for group in range(2):
        for i, piece in enumerate(pieces_of_field):
            field[group, :, i * 128:(i + 1) * 128] = piece[:, group * 128:(group + 1) * 128]
    point = lax.broadcasted_iota(jnp.int32, (128, 128), 0).astype(F32)

    def cell(n):
        owner = lax.rem(place[2] + 1 + lax.div(n, 8), 4)
        own_cell = lax.rem(n, 8)
        cyl, cz = lax.div(own_cell, 4), owner * 4 + lax.rem(own_cell, 4)

        def row(f):
            return atoms_ref[owner, own_cell, f:f + 1, :]

        ox, oy, oz, fx, fy, fz = [row(f) for f in range(6)]
        charge = by_species(row(6), charges)
        lower_z = oz + (lax.rem(cz, 8) * 16).astype(F32)
        lower = jnp.where(point == lower_z, 1.0, 0.0)
        slope = jnp.where(point == lower_z + 1.0, 1.0, 0.0) - lower
        right = jnp.concatenate([lower, slope], axis=1).astype(BF16)
        right = jnp.concatenate([right, right, right], axis=0)
        left = field_rows(field, lax.div(cz, 8), cyl)
        both = dot(left, right)
        tilt = both[:, 128:256].reshape(16, 16, 128)
        plain = both[:, 0:128].reshape(16, 16, 128) + fz * tilt
        spot = lax.broadcasted_iota(jnp.int32, (16, 128), 0).astype(F32)
        low_y, high_y = spot == oy, spot == oy + 1.0
        wy = jnp.where(low_y, 1.0 - fy, 0.0) + jnp.where(high_y, fy, 0.0)
        sy = jnp.where(high_y, 1.0, 0.0) - jnp.where(low_y, 1.0, 0.0)

        def fold(value):
            return value[:, 0:8] + value[:, 8:16]

        plain_w, plain_s, tilt_w = fold(plain * wy), fold(plain * sy), fold(tilt * wy)
        x_sum = jnp.zeros((8, 128), F32)
        y_sum, z_sum = x_sum, x_sum
        for x in range(16):
            low_x, high_x = ox == x, ox == x - 1
            wx = jnp.where(low_x, 1.0 - fx, 0.0) + jnp.where(high_x, fx, 0.0)
            sx = jnp.where(high_x, 1.0, 0.0) - jnp.where(low_x, 1.0, 0.0)
            x_sum = x_sum + sx * plain_w[x]
            y_sum = y_sum + wx * plain_s[x]
            z_sum = z_sum + wx * tilt_w[x]
        for f, value in enumerate((x_sum, y_sum, z_sum)):
            out[owner, cyl, f, pl.ds(lax.rem(own_cell, 4), 1), :] = -charge * jnp.sum(value, axis=0, keepdims=True)

    def group(g, _):
        for n in range(2):
            cell(g * 8 + n)

        @pl.when(g > 0)
        def _():
            column_copy(out, back_ref, place, send_sem, recv_sem, g - 1).start()

        for n in range(2, 8):
            cell(g * 8 + n)
        return 0

    lax.fori_loop(0, 4, group, 0)
    copies = [column_copy(out, back_ref, place, send_sem, recv_sem, n) for n in range(3)]
    back_ref[place[2]] = out[place[2]]
    for copy in copies:
        copy.wait()


def field_rows(field, group, cyl):
    start = pl.multiple_of(cyl * 16, 16)
    return jnp.concatenate([field[group, pl.ds(start + 32 * x, 16), :] for x in range(16)], axis=0)


TABLE, MIXED = tables()


def constants():
    return (parts_of(TABLE), parts_of(TABLE.T)[:2], parts_of(MIXED)[:2], parts_of(MIXED.T))


def front_pass(*arrays):
    hbm = pl.BlockSpec(memory_space=pltpu.HBM)
    small = [pltpu.SMEM((2,), F32)] * 4 + [pltpu.SMEM((4, 2, 4), jnp.int32)]
    return pl.pallas_call(
        front_kernel,
        out_shape=[
            jax.ShapeDtypeStruct((6, 4, 6, 4, 128), F32),
            jax.ShapeDtypeStruct((8, 4, 128), F32),
            jax.ShapeDtypeStruct((6, 4, 6, 1, 128), F32),
            jax.ShapeDtypeStruct((4, 2, 3, 4, 128), F32),
        ],
        in_specs=[hbm] * 12,
        out_specs=[VMEM_SPEC] * 4,
        scratch_shapes=small + [
            pltpu.VMEM((4, 2, 3, 4, 128), jnp.int32),
            pltpu.VMEM((4, 2, 3, 4, 128), F32),
            pltpu.VMEM((4, 2, 4, 128), jnp.int32),
            pltpu.VMEM((3, 256, 256), BF16),
            pltpu.VMEM((2, 256, 256), BF16),
            pltpu.VMEM((2, 256, 512), BF16),
            pltpu.VMEM((3, 512, 256), BF16),
            pltpu.VMEM((4, 8, 8, 128), F32),
            pltpu.VMEM((4, 8, 8, 128), F32),
            pltpu.VMEM((256, 512), F32),
            pltpu.VMEM((1024, 128), F32),
            pltpu.VMEM((1024, 128), F32),
            pltpu.VMEM((1024, 128), F32),
            pltpu.VMEM((1024, 128), F32),
            pltpu.VMEM((4, 2, 4, 1, 128), F32),
        ] + features_scratch() + [
            pltpu.VMEM((256, 128), F32),
            pltpu.VMEM((128, 128), F32),
            pltpu.VMEM((2, 512, 384), BF16),
            pltpu.VMEM((4, 2, 3, 4, 128), F32),
            DMA((12,)),
            DMA((26,)), DMA((26,)), DMA((3,)), DMA((3,)), DMA((26,)), DMA((26,)), DMA((1,)), DMA((1,)),
            DMA((1,)), DMA((1,)), DMA((3,)), DMA((3,)),
        ],
        compiler_params=pltpu.CompilerParams(collective_id=0, has_side_effects=True, vmem_limit_bytes=67043328),
        name="front_pass",
    )(*arrays)


def on_device(cell_counts, grid_offset, fraction, species, species_density, species_pair, species_embed, species_charge):
    table, turned, mixed, mixed_turned = constants()
    order = (0, 1, 3, 2, 4)
    extended, density, wide_slope, electric = front_pass(
        species_charge, species_density, species_pair, species_embed, cell_counts, grid_offset.transpose(order),
        fraction.transpose(order), species, table, turned, mixed, mixed_turned)
    forces, density = force_pass(
        cell_counts, species_density, species_pair, extended, wide_slope, density, electric.reshape(8, 3, 4, 128))
    return forces.reshape(4, 2, 3, 4, 128).transpose(order), density.reshape(4, 2, 4, 128)


def solution(mesh):
    return jax.shard_map(
        on_device,
        mesh=mesh,
        in_specs=(
            P("gx", "gy", "gz"),
            P("gx", "gy", "gz", None, None),
            P("gx", "gy", "gz", None, None),
            P("gx", "gy", "gz", None),
            P(),
            P(),
            P(),
            P(),
        ),
        out_specs=(P("gx", "gy", "gz", None, None), P("gx", "gy", "gz", None)),
        check_vma=False,
    )
```

```python
import itertools
import math

import jax
import jax.numpy as jnp
import numpy as np
from jax import lax
from jax.experimental import pallas as pl
from jax.experimental.pallas import tpu as pltpu
from jax.sharding import PartitionSpec as P

PPC = 16
COUPLING = 8.0
F32, BF16 = jnp.float32, jnp.bfloat16
VMEM_SPEC = pl.BlockSpec(memory_space=pltpu.VMEM)
SMEM_SPEC = pl.BlockSpec(memory_space=pltpu.SMEM)


MESH = pl.DeviceIdType.MESH
AXES = ("gx", "gy", "gz")
SIZES = (4, 8, 4)
SIDES = [side for side in itertools.product((-1, 0, 1), repeat=3) if side != (0, 0, 0)]


def here():
    return [lax.axis_index(axis) for axis in AXES]


def toward(place, side):
    return tuple(lax.rem(p + s + n, n) for p, s, n in zip(place, side, SIZES))


def send(src, dst, send_sem, recv_sem, device):
    copy = pltpu.make_async_remote_copy(
        src_ref=src, dst_ref=dst, send_sem=send_sem, recv_sem=recv_sem, device_id=device, device_id_type=MESH)
    return copy


def halo_copies(own_ref, rim, ext_ref, place, send_sem, recv_sem):
    copies = []
    for n, side in enumerate(SIDES):
        src, dst = [], []
        for s, cells in zip(side, (4, 2, 4)):
            src.append(pl.ds(rim, cells) if s == 0 else pl.ds(rim + (cells - 1 if s == 1 else 0), 1))
            dst.append(pl.ds(1, cells) if s == 0 else pl.ds(0 if s == 1 else cells + 1, 1))
        copies.append(send(own_ref.at[tuple(src)], ext_ref.at[tuple(dst)], send_sem.at[n], recv_sem.at[n],
                           toward(place, side)))
    for copy in copies:
        copy.start()
    return copies


def column_copy(src_ref, dst_ref, place, send_sem, recv_sem, n):
    gx, gy, gz = place
    other = lax.rem(gz + n + 1, 4)
    return send(src_ref.at[other], dst_ref.at[gz], send_sem.at[n], recv_sem.at[n], (gx, gy, other))


def column_copies(src_ref, dst_ref, place, send_sem, recv_sem):
    copies = [column_copy(src_ref, dst_ref, place, send_sem, recv_sem, n) for n in range(3)]
    for copy in copies:
        copy.start()
    return copies


DMA = pltpu.SemaphoreType.DMA


ROWS = 16
KF = 32


def pieces(value):
    first = value.astype(BF16).astype(F32)
    rest = value - first
    second = rest.astype(BF16).astype(F32)
    third = (rest - second).astype(BF16).astype(F32)
    return first, second, third


def by_species(code, values):
    return jnp.where(code == 0.0, values[0], jnp.where(code == 1.0, values[1], 0.0))


def filled(ref, k):
    return jnp.full((8, 128), ref[k], F32)


def cube_root(value):
    guess = jnp.exp(jnp.log(value) * (1.0 / 3.0))
    return guess - (guess * guess * guess - value) / (3.0 * guess * guess)


def sublane():
    return lax.broadcasted_iota(jnp.int32, (8, 128), 0)


def assemble(blocks, ones, twos):
    rows = []
    for value, one, two in zip(blocks, ones, twos):
        first, second, third = pieces(value)
        rows.append(jnp.where(one, first, jnp.where(two, second, third)))
    return jnp.concatenate(rows, axis=0)


def patterns(first, second, last_first, last_second):
    ones, twos = [], []
    for block in range(4):
        one = two = None
        for k in range(block * 8, block * 8 + 8):
            here_one = (k % 6 in first) if k < 24 else k in last_first
            here_two = (k % 6 in second) if k < 24 else k in last_second
            if here_one:
                one = (sublane() == k % 8) if one is None else one | (sublane() == k % 8)
            if here_two:
                two = (sublane() == k % 8) if two is None else two | (sublane() == k % 8)
        ones.append(one)
        twos.append(two)
    return ones, twos


def cell_at(r):
    return lax.div(r, 24), lax.rem(lax.div(r, 6), 4), lax.rem(r, 6)


def source_features(ext_ref, feat_b, scales, first, last):
    ones, twos = patterns((0, 2, 5), (1, 3), (24,), (25,))
    low_six, low_four, low_two, low_three = [sublane() < n for n in (6, 4, 2, 3)]

    def cell(r, _):
        def row(f):
            x, y, z = cell_at(r)
            return jnp.broadcast_to(ext_ref[x, y, z, f:f + 1, :], (8, 128))

        x = row(0) + (lax.div(r, 24) - 3).astype(F32)
        y = row(1) + (lax.rem(lax.div(r, 6), 4) - 2).astype(F32)
        z = row(2) + (lax.rem(r, 6) - 3).astype(F32)
        code = row(3)
        scale = by_species(code, scales)
        square = -scale * (x * x + y * y + z * z)
        double = scale + scale
        x, y, z = double * x, double * y, double * z
        blocks = [jnp.where(low_six, scale, x), jnp.where(low_four, x, y), jnp.where(low_two, y, z),
                  jnp.where(low_three, square, 0.0)]
        feat_b[pl.ds(pl.multiple_of(r * KF, KF), KF), :] = assemble(blocks, ones, twos).astype(BF16)
        return 0

    def four(n, _):
        for i in range(4):
            cell(n * 4 + i, 0)
        return 0

    lax.fori_loop(first // 4, last // 4, four, 0)


def fill_wide(ext_ref, slope_ref, wide, ratios):
    def cell(r, _):
        place = cell_at(r)

        def row(f):
            return jnp.broadcast_to(ext_ref[place + (slice(f, f + 1), slice(None))], (8, 128))

        wide[r, 0] = row(0) + (place[0] - 3).astype(F32)
        wide[r, 1] = row(1) + (place[1] - 2).astype(F32)
        wide[r, 2] = row(2) + (place[2] - 3).astype(F32)
        wide[r, 3] = jnp.where(row(3) == 1.0, ratios[1], ratios[0])
        wide[r, 4] = jnp.broadcast_to(slope_ref[place], (8, 128))
        return 0

    lax.fori_loop(0, 144, cell, 0, unroll=4)


def corner(t):
    return (lax.div(t, 8) * 4 + lax.rem(lax.div(t, 4), 2)) * 6 + lax.rem(t, 4)


def target_features(ext_ref, own_t, keep, slope_ref, gains, ratios):
    ones, twos = patterns((0, 1, 4), (2, 3), (24, 25, 26, 27, 29), (28, 30))
    low_six, low_four, low_two, low_three = [sublane() < n for n in (6, 4, 2, 3)]
    low_five, low_seven = sublane() < 5, sublane() < 7

    def cell(t, _):
        r = corner(t) + 31

        def row(f):
            x, y, z = cell_at(r)
            return jnp.broadcast_to(ext_ref[x, y, z, f:f + 1, :], (8, 128))

        x = row(0) + (lax.div(t, 8) - 2).astype(F32)
        y = row(1) + (lax.rem(lax.div(t, 4), 2) - 1).astype(F32)
        z = row(2) + (lax.rem(t, 4) - 2).astype(F32)
        code = row(3)
        for n, value in enumerate((x, y, z, code)):
            keep[n, pl.ds(t, 1), :] = value[0:1]
        rest = 1.0 - (x * x + y * y + z * z)
        tail = jnp.zeros((8, 128), F32)
        if gains is not None:
            second = code == 1.0
            tilt = jnp.broadcast_to(slope_ref[cell_at(r)], (8, 128)) / jnp.where(second, ratios[1], ratios[0])
            tail = jnp.where(low_five, jnp.where(second, gains[1], gains[0]), jnp.where(low_seven, tilt, 0.0))
        blocks = [jnp.where(low_six, rest, x), jnp.where(low_four, x, y), jnp.where(low_two, y, z),
                  jnp.where(low_three, 1.0, tail)]
        own_t[t] = assemble(blocks, ones, twos).T.astype(BF16)
        return 0

    lax.fori_loop(0, 32, cell, 0, unroll=4)


def split3(value):
    first = value.astype(BF16)
    rest = value - first.astype(F32)
    second = rest.astype(BF16)
    return first, second, (rest - second.astype(F32)).astype(BF16)


def lane_sums(rows):
    ones = jnp.ones((8, rows.shape[1]), BF16)
    return lax.dot_general(ones, rows, (((1,), (1,)), ((), ())), preferred_element_type=F32)


def right_side(feat_b, cell):
    r = pl.multiple_of(cell * KF, KF)
    return jnp.concatenate([feat_b[pl.ds(r + KF * dz, KF), :] for dz in range(3)], axis=1)


def density_steps(feat_b, own_t, totals, mat):
    lanes = lax.broadcasted_iota(jnp.int32, (128, 128), 1)
    other = lanes != lax.broadcasted_iota(jnp.int32, (128, 128), 0)

    def target(t):
        cx, cy, cz = lax.div(t, 8), lax.rem(lax.div(t, 4), 2), lax.rem(t, 4)
        left = own_t[t]
        total = jnp.zeros((128, 128), F32)
        for dx in range(3):
            for dy in range(3):
                right = right_side(feat_b, ((cx + dx) * 4 + cy + dy) * 6 + cz)
                weight = jnp.dot(left, right, preferred_element_type=F32)
                weight = jnp.maximum(weight, 0.0)
                for dz in range(3):
                    part = weight[:, dz * 128:(dz + 1) * 128]
                    if dx == 1 and dy == 1 and dz == 1:
                        part = jnp.where(other, part, 0.0)
                    total = total + part * part * part
        return total

    def settle(n):
        first, second, _ = split3(totals[...])
        sums = lane_sums(jnp.concatenate([first, second], axis=1))
        mat[pl.ds(2 * n, 1), :] = sums[0:1, 0:128]
        mat[pl.ds(2 * n + 1, 1), :] = sums[0:1, 128:256]

    def both(n, _):
        settle(jnp.maximum(n - 1, 0))
        totals[0:128, :] = target(2 * n)
        totals[128:256, :] = target(2 * n + 1)
        return 0

    def run(first, last):
        lax.fori_loop(first, last, both, 0)

    return run, lambda: settle(15)


def densities(pairs, embeds, density_ref, slope_ref, keep, mat):
    code = keep[3]
    alive = by_species(code, (1.0, 1.0))
    density = mat[0:32, :] * alive
    density_ref[...] = density.reshape(8, 4, 128)
    tilts = [jnp.concatenate([3.0 * embed / (pair * pair)] * 4, axis=0) for embed, pair in zip(embeds, pairs)]
    slope_ref[...] = (by_species(code, tilts) / jnp.sqrt(1.0 + density)).reshape(4, 2, 4, 1, 128)


def force_kernel(count_hbm, amplitude_hbm, pair_hbm, ext_hbm, slope_hbm, given_hbm, electric_hbm, feat_hbm, out_ref, density_ref,
                 count_ref, amplitude_ref, pair_ref, ext_ref, slope_ref, given_ref, electric_ref, feat_b, own_t, keep, wide,
                 near_a, near_b, part_a, part_b, mat, table, load_sem):
    loads = [
        pltpu.make_async_copy(src, dst, load_sem.at[n])
        for n, (src, dst) in enumerate((
            (amplitude_hbm, amplitude_ref), (pair_hbm, pair_ref), (ext_hbm, ext_ref), (slope_hbm, slope_ref),
            (count_hbm, count_ref), (given_hbm, given_ref), (electric_hbm, electric_ref),
            (feat_hbm, feat_b.at[0:144 * KF, :])))
    ]
    for load in loads:
        load.start()
    part_a[...] = jnp.zeros((4, 128, 128), F32)
    part_b[...] = jnp.zeros((4, 128, 128), F32)
    for load in loads[:4]:
        load.wait()
    amplitudes, pairs = [[filled(ref, k) for k in range(2)] for ref in (amplitude_ref, pair_ref)]
    ratios = [amplitude / (pair * pair) for amplitude, pair in zip(amplitudes, pairs)]
    gains = [-4.0 * pair / amplitude for amplitude, pair in zip(amplitudes, pairs)]
    fill_wide(ext_ref, slope_ref, wide, ratios)
    target_features(ext_ref, own_t, keep, slope_ref, gains, ratios)
    feat_b[144 * KF:146 * KF, :] = jnp.concatenate([sel_matrix()[:, 0:128], sel_matrix()[:, 128:256]], axis=0)

    def fill(n, _):
        table[n] = jnp.where(n < 27, (lax.div(n, 9) * 4 + lax.rem(lax.div(n, 3), 3)) * 6 + lax.rem(n, 3),
                             jnp.where(n == 28, 145, 144))
        table[32 + n] = jnp.where(n < 27, 1, 0)
        return 0

    lax.fori_loop(0, 32, fill, 0)
    lane = lax.broadcasted_iota(jnp.int32, (ROWS, 128), 1)
    lane3 = lax.broadcasted_iota(jnp.int32, (ROWS // 8, 8, 128), 2)
    row3 = lax.broadcasted_iota(jnp.int32, (ROWS // 8, 8, 128), 0) * 8 + lax.broadcasted_iota(
        jnp.int32, (ROWS // 8, 8, 128), 1)

    def around(base, k):
        return base + (k // 9 * 4 + k // 3 % 3) * 6 + k % 3

    def multiply(t, near, part):
        left, base = own_t[t], corner(t)
        for k in range(0, 8, 2):
            right = []
            for n in (part * 8 + k, part * 8 + k + 1):
                start = pl.multiple_of((table[n] + table[32 + n] * base) * KF, KF)
                right.append(feat_b[pl.ds(start, KF), :])
            product = jnp.dot(left, jnp.concatenate(right, axis=1), preferred_element_type=F32)
            near[part * 8 + k] = product[:, 0:128]
            near[part * 8 + k + 1] = product[:, 128:256]

    def chunk(t, near, part, c):
        rows = pl.ds(pl.multiple_of(c * ROWS, ROWS), ROWS)
        base = corner(t)

        def block(k):
            return near[k, rows, :].reshape(ROWS // 8, 8, 128)

        gain, tilt = block(27), block(28)
        zero = jnp.zeros((ROWS // 8, 8, 128), F32)
        m0, mx, my, mz = zero, zero, zero, zero
        for k in range(27):
            r = around(base, k)
            w = jnp.maximum(block(k), 0.0)
            if k == 13:
                w = jnp.where(lane3 != row3 + c * ROWS, w, 0.0)
            value = ((tilt * wide[r, 3] + wide[r, 4]) * w + gain) * w
            m0 = m0 + value
            mx = mx + value * wide[r, 0]
            my = my + value * wide[r, 1]
            mz = mz + value * wide[r, 2]
        for m, value in enumerate((m0, mx, my, mz)):
            part[m, rows, :] = value.reshape(ROWS, 128)

    def settle(t, part):
        for m in (0, 2):
            first, second, third = split3(jnp.concatenate([part[m], part[m + 1]], axis=0))
            sums = lane_sums(jnp.concatenate([first, second], axis=1)) + lane_sums(third)
            mat[pl.ds(t * 4 + m, 1), :] = sums[0:1, 0:128]
            mat[pl.ds(t * 4 + m + 1, 1), :] = sums[0:1, 128:256]

    for load in loads[4:]:
        load.wait()
    density_ref[...] = given_ref[...]
    for part in range(4):
        multiply(0, near_a, part)

    def target(t, near, following, part, before):
        later = jnp.minimum(t + 1, 31)

        def rest(c, _):
            chunk(t, near, part, c)
            return 0

        settle(jnp.maximum(t - 1, 0), before)
        for n in range(4):
            multiply(later, following, n)
            chunk(t, near, part, n)
        lax.fori_loop(4, lax.div(count_ref[lax.div(t, 8), lax.rem(lax.div(t, 4), 2), lax.rem(t, 4)] + ROWS - 1, ROWS), rest, 0)

    def pair(n, _):
        target(2 * n, near_a, near_b, part_a, part_b)
        target(2 * n + 1, near_b, near_a, part_b, part_a)
        return 0

    lax.fori_loop(0, 16, pair, 0)
    settle(31, part_b)
    whole = mat[pl.ds(0, 32, stride=4), :]
    amplitude = by_species(keep[3], [jnp.concatenate([value] * 4, axis=0) for value in amplitudes])
    for m in range(3):
        value = amplitude * (mat[pl.ds(m + 1, 32, stride=4), :] - keep[m] * whole)
        out_ref[:, m] = value.reshape(8, 4, 128) + COUPLING * electric_ref[:, m]


def sel_matrix():
    row = lax.broadcasted_iota(jnp.int32, (KF, 256), 0)
    lane = lax.broadcasted_iota(jnp.int32, (KF, 256), 1)
    first = (row >= 27) & (row < 29) & (lane < 128)
    second = (row >= 29) & (row < 31) & (lane >= 128)
    return jnp.where(first | second, 1.0, 0.0).astype(BF16)


def features_scratch():
    return [pltpu.VMEM((146 * KF, 128), BF16), pltpu.VMEM((32, 128, KF), BF16), pltpu.VMEM((4, 32, 128), F32)]


def force_pass(*arrays):
    return pl.pallas_call(
        force_kernel,
        out_shape=[jax.ShapeDtypeStruct((8, 3, 4, 128), F32), jax.ShapeDtypeStruct((8, 4, 128), F32)],
        in_specs=[pl.BlockSpec(memory_space=pltpu.HBM)] * 8,
        out_specs=[VMEM_SPEC] * 2,
        scratch_shapes=[
            pltpu.SMEM((4, 2, 4), jnp.int32),
            pltpu.SMEM((2,), F32),
            pltpu.SMEM((2,), F32),
            pltpu.VMEM((6, 4, 6, 4, 128), F32),
            pltpu.VMEM((6, 4, 6, 1, 128), F32),
            pltpu.VMEM((8, 4, 128), F32),
            pltpu.VMEM((8, 3, 4, 128), F32),
        ] + features_scratch() + [
            pltpu.VMEM((144, 5, 8, 128), F32),
            pltpu.VMEM((32, 128, 128), F32),
            pltpu.VMEM((32, 128, 128), F32),
            pltpu.VMEM((4, 128, 128), F32),
            pltpu.VMEM((4, 128, 128), F32),
            pltpu.VMEM((128, 128), F32),
            pltpu.SMEM((64,), jnp.int32),
            pltpu.SemaphoreType.DMA((8,)),
        ],
        compiler_params=pltpu.CompilerParams(vmem_limit_bytes=67043328),
        cost_estimate=pl.CostEstimate(flops=20_000_000_000, bytes_accessed=1_000_000, transcendentals=0),
        name="force_pass",
    )(*arrays)


EWALD_SPLIT = 0.7


def tables():
    mode = np.arange(256)[:, None]
    point = np.arange(256)[None, :]
    cosine = np.cos(2 * np.pi * (mode * point % 256) / 256) * np.sqrt(2 / 256)
    cosine[0] /= np.sqrt(2)
    cosine[128] /= np.sqrt(2)
    sine = np.sin(2 * np.pi * ((mode - 128) * point % 256) / 256) * np.sqrt(2 / 256)
    table = np.where(mode <= 128, cosine, sine)
    row = np.arange(512)
    xr, cell, s = row // 128, row // 8 % 16, row % 8
    mixed = table[:, cell * 16 + s % 4 * 4 + xr]
    return table, mixed


def parts_of(array):
    parts = []
    for _ in range(3):
        parts.append(array.astype(np.float32).astype(jnp.bfloat16))
        array = array - parts[-1].astype(np.float64)
    return np.stack(parts)


def split(value):
    high = value.astype(BF16)
    return high, (value - high.astype(F32)).astype(BF16)


def dot(a, b):
    return jnp.dot(a, b, preferred_element_type=F32)


def dot3(a, b):
    return dot(a[0], b[0]) + (dot(a[1], b[0]) + dot(a[0], b[1]))


def dot6(a, b):
    small = dot(a[1], b[1]) + (dot(a[2], b[0]) + dot(a[0], b[2]))
    return dot(a[0], b[0]) + (dot(a[1], b[0]) + dot(a[0], b[1]) + small)


def hat(count, lower, weight):
    point = lax.broadcasted_iota(jnp.int32, (count, lower.shape[1]), 0).astype(F32)
    return jnp.where(point == lower, 1.0 - weight, 0.0) + jnp.where(point == lower + 1.0, weight, 0.0)


def spread_and_transform(atoms_ref, charges, table_ref, out_ref, rho, gz, arrivals):
    def layer(cz, _):
        source, cell = lax.div(cz, 4), lax.rem(cz, 4)

        def row(f, shift=0.0):
            first = atoms_ref[source, cell, f:f + 1, :]
            second = atoms_ref[source, cell + 4, f:f + 1, :] + shift
            return jnp.concatenate([first, second], axis=1)

        ox, oy, oz, fx, fy, fz = row(0), row(1, 16.0), row(2), row(3), row(4), row(5)
        charge = by_species(row(6), charges)
        wy = hat(32, oy, fy)
        wz = split(hat(16, oz, fz) * charge)
        parts = []
        for x in range(16):
            wx = jnp.where(ox == x, 1.0 - fx, 0.0) + jnp.where(ox == x - 1, fx, 0.0)
            parts.append(wx * wy)
        plane = split(jnp.concatenate(parts, axis=0))
        dims = (((1,), (1,)), ((), ()))

        def against(a, b):
            return lax.dot_general(a, b, dims, preferred_element_type=F32)

        value = against(wz[0], plane[0]) + (against(wz[1], plane[0]) + against(wz[0], plane[1]))
        rho[pl.ds(pl.multiple_of(cz * 16, 16), 16), :] = value
        return 0

    for n, arrival in enumerate([None] + arrivals):
        if arrival is not None:
            arrival.wait()
        start = lax.rem(gz + 4 - n, 4) * 4
        lax.fori_loop(start, start + 4, layer, 0, unroll=False)
    lines = dot3((table_ref[0], table_ref[1]), split(rho[...]))
    for plane in range(2):
        for xq in range(4):
            out_ref[pl.ds(plane * 4 + xq, 128, stride=8), :] = lines[
                plane * 128:(plane + 1) * 128, xq * 128:(xq + 1) * 128]


def front_kernel(charge_hbm, amplitude_hbm, pair_hbm, embed_hbm, count_hbm, offset_hbm, fraction_hbm, species_hbm, table_hbm,
                 turned_hbm, mixed_hbm, mixed_turned_hbm, ext_ref, density_ref, wide_ref, electric_ref, feat_hbm,
                 charge_ref, amplitude_ref, pair_ref, embed_ref, count_ref, offset_ref, fraction_ref, species_ref, table_ref,
                 turned_ref, mixed_ref, mixed_turned_ref, atoms, got_ref, rho, lines, planes, fields, back, slopes, feat_b, own_t, rows, feat_c, totals, mat, field, out,
                 load_sem, halo_send, halo_recv, column_send, column_recv, slope_send, slope_recv, line_send, line_recv,
                 field_send, field_recv, return_send, return_recv, feat_sem):
    place = here()
    me = place[0] * 32 + place[1] * 4 + place[2]
    loads = [
        pltpu.make_async_copy(src, dst, load_sem.at[n])
        for n, (src, dst) in enumerate((
            (count_hbm, count_ref), (species_hbm, species_ref), (offset_hbm, offset_ref), (fraction_hbm, fraction_ref),
            (charge_hbm, charge_ref), (amplitude_hbm, amplitude_ref), (pair_hbm, pair_ref), (embed_hbm, embed_ref),
            (table_hbm, table_ref), (turned_hbm, turned_ref), (mixed_hbm, mixed_ref), (mixed_turned_hbm, mixed_turned_ref)))
    ]
    for load in loads:
        load.start()
    barrier = pltpu.get_barrier_semaphore()

    def greet(other, _):
        pl.semaphore_signal(barrier, inc=1, device_id=other, device_id_type=pl.DeviceIdType.LOGICAL)
        return 0

    lax.fori_loop(me + 1, 128, greet, 0)
    lax.fori_loop(0, me, greet, 0)
    for load in loads[:4]:
        load.wait()
    slot = lax.broadcasted_iota(jnp.int32, (1, 128), 1)

    def pack(n, _):
        x, y = lax.div(n, 2), lax.rem(n, 2)
        for z in range(4):
            code = jnp.where(slot < count_ref[x, y, z], species_ref[x, y, z:z + 1, :].astype(F32), -1.0)
            for d in range(3):
                offset, fraction = offset_ref[x, y, d, z:z + 1, :].astype(F32), fraction_ref[x, y, d, z:z + 1, :]
                ext_ref[x + 1, y + 1, z + 1, d:d + 1, :] = (offset + 0.5 + fraction) * (1.0 / PPC)
                atoms[x, y * 4 + z, d:d + 1, :] = offset
                atoms[x, y * 4 + z, d + 3:d + 4, :] = fraction
            ext_ref[x + 1, y + 1, z + 1, 3:4, :] = code
            atoms[x, y * 4 + z, 6:7, :] = code
            atoms[x, y * 4 + z, 7:8, :] = code
        return 0

    lax.fori_loop(0, 8, pack, 0)

    def keep_own(n, _):
        got_ref[place[2], n] = atoms[place[2], n]
        return 0

    lax.fori_loop(0, 8, keep_own, 0)
    target_features(ext_ref, own_t, rows, None, None, None)
    for load in loads[4:]:
        load.wait()
    pl.semaphore_wait(barrier, 127)
    columns = column_copies(atoms, got_ref, place, column_send, column_recv)
    halo = halo_copies(ext_ref, 1, ext_ref, place, halo_send, halo_recv)
    charges = [charge_ref[k] for k in range(2)]
    spread_and_transform(got_ref, charges, table_ref, lines, rho, place[2], columns)
    for copy in halo:
        copy.wait()
    amplitudes, pairs, embeds = [[filled(ref, k) for k in range(2)] for ref in (amplitude_ref, pair_ref, embed_ref)]

    def exchange(src, dst, send_sem, recv_sem):
        mine = pl.ds(pl.multiple_of(me * 8, 8), 8)

        def start(other, _):
            pltpu.make_async_remote_copy(
                src_ref=src.at[pl.ds(pl.multiple_of(other * 8, 8), 8), :],
                dst_ref=dst.at[mine, :],
                send_sem=send_sem.at[0],
                recv_sem=recv_sem.at[0],
                device_id=other,
                device_id_type=pl.DeviceIdType.LOGICAL,
            ).start()
            return 0

        lax.fori_loop(me + 1, 128, start, 0)
        lax.fori_loop(0, me, start, 0)
        dst[mine, :] = src[mine, :]

        def finish():
            pltpu.make_async_copy(src.at[0:1016, :], dst.at[0:1016, :], recv_sem.at[0]).wait()
            pltpu.make_async_copy(src.at[0:1016, :], dst.at[0:1016, :], send_sem.at[0]).wait()

        return finish

    roots = [cube_root(value) for value in amplitudes]
    source_features(ext_ref, feat_b, roots, 0, 24)
    finish_lines = exchange(lines, planes, line_send, line_recv)
    source_features(ext_ref, feat_b, roots, 24, 144)
    run, end = density_steps(feat_b, own_t, totals, mat)
    totals[...] = jnp.zeros((256, 128), F32)
    run(0, 8)
    finish_lines()
    transform_planes(me, planes, table_ref, turned_ref, mixed_ref, mixed_turned_ref, fields)
    run(8, 9)
    finish_fields = exchange(fields, back, field_send, field_recv)
    run(9, 16)
    end()
    densities(pairs, embeds, density_ref, slopes, rows, mat)

    def keep_slope(t, _):
        x, y, z = lax.div(t, 8), lax.rem(lax.div(t, 4), 2), lax.rem(t, 4)
        wide_ref[x + 1, y + 1, z + 1] = slopes[x, y, z]
        return 0

    lax.fori_loop(0, 32, keep_slope, 0)
    halo = halo_copies(slopes, 0, wide_ref, place, slope_send, slope_recv)
    source_features(ext_ref, feat_c, pairs, 0, 144)
    finish_fields()
    feat_copy = pltpu.make_async_copy(feat_c, feat_hbm, feat_sem.at[0])
    feat_copy.start()
    sample(place, charges, back, got_ref, table_ref, electric_ref, field, out, return_send, return_recv)
    for copy in halo:
        copy.wait()
    feat_copy.wait()


def transform_planes(me, in_ref, table_ref, turned_ref, mixed_ref, mixed_turned_ref, out_ref):
    lane = lax.broadcasted_iota(jnp.int32, (16, 8, 128), 2)

    def pick(ref, half, g):
        starts = [(gx * 32 + (half * 4 + g) * 4) * 8 for gx in range(4)]
        return jnp.concatenate([ref[start:start + 32, :] for start in starts], axis=0).reshape(16, 8, 128)

    rows = []
    for xr in range(4):
        pair = []
        for half in range(2):
            value = jnp.zeros((16, 8, 128), F32)
            for g in range(4):
                block = pick(in_ref, half, g)
                if g != xr:
                    block = pltpu.roll(block.reshape(128, 128), (g - xr) * 32 % 128, 1).reshape(16, 8, 128)
                value = jnp.where(lax.div(lane, 32) == g, block, value)
            pair.append(value.reshape(128, 128))
        rows.append(jnp.concatenate(pair, axis=1))
    plane = jnp.concatenate(rows, axis=0)
    turned = (turned_ref[0], turned_ref[1])
    along_y = dot3(split(plane), turned)

    row = lax.broadcasted_iota(jnp.int32, (256, 256), 0)
    col = lax.broadcasted_iota(jnp.int32, (256, 256), 1)
    scale = 2.0 * math.pi / 256
    wave_x = jnp.where(row <= 128, row, row - 128).astype(F32) * scale
    wave_y = jnp.where(col <= 128, col, col - 128).astype(F32) * scale
    flat = wave_x * wave_x + wave_y * wave_y
    side = lax.div(lax.rem(lax.broadcasted_iota(jnp.int32, (512, 256), 0), 8), 4)
    total = None
    for p in range(2):
        mode = me if p == 0 else jnp.where(me == 0, 128, me)
        wave_z = jnp.full((256, 256), mode, jnp.int32).astype(F32) * scale
        squared = flat + wave_z * wave_z
        anchor = squared == 0.0
        green = jnp.where(anchor, 0.0, 4.0 * math.pi * jnp.exp(-squared / (4.0 * EWALD_SPLIT * EWALD_SPLIT))
                          / jnp.where(anchor, 1.0, squared))
        modes = split3(dot3((mixed_ref[0], mixed_ref[1]), split(jnp.where(side == p, along_y, 0.0))) * green)
        part = dot6([mixed_turned_ref[i] for i in range(3)], modes)
        total = part if total is None else jnp.where(side == 0, total, part)
    field = dot6(split3(total), [table_ref[i] for i in range(3)])
    for half in range(2):
        block = [field[xr * 128:(xr + 1) * 128, half * 128:(half + 1) * 128] for xr in range(4)]
        for g in range(4):
            value = jnp.zeros((16, 8, 128), F32)
            for xr in range(4):
                moved = block[xr]
                if g != xr:
                    moved = pltpu.roll(moved, (xr - g) * 32 % 128, 1)
                value = jnp.where(lax.div(lane, 32) == xr, moved.reshape(16, 8, 128), value)
            for gx in range(4):
                start = (gx * 32 + (half * 4 + g) * 4) * 8
                out_ref[start:start + 32, :] = value[gx * 4:(gx + 1) * 4].reshape(32, 128)


def sample(place, charges, in_ref, atoms_ref, table_ref, back_ref, field, out, send_sem, recv_sem):
    columns = [
        jnp.concatenate([in_ref[pl.ds(plane * 4 + xq, 128, stride=8), :] for xq in range(4)], axis=1)
        for plane in range(2)
    ]
    modes = jnp.concatenate(columns, axis=0)
    lines = jnp.concatenate([modes[:, i * 128:(i + 1) * 128].T for i in range(4)], axis=0)
    pieces_of_field = split3(dot6(split3(lines), [table_ref[i] for i in range(3)]))
    for group in range(2):
        for i, piece in enumerate(pieces_of_field):
            field[group, :, i * 128:(i + 1) * 128] = piece[:, group * 128:(group + 1) * 128]
    point = lax.broadcasted_iota(jnp.int32, (128, 128), 0).astype(F32)

    def cell(n):
        owner = lax.rem(place[2] + 1 + lax.div(n, 8), 4)
        own_cell = lax.rem(n, 8)
        cyl, cz = lax.div(own_cell, 4), owner * 4 + lax.rem(own_cell, 4)

        def row(f):
            return atoms_ref[owner, own_cell, f:f + 1, :]

        ox, oy, oz, fx, fy, fz = [row(f) for f in range(6)]
        charge = by_species(row(6), charges)
        lower_z = oz + (lax.rem(cz, 8) * 16).astype(F32)
        lower = jnp.where(point == lower_z, 1.0, 0.0)
        slope = jnp.where(point == lower_z + 1.0, 1.0, 0.0) - lower
        right = jnp.concatenate([lower, slope], axis=1).astype(BF16)
        right = jnp.concatenate([right, right, right], axis=0)
        left = field_rows(field, lax.div(cz, 8), cyl)
        both = dot(left, right)
        tilt = both[:, 128:256].reshape(16, 16, 128)
        plain = both[:, 0:128].reshape(16, 16, 128) + fz * tilt
        spot = lax.broadcasted_iota(jnp.int32, (16, 128), 0).astype(F32)
        low_y, high_y = spot == oy, spot == oy + 1.0
        wy = jnp.where(low_y, 1.0 - fy, 0.0) + jnp.where(high_y, fy, 0.0)
        sy = jnp.where(high_y, 1.0, 0.0) - jnp.where(low_y, 1.0, 0.0)

        def fold(value):
            return value[:, 0:8] + value[:, 8:16]

        plain_w, plain_s, tilt_w = fold(plain * wy), fold(plain * sy), fold(tilt * wy)
        x_sum = jnp.zeros((8, 128), F32)
        y_sum, z_sum = x_sum, x_sum
        for x in range(16):
            low_x, high_x = ox == x, ox == x - 1
            wx = jnp.where(low_x, 1.0 - fx, 0.0) + jnp.where(high_x, fx, 0.0)
            sx = jnp.where(high_x, 1.0, 0.0) - jnp.where(low_x, 1.0, 0.0)
            x_sum = x_sum + sx * plain_w[x]
            y_sum = y_sum + wx * plain_s[x]
            z_sum = z_sum + wx * tilt_w[x]
        for f, value in enumerate((x_sum, y_sum, z_sum)):
            out[owner, cyl, f, pl.ds(lax.rem(own_cell, 4), 1), :] = -charge * jnp.sum(value, axis=0, keepdims=True)

    def group(g, _):
        for n in range(2):
            cell(g * 8 + n)

        @pl.when(g > 0)
        def _():
            column_copy(out, back_ref, place, send_sem, recv_sem, g - 1).start()

        for n in range(2, 8):
            cell(g * 8 + n)
        return 0

    lax.fori_loop(0, 4, group, 0)
    copies = [column_copy(out, back_ref, place, send_sem, recv_sem, n) for n in range(3)]
    back_ref[place[2]] = out[place[2]]
    for copy in copies:
        copy.wait()


def field_rows(field, group, cyl):
    start = pl.multiple_of(cyl * 16, 16)
    return jnp.concatenate([field[group, pl.ds(start + 32 * x, 16), :] for x in range(16)], axis=0)


TABLE, MIXED = tables()


def constants():
    return (parts_of(TABLE), parts_of(TABLE.T)[:2], parts_of(MIXED)[:2], parts_of(MIXED.T))


def front_pass(*arrays):
    hbm = pl.BlockSpec(memory_space=pltpu.HBM)
    small = [pltpu.SMEM((2,), F32)] * 4 + [pltpu.SMEM((4, 2, 4), jnp.int32)]
    return pl.pallas_call(
        front_kernel,
        out_shape=[
            jax.ShapeDtypeStruct((6, 4, 6, 4, 128), F32),
            jax.ShapeDtypeStruct((8, 4, 128), F32),
            jax.ShapeDtypeStruct((6, 4, 6, 1, 128), F32),
            jax.ShapeDtypeStruct((4, 2, 3, 4, 128), F32),
            jax.ShapeDtypeStruct((144 * KF, 128), BF16),
        ],
        in_specs=[hbm] * 12,
        out_specs=[VMEM_SPEC] * 4 + [hbm],
        scratch_shapes=small + [
            pltpu.VMEM((4, 2, 3, 4, 128), jnp.int32),
            pltpu.VMEM((4, 2, 3, 4, 128), F32),
            pltpu.VMEM((4, 2, 4, 128), jnp.int32),
            pltpu.VMEM((3, 256, 256), BF16),
            pltpu.VMEM((2, 256, 256), BF16),
            pltpu.VMEM((2, 256, 512), BF16),
            pltpu.VMEM((3, 512, 256), BF16),
            pltpu.VMEM((4, 8, 8, 128), F32),
            pltpu.VMEM((4, 8, 8, 128), F32),
            pltpu.VMEM((256, 512), F32),
            pltpu.VMEM((1024, 128), F32),
            pltpu.VMEM((1024, 128), F32),
            pltpu.VMEM((1024, 128), F32),
            pltpu.VMEM((1024, 128), F32),
            pltpu.VMEM((4, 2, 4, 1, 128), F32),
        ] + features_scratch() + [
            pltpu.VMEM((144 * KF, 128), BF16),
            pltpu.VMEM((256, 128), F32),
            pltpu.VMEM((128, 128), F32),
            pltpu.VMEM((2, 512, 384), BF16),
            pltpu.VMEM((4, 2, 3, 4, 128), F32),
            DMA((12,)),
            DMA((26,)), DMA((26,)), DMA((3,)), DMA((3,)), DMA((26,)), DMA((26,)), DMA((1,)), DMA((1,)),
            DMA((1,)), DMA((1,)), DMA((3,)), DMA((3,)), DMA((1,)),
        ],
        compiler_params=pltpu.CompilerParams(collective_id=0, has_side_effects=True, vmem_limit_bytes=67043328),
        name="front_pass",
    )(*arrays)


def on_device(cell_counts, grid_offset, fraction, species, species_density, species_pair, species_embed, species_charge):
    table, turned, mixed, mixed_turned = constants()
    order = (0, 1, 3, 2, 4)
    extended, density, wide_slope, electric, features = front_pass(
        species_charge, species_density, species_pair, species_embed, cell_counts, grid_offset.transpose(order),
        fraction.transpose(order), species, table, turned, mixed, mixed_turned)
    forces, density = force_pass(
        cell_counts, species_density, species_pair, extended, wide_slope, density, electric.reshape(8, 3, 4, 128),
        features)
    return forces.reshape(4, 2, 3, 4, 128).transpose(order), density.reshape(4, 2, 4, 128)


def solution(mesh):
    return jax.shard_map(
        on_device,
        mesh=mesh,
        in_specs=(
            P("gx", "gy", "gz"),
            P("gx", "gy", "gz", None, None),
            P("gx", "gy", "gz", None, None),
            P("gx", "gy", "gz", None),
            P(),
            P(),
            P(),
            P(),
        ),
        out_specs=(P("gx", "gy", "gz", None, None), P("gx", "gy", "gz", None)),
        check_vma=False,
    )
```

```python
import itertools
import math

import jax
import jax.numpy as jnp
import numpy as np
from jax import lax
from jax.experimental import pallas as pl
from jax.experimental.pallas import tpu as pltpu
from jax.sharding import PartitionSpec as P

PPC = 16
COUPLING = 8.0
F32, BF16 = jnp.float32, jnp.bfloat16
VMEM_SPEC = pl.BlockSpec(memory_space=pltpu.VMEM)
SMEM_SPEC = pl.BlockSpec(memory_space=pltpu.SMEM)


MESH = pl.DeviceIdType.MESH
AXES = ("gx", "gy", "gz")
SIZES = (4, 8, 4)
SIDES = [side for side in itertools.product((-1, 0, 1), repeat=3) if side != (0, 0, 0)]


def here():
    return [lax.axis_index(axis) for axis in AXES]


def toward(place, side):
    return tuple(lax.rem(p + s + n, n) for p, s, n in zip(place, side, SIZES))


def send(src, dst, send_sem, recv_sem, device):
    copy = pltpu.make_async_remote_copy(
        src_ref=src, dst_ref=dst, send_sem=send_sem, recv_sem=recv_sem, device_id=device, device_id_type=MESH)
    return copy


def halo_copies(own_ref, rim, ext_ref, place, send_sem, recv_sem):
    copies = []
    for n, side in enumerate(SIDES):
        src, dst = [], []
        for s, cells in zip(side, (4, 2, 4)):
            src.append(pl.ds(rim, cells) if s == 0 else pl.ds(rim + (cells - 1 if s == 1 else 0), 1))
            dst.append(pl.ds(1, cells) if s == 0 else pl.ds(0 if s == 1 else cells + 1, 1))
        copies.append(send(own_ref.at[tuple(src)], ext_ref.at[tuple(dst)], send_sem.at[n], recv_sem.at[n],
                           toward(place, side)))
    for copy in copies:
        copy.start()
    return copies


def column_copy(src_ref, dst_ref, place, send_sem, recv_sem, n):
    gx, gy, gz = place
    other = lax.rem(gz + n + 1, 4)
    return send(src_ref.at[other], dst_ref.at[gz], send_sem.at[n], recv_sem.at[n], (gx, gy, other))


def column_copies(src_ref, dst_ref, place, send_sem, recv_sem):
    copies = [column_copy(src_ref, dst_ref, place, send_sem, recv_sem, n) for n in range(3)]
    for copy in copies:
        copy.start()
    return copies


DMA = pltpu.SemaphoreType.DMA


ROWS = 16
KF = 32


def pieces(value):
    first = value.astype(BF16).astype(F32)
    rest = value - first
    second = rest.astype(BF16).astype(F32)
    third = (rest - second).astype(BF16).astype(F32)
    return first, second, third


def by_species(code, values):
    return jnp.where(code == 0.0, values[0], jnp.where(code == 1.0, values[1], 0.0))


def filled(ref, k):
    return jnp.full((8, 128), ref[k], F32)


def cube_root(value):
    guess = jnp.exp(jnp.log(value) * (1.0 / 3.0))
    return guess - (guess * guess * guess - value) / (3.0 * guess * guess)


def sublane():
    return lax.broadcasted_iota(jnp.int32, (8, 128), 0)


def assemble(blocks, ones, twos):
    rows = []
    for value, one, two in zip(blocks, ones, twos):
        first, second, third = pieces(value)
        rows.append(jnp.where(one, first, jnp.where(two, second, third)))
    return jnp.concatenate(rows, axis=0)


def patterns(first, second, last_first, last_second):
    ones, twos = [], []
    for block in range(4):
        one = two = None
        for k in range(block * 8, block * 8 + 8):
            here_one = (k % 6 in first) if k < 24 else k in last_first
            here_two = (k % 6 in second) if k < 24 else k in last_second
            if here_one:
                one = (sublane() == k % 8) if one is None else one | (sublane() == k % 8)
            if here_two:
                two = (sublane() == k % 8) if two is None else two | (sublane() == k % 8)
        ones.append(one)
        twos.append(two)
    return ones, twos


def source_features(ext_ref, feat_b, scales, first, last):
    ones, twos = patterns((0, 2, 5), (1, 3), (24,), (25,))
    low_six, low_four, low_two, low_three = [sublane() < n for n in (6, 4, 2, 3)]

    def cell(n, cx, cy, cz):
        r = n * 6 + cz

        def row(f):
            return jnp.broadcast_to(ext_ref[cx, cy, cz, f:f + 1, :], (8, 128))

        x = row(0) + (cx - 3).astype(F32)
        y = row(1) + (cy - 2).astype(F32)
        z = row(2) + (cz - 3.0)
        code = row(3)
        scale = by_species(code, scales)
        square = -scale * (x * x + y * y + z * z)
        double = scale + scale
        x, y, z = double * x, double * y, double * z
        blocks = [jnp.where(low_six, scale, x), jnp.where(low_four, x, y), jnp.where(low_two, y, z),
                  jnp.where(low_three, square, 0.0)]
        feat_b[pl.ds(pl.multiple_of(r * KF, KF), KF), :] = assemble(blocks, ones, twos).astype(BF16)

    def column(n, _):
        for z in range(6):
            cell(n, lax.div(n, 4), lax.rem(n, 4), z)
        return 0

    lax.fori_loop(first, last, column, 0)


def fill_wide(ext_ref, slope_ref, wide, ratios):
    def column(n, _):
        cx, cy = lax.div(n, 4), lax.rem(n, 4)
        offset_x, offset_y = (cx - 3).astype(F32), (cy - 2).astype(F32)
        for cz in range(6):
            def row(f):
                return jnp.broadcast_to(ext_ref[cx, cy, cz, f:f + 1, :], (8, 128))

            r = n * 6 + cz
            wide[r, 0] = row(0) + offset_x
            wide[r, 1] = row(1) + offset_y
            wide[r, 2] = row(2) + (cz - 3.0)
            wide[r, 3] = jnp.where(row(3) == 1.0, ratios[1], ratios[0])
            wide[r, 4] = jnp.broadcast_to(slope_ref[cx, cy, cz], (8, 128))
        return 0

    lax.fori_loop(0, 24, column, 0)


def corner(t):
    return (lax.div(t, 8) * 4 + lax.rem(lax.div(t, 4), 2)) * 6 + lax.rem(t, 4)


def target_features(ext_ref, own_t, keep, slope_ref, gains, ratios):
    ones, twos = patterns((0, 1, 4), (2, 3), (24, 25, 26, 27, 29), (28, 30))
    low_six, low_four, low_two, low_three = [sublane() < n for n in (6, 4, 2, 3)]
    low_five, low_seven = sublane() < 5, sublane() < 7

    def cell(n, cx, cy, cz):
        t, place = n * 4 + cz, (cx + 1, cy + 1, cz + 1)

        def row(f):
            return jnp.broadcast_to(ext_ref[place + (slice(f, f + 1), slice(None))], (8, 128))

        x = row(0) + (cx - 2).astype(F32)
        y = row(1) + (cy - 1).astype(F32)
        z = row(2) + (cz - 2.0)
        code = row(3)
        for k, value in enumerate((x, y, z, code)):
            keep[k, pl.ds(t, 1), :] = value[0:1]
        rest = 1.0 - (x * x + y * y + z * z)
        tail = jnp.zeros((8, 128), F32)
        if gains is not None:
            second = code == 1.0
            tilt = jnp.broadcast_to(slope_ref[place], (8, 128)) / jnp.where(second, ratios[1], ratios[0])
            tail = jnp.where(low_five, jnp.where(second, gains[1], gains[0]), jnp.where(low_seven, tilt, 0.0))
        blocks = [jnp.where(low_six, rest, x), jnp.where(low_four, x, y), jnp.where(low_two, y, z),
                  jnp.where(low_three, 1.0, tail)]
        own_t[t] = assemble(blocks, ones, twos).T.astype(BF16)

    def column(n, _):
        for cz in range(4):
            cell(n, lax.div(n, 2), lax.rem(n, 2), cz)
        return 0

    lax.fori_loop(0, 8, column, 0)


def split3(value):
    first = value.astype(BF16)
    rest = value - first.astype(F32)
    second = rest.astype(BF16)
    return first, second, (rest - second.astype(F32)).astype(BF16)


def lane_sums(rows):
    ones = jnp.ones((8, rows.shape[1]), BF16)
    return lax.dot_general(ones, rows, (((1,), (1,)), ((), ())), preferred_element_type=F32)


def right_side(feat_b, cell):
    r = pl.multiple_of(cell * KF, KF)
    return jnp.concatenate([feat_b[pl.ds(r + KF * dz, KF), :] for dz in range(3)], axis=1)


def density_steps(feat_b, own_t, totals, mat):
    lanes = lax.broadcasted_iota(jnp.int32, (128, 128), 1)
    other = lanes != lax.broadcasted_iota(jnp.int32, (128, 128), 0)

    def target(t):
        cx, cy, cz = lax.div(t, 8), lax.rem(lax.div(t, 4), 2), lax.rem(t, 4)
        left = own_t[t]
        total = jnp.zeros((128, 128), F32)
        for dx in range(3):
            for dy in range(3):
                right = right_side(feat_b, ((cx + dx) * 4 + cy + dy) * 6 + cz)
                weight = jnp.dot(left, right, preferred_element_type=F32)
                weight = jnp.maximum(weight, 0.0)
                for dz in range(3):
                    part = weight[:, dz * 128:(dz + 1) * 128]
                    if dx == 1 and dy == 1 and dz == 1:
                        part = jnp.where(other, part, 0.0)
                    total = total + part * part * part
        return total

    def settle(n):
        first, second, _ = split3(totals[...])
        sums = lane_sums(jnp.concatenate([first, second], axis=1))
        mat[pl.ds(2 * n, 1), :] = sums[0:1, 0:128]
        mat[pl.ds(2 * n + 1, 1), :] = sums[0:1, 128:256]

    def both(n, _):
        settle(jnp.maximum(n - 1, 0))
        totals[0:128, :] = target(2 * n)
        totals[128:256, :] = target(2 * n + 1)
        return 0

    def run(first, last):
        lax.fori_loop(first, last, both, 0)

    return run, lambda: settle(15)


def densities(pairs, embeds, density_ref, slope_ref, keep, mat):
    code = keep[3]
    alive = by_species(code, (1.0, 1.0))
    density = mat[0:32, :] * alive
    density_ref[...] = density.reshape(8, 4, 128)
    tilts = [jnp.concatenate([3.0 * embed / (pair * pair)] * 4, axis=0) for embed, pair in zip(embeds, pairs)]
    slope_ref[...] = (by_species(code, tilts) / jnp.sqrt(1.0 + density)).reshape(4, 2, 4, 1, 128)


def force_kernel(count_hbm, amplitude_hbm, pair_hbm, ext_hbm, slope_hbm, given_hbm, electric_hbm, feat_hbm, out_ref, density_ref,
                 count_ref, amplitude_ref, pair_ref, ext_ref, slope_ref, given_ref, electric_ref, feat_b, own_t, keep, wide,
                 near_a, near_b, part_a, part_b, mat, table, load_sem):
    loads = [
        pltpu.make_async_copy(src, dst, load_sem.at[n])
        for n, (src, dst) in enumerate((
            (amplitude_hbm, amplitude_ref), (pair_hbm, pair_ref), (ext_hbm, ext_ref), (slope_hbm, slope_ref),
            (count_hbm, count_ref), (given_hbm, given_ref), (electric_hbm, electric_ref),
            (feat_hbm, feat_b.at[0:144 * KF, :])))
    ]
    for load in loads:
        load.start()
    part_a[...] = jnp.zeros((4, 128, 128), F32)
    part_b[...] = jnp.zeros((4, 128, 128), F32)
    for load in loads[:4]:
        load.wait()
    amplitudes, pairs = [[filled(ref, k) for k in range(2)] for ref in (amplitude_ref, pair_ref)]
    ratios = [amplitude / (pair * pair) for amplitude, pair in zip(amplitudes, pairs)]
    gains = [-4.0 * pair / amplitude for amplitude, pair in zip(amplitudes, pairs)]
    fill_wide(ext_ref, slope_ref, wide, ratios)
    target_features(ext_ref, own_t, keep, slope_ref, gains, ratios)
    feat_b[144 * KF:146 * KF, :] = jnp.concatenate([sel_matrix()[:, 0:128], sel_matrix()[:, 128:256]], axis=0)

    def fill(n, _):
        table[n] = jnp.where(n < 27, (lax.div(n, 9) * 4 + lax.rem(lax.div(n, 3), 3)) * 6 + lax.rem(n, 3),
                             jnp.where(n == 28, 145, 144))
        table[32 + n] = jnp.where(n < 27, 1, 0)
        return 0

    lax.fori_loop(0, 32, fill, 0)
    lane = lax.broadcasted_iota(jnp.int32, (ROWS, 128), 1)
    lane3 = lax.broadcasted_iota(jnp.int32, (ROWS // 8, 8, 128), 2)
    row3 = lax.broadcasted_iota(jnp.int32, (ROWS // 8, 8, 128), 0) * 8 + lax.broadcasted_iota(
        jnp.int32, (ROWS // 8, 8, 128), 1)

    def around(base, k):
        return base + (k // 9 * 4 + k // 3 % 3) * 6 + k % 3

    def multiply(t, near, part):
        left, base = own_t[t], corner(t)
        for k in range(0, 8, 2):
            right = []
            for n in (part * 8 + k, part * 8 + k + 1):
                start = pl.multiple_of((table[n] + table[32 + n] * base) * KF, KF)
                right.append(feat_b[pl.ds(start, KF), :])
            product = jnp.dot(left, jnp.concatenate(right, axis=1), preferred_element_type=F32)
            near[part * 8 + k] = product[:, 0:128]
            near[part * 8 + k + 1] = product[:, 128:256]

    def chunk(t, near, part, c):
        rows = pl.ds(pl.multiple_of(c * ROWS, ROWS), ROWS)
        base = corner(t)

        def block(k):
            return near[k, rows, :].reshape(ROWS // 8, 8, 128)

        gain, tilt = block(27), block(28)
        zero = jnp.zeros((ROWS // 8, 8, 128), F32)
        m0, mx, my, mz = zero, zero, zero, zero
        for k in range(27):
            r = around(base, k)
            w = jnp.maximum(block(k), 0.0)
            if k == 13:
                w = jnp.where(lane3 != row3 + c * ROWS, w, 0.0)
            value = ((tilt * wide[r, 3] + wide[r, 4]) * w + gain) * w
            m0 = m0 + value
            mx = mx + value * wide[r, 0]
            my = my + value * wide[r, 1]
            mz = mz + value * wide[r, 2]
        for m, value in enumerate((m0, mx, my, mz)):
            part[m, rows, :] = value.reshape(ROWS, 128)

    def settle(t, part):
        for m in (0, 2):
            first, second, third = split3(jnp.concatenate([part[m], part[m + 1]], axis=0))
            sums = lane_sums(jnp.concatenate([first, second], axis=1)) + lane_sums(third)
            mat[pl.ds(t * 4 + m, 1), :] = sums[0:1, 0:128]
            mat[pl.ds(t * 4 + m + 1, 1), :] = sums[0:1, 128:256]

    for load in loads[4:]:
        load.wait()
    density_ref[...] = given_ref[...]
    for part in range(4):
        multiply(0, near_a, part)

    def target(t, near, following, part, before):
        later = jnp.minimum(t + 1, 31)

        def rest(c, _):
            chunk(t, near, part, c)
            return 0

        settle(jnp.maximum(t - 1, 0), before)
        for n in range(4):
            multiply(later, following, n)
            chunk(t, near, part, n)
        lax.fori_loop(4, lax.div(count_ref[lax.div(t, 8), lax.rem(lax.div(t, 4), 2), lax.rem(t, 4)] + ROWS - 1, ROWS), rest, 0)

    def pair(n, _):
        target(2 * n, near_a, near_b, part_a, part_b)
        target(2 * n + 1, near_b, near_a, part_b, part_a)
        return 0

    lax.fori_loop(0, 16, pair, 0)
    settle(31, part_b)
    whole = mat[pl.ds(0, 32, stride=4), :]
    amplitude = by_species(keep[3], [jnp.concatenate([value] * 4, axis=0) for value in amplitudes])
    for m in range(3):
        value = amplitude * (mat[pl.ds(m + 1, 32, stride=4), :] - keep[m] * whole)
        out_ref[:, m] = value.reshape(8, 4, 128) + COUPLING * electric_ref[:, m]


def sel_matrix():
    row = lax.broadcasted_iota(jnp.int32, (KF, 256), 0)
    lane = lax.broadcasted_iota(jnp.int32, (KF, 256), 1)
    first = (row >= 27) & (row < 29) & (lane < 128)
    second = (row >= 29) & (row < 31) & (lane >= 128)
    return jnp.where(first | second, 1.0, 0.0).astype(BF16)


def features_scratch():
    return [pltpu.VMEM((146 * KF, 128), BF16), pltpu.VMEM((32, 128, KF), BF16), pltpu.VMEM((4, 32, 128), F32)]


def force_pass(*arrays):
    return pl.pallas_call(
        force_kernel,
        out_shape=[jax.ShapeDtypeStruct((8, 3, 4, 128), F32), jax.ShapeDtypeStruct((8, 4, 128), F32)],
        in_specs=[pl.BlockSpec(memory_space=pltpu.HBM)] * 8,
        out_specs=[VMEM_SPEC] * 2,
        scratch_shapes=[
            pltpu.SMEM((4, 2, 4), jnp.int32),
            pltpu.SMEM((2,), F32),
            pltpu.SMEM((2,), F32),
            pltpu.VMEM((6, 4, 6, 4, 128), F32),
            pltpu.VMEM((6, 4, 6, 1, 128), F32),
            pltpu.VMEM((8, 4, 128), F32),
            pltpu.VMEM((8, 3, 4, 128), F32),
        ] + features_scratch() + [
            pltpu.VMEM((144, 5, 8, 128), F32),
            pltpu.VMEM((32, 128, 128), F32),
            pltpu.VMEM((32, 128, 128), F32),
            pltpu.VMEM((4, 128, 128), F32),
            pltpu.VMEM((4, 128, 128), F32),
            pltpu.VMEM((128, 128), F32),
            pltpu.SMEM((64,), jnp.int32),
            pltpu.SemaphoreType.DMA((8,)),
        ],
        compiler_params=pltpu.CompilerParams(vmem_limit_bytes=67043328),
        cost_estimate=pl.CostEstimate(flops=20_000_000_000, bytes_accessed=1_000_000, transcendentals=0),
        name="force_pass",
    )(*arrays)


EWALD_SPLIT = 0.7


def tables():
    mode = np.arange(256)[:, None]
    point = np.arange(256)[None, :]
    cosine = np.cos(2 * np.pi * (mode * point % 256) / 256) * np.sqrt(2 / 256)
    cosine[0] /= np.sqrt(2)
    cosine[128] /= np.sqrt(2)
    sine = np.sin(2 * np.pi * ((mode - 128) * point % 256) / 256) * np.sqrt(2 / 256)
    table = np.where(mode <= 128, cosine, sine)
    row = np.arange(512)
    xr, cell, s = row // 128, row // 8 % 16, row % 8
    mixed = table[:, cell * 16 + s % 4 * 4 + xr]
    return table, mixed


def parts_of(array):
    parts = []
    for _ in range(3):
        parts.append(array.astype(np.float32).astype(jnp.bfloat16))
        array = array - parts[-1].astype(np.float64)
    return np.stack(parts)


def split(value):
    high = value.astype(BF16)
    return high, (value - high.astype(F32)).astype(BF16)


def dot(a, b):
    return jnp.dot(a, b, preferred_element_type=F32)


def dot3(a, b):
    return dot(a[0], b[0]) + (dot(a[1], b[0]) + dot(a[0], b[1]))


def dot6(a, b):
    small = dot(a[1], b[1]) + (dot(a[2], b[0]) + dot(a[0], b[2]))
    return dot(a[0], b[0]) + (dot(a[1], b[0]) + dot(a[0], b[1]) + small)


def hat(count, lower, weight):
    point = lax.broadcasted_iota(jnp.int32, (count, lower.shape[1]), 0).astype(F32)
    return jnp.where(point == lower, 1.0 - weight, 0.0) + jnp.where(point == lower + 1.0, weight, 0.0)


def spread_and_transform(atoms_ref, charges, table_ref, out_ref, rho, gz, arrivals):
    def layer(cz, _):
        source, cell = lax.div(cz, 4), lax.rem(cz, 4)

        def row(f, shift=0.0):
            first = atoms_ref[source, cell, f:f + 1, :]
            second = atoms_ref[source, cell + 4, f:f + 1, :] + shift
            return jnp.concatenate([first, second], axis=1)

        ox, oy, oz, fx, fy, fz = row(0), row(1, 16.0), row(2), row(3), row(4), row(5)
        charge = by_species(row(6), charges)
        wy = hat(32, oy, fy)
        wz = split(hat(16, oz, fz) * charge)
        parts = []
        for x in range(16):
            wx = jnp.where(ox == x, 1.0 - fx, 0.0) + jnp.where(ox == x - 1, fx, 0.0)
            parts.append(wx * wy)
        plane = split(jnp.concatenate(parts, axis=0))
        dims = (((1,), (1,)), ((), ()))

        def against(a, b):
            return lax.dot_general(a, b, dims, preferred_element_type=F32)

        value = against(wz[0], plane[0]) + (against(wz[1], plane[0]) + against(wz[0], plane[1]))
        rho[pl.ds(pl.multiple_of(cz * 16, 16), 16), :] = value
        return 0

    for n, arrival in enumerate([None] + arrivals):
        if arrival is not None:
            arrival.wait()
        start = lax.rem(gz + 4 - n, 4) * 4
        lax.fori_loop(start, start + 4, layer, 0)
    lines = dot3((table_ref[0], table_ref[1]), split(rho[...]))
    for plane in range(2):
        for xq in range(4):
            out_ref[pl.ds(plane * 4 + xq, 128, stride=8), :] = lines[
                plane * 128:(plane + 1) * 128, xq * 128:(xq + 1) * 128]


def front_kernel(charge_hbm, amplitude_hbm, pair_hbm, embed_hbm, count_hbm, offset_hbm, fraction_hbm, species_hbm, table_hbm,
                 turned_hbm, mixed_hbm, mixed_turned_hbm, ext_ref, density_ref, wide_ref, electric_ref, feat_hbm,
                 charge_ref, amplitude_ref, pair_ref, embed_ref, count_ref, offset_ref, fraction_ref, species_ref, table_ref,
                 turned_ref, mixed_ref, mixed_turned_ref, atoms, got_ref, rho, lines, planes, fields, back, slopes, feat_b, own_t, rows, feat_c, totals, mat, field, out,
                 load_sem, halo_send, halo_recv, column_send, column_recv, slope_send, slope_recv, line_send, line_recv,
                 field_send, field_recv, return_send, return_recv, feat_sem):
    place = here()
    me = place[0] * 32 + place[1] * 4 + place[2]
    loads = [
        pltpu.make_async_copy(src, dst, load_sem.at[n])
        for n, (src, dst) in enumerate((
            (count_hbm, count_ref), (species_hbm, species_ref), (offset_hbm, offset_ref), (fraction_hbm, fraction_ref),
            (charge_hbm, charge_ref), (amplitude_hbm, amplitude_ref), (pair_hbm, pair_ref), (embed_hbm, embed_ref),
            (table_hbm, table_ref), (turned_hbm, turned_ref), (mixed_hbm, mixed_ref), (mixed_turned_hbm, mixed_turned_ref)))
    ]
    for load in loads:
        load.start()
    barrier = pltpu.get_barrier_semaphore()

    def greet(other, _):
        pl.semaphore_signal(barrier, inc=1, device_id=other, device_id_type=pl.DeviceIdType.LOGICAL)
        return 0

    lax.fori_loop(me + 1, 128, greet, 0)
    lax.fori_loop(0, me, greet, 0)
    for load in loads[:4]:
        load.wait()
    slot = lax.broadcasted_iota(jnp.int32, (1, 128), 1)

    def pack(n, _):
        x, y = lax.div(n, 2), lax.rem(n, 2)
        for z in range(4):
            code = jnp.where(slot < count_ref[x, y, z], species_ref[x, y, z:z + 1, :].astype(F32), -1.0)
            for d in range(3):
                offset, fraction = offset_ref[x, y, d, z:z + 1, :].astype(F32), fraction_ref[x, y, d, z:z + 1, :]
                ext_ref[x + 1, y + 1, z + 1, d:d + 1, :] = (offset + 0.5 + fraction) * (1.0 / PPC)
                atoms[x, y * 4 + z, d:d + 1, :] = offset
                atoms[x, y * 4 + z, d + 3:d + 4, :] = fraction
            ext_ref[x + 1, y + 1, z + 1, 3:4, :] = code
            atoms[x, y * 4 + z, 6:7, :] = code
            atoms[x, y * 4 + z, 7:8, :] = code
        return 0

    lax.fori_loop(0, 8, pack, 0)

    def keep_own(n, _):
        got_ref[place[2], n] = atoms[place[2], n]
        return 0

    lax.fori_loop(0, 8, keep_own, 0)
    target_features(ext_ref, own_t, rows, None, None, None)
    for load in loads[4:]:
        load.wait()
    pl.semaphore_wait(barrier, 127)
    columns = column_copies(atoms, got_ref, place, column_send, column_recv)
    halo = halo_copies(ext_ref, 1, ext_ref, place, halo_send, halo_recv)
    charges = [charge_ref[k] for k in range(2)]
    spread_and_transform(got_ref, charges, table_ref, lines, rho, place[2], columns)
    for copy in halo:
        copy.wait()
    amplitudes, pairs, embeds = [[filled(ref, k) for k in range(2)] for ref in (amplitude_ref, pair_ref, embed_ref)]

    def exchange(src, dst, send_sem, recv_sem):
        mine = pl.ds(pl.multiple_of(me * 8, 8), 8)

        def start(other, _):
            pltpu.make_async_remote_copy(
                src_ref=src.at[pl.ds(pl.multiple_of(other * 8, 8), 8), :],
                dst_ref=dst.at[mine, :],
                send_sem=send_sem.at[0],
                recv_sem=recv_sem.at[0],
                device_id=other,
                device_id_type=pl.DeviceIdType.LOGICAL,
            ).start()
            return 0

        lax.fori_loop(me + 1, 128, start, 0)
        lax.fori_loop(0, me, start, 0)
        dst[mine, :] = src[mine, :]

        def finish():
            pltpu.make_async_copy(src.at[0:1016, :], dst.at[0:1016, :], recv_sem.at[0]).wait()
            pltpu.make_async_copy(src.at[0:1016, :], dst.at[0:1016, :], send_sem.at[0]).wait()

        return finish

    roots = [cube_root(value) for value in amplitudes]
    source_features(ext_ref, feat_b, roots, 0, 4)
    finish_lines = exchange(lines, planes, line_send, line_recv)
    source_features(ext_ref, feat_b, roots, 4, 24)
    run, end = density_steps(feat_b, own_t, totals, mat)
    totals[...] = jnp.zeros((256, 128), F32)
    run(0, 8)
    finish_lines()
    transform_planes(me, planes, table_ref, turned_ref, mixed_ref, mixed_turned_ref, fields)
    run(8, 9)
    finish_fields = exchange(fields, back, field_send, field_recv)
    run(9, 16)
    end()
    densities(pairs, embeds, density_ref, slopes, rows, mat)

    def keep_slope(t, _):
        x, y, z = lax.div(t, 8), lax.rem(lax.div(t, 4), 2), lax.rem(t, 4)
        wide_ref[x + 1, y + 1, z + 1] = slopes[x, y, z]
        return 0

    lax.fori_loop(0, 32, keep_slope, 0)
    halo = halo_copies(slopes, 0, wide_ref, place, slope_send, slope_recv)
    source_features(ext_ref, feat_c, pairs, 0, 14)
    finish_fields()
    returns = sample(place, charges, back, got_ref, table_ref, electric_ref, field, out, return_send, return_recv)
    source_features(ext_ref, feat_c, pairs, 14, 24)
    for copy in halo:
        copy.wait()
    feat_copy = pltpu.make_async_copy(feat_c, feat_hbm, feat_sem.at[0])
    feat_copy.start()
    for copy in returns:
        copy.wait()
    feat_copy.wait()


def transform_planes(me, in_ref, table_ref, turned_ref, mixed_ref, mixed_turned_ref, out_ref):
    lane = lax.broadcasted_iota(jnp.int32, (16, 8, 128), 2)

    def pick(ref, half, g):
        starts = [(gx * 32 + (half * 4 + g) * 4) * 8 for gx in range(4)]
        return jnp.concatenate([ref[start:start + 32, :] for start in starts], axis=0).reshape(16, 8, 128)

    rows = []
    for xr in range(4):
        pair = []
        for half in range(2):
            value = jnp.zeros((16, 8, 128), F32)
            for g in range(4):
                block = pick(in_ref, half, g)
                if g != xr:
                    block = pltpu.roll(block.reshape(128, 128), (g - xr) * 32 % 128, 1).reshape(16, 8, 128)
                value = jnp.where(lax.div(lane, 32) == g, block, value)
            pair.append(value.reshape(128, 128))
        rows.append(jnp.concatenate(pair, axis=1))
    plane = jnp.concatenate(rows, axis=0)
    turned = (turned_ref[0], turned_ref[1])
    along_y = dot3(split(plane), turned)

    row = lax.broadcasted_iota(jnp.int32, (256, 256), 0)
    col = lax.broadcasted_iota(jnp.int32, (256, 256), 1)
    scale = 2.0 * math.pi / 256
    wave_x = jnp.where(row <= 128, row, row - 128).astype(F32) * scale
    wave_y = jnp.where(col <= 128, col, col - 128).astype(F32) * scale
    flat = wave_x * wave_x + wave_y * wave_y
    side = lax.div(lax.rem(lax.broadcasted_iota(jnp.int32, (512, 256), 0), 8), 4)
    total = None
    for p in range(2):
        mode = me if p == 0 else jnp.where(me == 0, 128, me)
        wave_z = jnp.full((256, 256), mode, jnp.int32).astype(F32) * scale
        squared = flat + wave_z * wave_z
        anchor = squared == 0.0
        green = jnp.where(anchor, 0.0, 4.0 * math.pi * jnp.exp(-squared / (4.0 * EWALD_SPLIT * EWALD_SPLIT))
                          / jnp.where(anchor, 1.0, squared))
        modes = split3(dot3((mixed_ref[0], mixed_ref[1]), split(jnp.where(side == p, along_y, 0.0))) * green)
        part = dot6([mixed_turned_ref[i] for i in range(3)], modes)
        total = part if total is None else jnp.where(side == 0, total, part)
    field = dot6(split3(total), [table_ref[i] for i in range(3)])
    for half in range(2):
        block = [field[xr * 128:(xr + 1) * 128, half * 128:(half + 1) * 128] for xr in range(4)]
        for g in range(4):
            value = jnp.zeros((16, 8, 128), F32)
            for xr in range(4):
                moved = block[xr]
                if g != xr:
                    moved = pltpu.roll(moved, (xr - g) * 32 % 128, 1)
                value = jnp.where(lax.div(lane, 32) == xr, moved.reshape(16, 8, 128), value)
            for gx in range(4):
                start = (gx * 32 + (half * 4 + g) * 4) * 8
                out_ref[start:start + 32, :] = value[gx * 4:(gx + 1) * 4].reshape(32, 128)


def sample(place, charges, in_ref, atoms_ref, table_ref, back_ref, field, out, send_sem, recv_sem):
    columns = [
        jnp.concatenate([in_ref[pl.ds(plane * 4 + xq, 128, stride=8), :] for xq in range(4)], axis=1)
        for plane in range(2)
    ]
    modes = jnp.concatenate(columns, axis=0)
    lines = jnp.concatenate([modes[:, i * 128:(i + 1) * 128].T for i in range(4)], axis=0)
    pieces_of_field = split3(dot6(split3(lines), [table_ref[i] for i in range(3)]))
    for group in range(2):
        for i, piece in enumerate(pieces_of_field):
            field[group, :, i * 128:(i + 1) * 128] = piece[:, group * 128:(group + 1) * 128]
    point = lax.broadcasted_iota(jnp.int32, (128, 128), 0).astype(F32)

    def cell(n):
        owner = lax.rem(place[2] + 1 + lax.div(n, 8), 4)
        own_cell = lax.rem(n, 8)
        cyl, cz = lax.div(own_cell, 4), owner * 4 + lax.rem(own_cell, 4)

        def row(f):
            return atoms_ref[owner, own_cell, f:f + 1, :]

        ox, oy, oz, fx, fy, fz = [row(f) for f in range(6)]
        charge = by_species(row(6), charges)
        lower_z = oz + (lax.rem(cz, 8) * 16).astype(F32)
        lower = jnp.where(point == lower_z, 1.0, 0.0)
        slope = jnp.where(point == lower_z + 1.0, 1.0, 0.0) - lower
        right = jnp.concatenate([lower, slope], axis=1).astype(BF16)
        right = jnp.concatenate([right, right, right], axis=0)
        left = field_rows(field, lax.div(cz, 8), cyl)
        both = dot(left, right)
        tilt = both[:, 128:256].reshape(16, 16, 128)
        plain = both[:, 0:128].reshape(16, 16, 128) + fz * tilt
        spot = lax.broadcasted_iota(jnp.int32, (16, 128), 0).astype(F32)
        low_y, high_y = spot == oy, spot == oy + 1.0
        wy = jnp.where(low_y, 1.0 - fy, 0.0) + jnp.where(high_y, fy, 0.0)
        sy = jnp.where(high_y, 1.0, 0.0) - jnp.where(low_y, 1.0, 0.0)

        def fold(value):
            return value[:, 0:8] + value[:, 8:16]

        plain_w, plain_s, tilt_w = fold(plain * wy), fold(plain * sy), fold(tilt * wy)
        x_sum = jnp.zeros((8, 128), F32)
        y_sum, z_sum = x_sum, x_sum
        for x in range(16):
            low_x, high_x = ox == x, ox == x - 1
            wx = jnp.where(low_x, 1.0 - fx, 0.0) + jnp.where(high_x, fx, 0.0)
            sx = jnp.where(high_x, 1.0, 0.0) - jnp.where(low_x, 1.0, 0.0)
            x_sum = x_sum + sx * plain_w[x]
            y_sum = y_sum + wx * plain_s[x]
            z_sum = z_sum + wx * tilt_w[x]
        for f, value in enumerate((x_sum, y_sum, z_sum)):
            out[owner, cyl, f, pl.ds(lax.rem(own_cell, 4), 1), :] = -charge * jnp.sum(value, axis=0, keepdims=True)

    def group(g, _):
        for n in range(2):
            cell(g * 8 + n)

        @pl.when(g > 0)
        def _():
            column_copy(out, back_ref, place, send_sem, recv_sem, g - 1).start()

        for n in range(2, 8):
            cell(g * 8 + n)
        return 0

    lax.fori_loop(0, 4, group, 0)
    copies = [column_copy(out, back_ref, place, send_sem, recv_sem, n) for n in range(3)]
    back_ref[place[2]] = out[place[2]]
    return copies


def field_rows(field, group, cyl):
    start = pl.multiple_of(cyl * 16, 16)
    return jnp.concatenate([field[group, pl.ds(start + 32 * x, 16), :] for x in range(16)], axis=0)


TABLE, MIXED = tables()


def constants():
    return (parts_of(TABLE), parts_of(TABLE.T)[:2], parts_of(MIXED)[:2], parts_of(MIXED.T))


def front_pass(*arrays):
    hbm = pl.BlockSpec(memory_space=pltpu.HBM)
    small = [pltpu.SMEM((2,), F32)] * 4 + [pltpu.SMEM((4, 2, 4), jnp.int32)]
    return pl.pallas_call(
        front_kernel,
        out_shape=[
            jax.ShapeDtypeStruct((6, 4, 6, 4, 128), F32),
            jax.ShapeDtypeStruct((8, 4, 128), F32),
            jax.ShapeDtypeStruct((6, 4, 6, 1, 128), F32),
            jax.ShapeDtypeStruct((4, 2, 3, 4, 128), F32),
            jax.ShapeDtypeStruct((144 * KF, 128), BF16),
        ],
        in_specs=[hbm] * 12,
        out_specs=[VMEM_SPEC] * 4 + [hbm],
        scratch_shapes=small + [
            pltpu.VMEM((4, 2, 3, 4, 128), jnp.int32),
            pltpu.VMEM((4, 2, 3, 4, 128), F32),
            pltpu.VMEM((4, 2, 4, 128), jnp.int32),
            pltpu.VMEM((3, 256, 256), BF16),
            pltpu.VMEM((2, 256, 256), BF16),
            pltpu.VMEM((2, 256, 512), BF16),
            pltpu.VMEM((3, 512, 256), BF16),
            pltpu.VMEM((4, 8, 8, 128), F32),
            pltpu.VMEM((4, 8, 8, 128), F32),
            pltpu.VMEM((256, 512), F32),
            pltpu.VMEM((1024, 128), F32),
            pltpu.VMEM((1024, 128), F32),
            pltpu.VMEM((1024, 128), F32),
            pltpu.VMEM((1024, 128), F32),
            pltpu.VMEM((4, 2, 4, 1, 128), F32),
        ] + features_scratch() + [
            pltpu.VMEM((144 * KF, 128), BF16),
            pltpu.VMEM((256, 128), F32),
            pltpu.VMEM((128, 128), F32),
            pltpu.VMEM((2, 512, 384), BF16),
            pltpu.VMEM((4, 2, 3, 4, 128), F32),
            DMA((12,)),
            DMA((26,)), DMA((26,)), DMA((3,)), DMA((3,)), DMA((26,)), DMA((26,)), DMA((1,)), DMA((1,)),
            DMA((1,)), DMA((1,)), DMA((3,)), DMA((3,)), DMA((1,)),
        ],
        compiler_params=pltpu.CompilerParams(collective_id=0, has_side_effects=True, vmem_limit_bytes=67043328),
        name="front_pass",
    )(*arrays)


def on_device(cell_counts, grid_offset, fraction, species, species_density, species_pair, species_embed, species_charge):
    table, turned, mixed, mixed_turned = constants()
    order = (0, 1, 3, 2, 4)
    extended, density, wide_slope, electric, features = front_pass(
        species_charge, species_density, species_pair, species_embed, cell_counts, grid_offset.transpose(order),
        fraction.transpose(order), species, table, turned, mixed, mixed_turned)
    forces, density = force_pass(
        cell_counts, species_density, species_pair, extended, wide_slope, density, electric.reshape(8, 3, 4, 128),
        features)
    return forces.reshape(4, 2, 3, 4, 128).transpose(order), density.reshape(4, 2, 4, 128)


def solution(mesh):
    return jax.shard_map(
        on_device,
        mesh=mesh,
        in_specs=(
            P("gx", "gy", "gz"),
            P("gx", "gy", "gz", None, None),
            P("gx", "gy", "gz", None, None),
            P("gx", "gy", "gz", None),
            P(),
            P(),
            P(),
            P(),
        ),
        out_specs=(P("gx", "gy", "gz", None, None), P("gx", "gy", "gz", None)),
        check_vma=False,
    )
```

```python
import itertools
import math

import jax
import jax.numpy as jnp
import numpy as np
from jax import lax
from jax.experimental import pallas as pl
from jax.experimental.pallas import tpu as pltpu
from jax.sharding import PartitionSpec as P

PPC = 16
COUPLING = 8.0
F32, BF16 = jnp.float32, jnp.bfloat16
VMEM_SPEC = pl.BlockSpec(memory_space=pltpu.VMEM)
SMEM_SPEC = pl.BlockSpec(memory_space=pltpu.SMEM)


MESH = pl.DeviceIdType.MESH
AXES = ("gx", "gy", "gz")
SIZES = (4, 8, 4)
SIDES = [side for side in itertools.product((-1, 0, 1), repeat=3) if side != (0, 0, 0)]


def here():
    return [lax.axis_index(axis) for axis in AXES]


def toward(place, side):
    return tuple(lax.rem(p + s + n, n) for p, s, n in zip(place, side, SIZES))


def send(src, dst, send_sem, recv_sem, device):
    copy = pltpu.make_async_remote_copy(
        src_ref=src, dst_ref=dst, send_sem=send_sem, recv_sem=recv_sem, device_id=device, device_id_type=MESH)
    return copy


def halo_copies(own_ref, rim, ext_ref, place, send_sem, recv_sem):
    copies = []
    for n, side in enumerate(SIDES):
        src, dst = [], []
        for s, cells in zip(side, (4, 2, 4)):
            src.append(pl.ds(rim, cells) if s == 0 else pl.ds(rim + (cells - 1 if s == 1 else 0), 1))
            dst.append(pl.ds(1, cells) if s == 0 else pl.ds(0 if s == 1 else cells + 1, 1))
        copies.append(send(own_ref.at[tuple(src)], ext_ref.at[tuple(dst)], send_sem.at[n], recv_sem.at[n],
                           toward(place, side)))
    for copy in copies:
        copy.start()
    return copies


def column_copy(src_ref, dst_ref, place, send_sem, recv_sem, n):
    gx, gy, gz = place
    other = lax.rem(gz + n + 1, 4)
    return send(src_ref.at[other], dst_ref.at[gz], send_sem.at[n], recv_sem.at[n], (gx, gy, other))


def column_copies(src_ref, dst_ref, place, send_sem, recv_sem):
    copies = [column_copy(src_ref, dst_ref, place, send_sem, recv_sem, n) for n in range(3)]
    for copy in copies:
        copy.start()
    return copies


DMA = pltpu.SemaphoreType.DMA


ROWS = 16
KF = 32


def pieces(value):
    first = value.astype(BF16).astype(F32)
    rest = value - first
    second = rest.astype(BF16).astype(F32)
    third = (rest - second).astype(BF16).astype(F32)
    return first, second, third


def by_species(code, values):
    return jnp.where(code == 0.0, values[0], jnp.where(code == 1.0, values[1], 0.0))


def filled(ref, k):
    return jnp.full((8, 128), ref[k], F32)


def cube_root(value):
    guess = jnp.exp(jnp.log(value) * (1.0 / 3.0))
    return guess - (guess * guess * guess - value) / (3.0 * guess * guess)


def sublane():
    return lax.broadcasted_iota(jnp.int32, (8, 128), 0)


def assemble(blocks, ones, twos):
    rows = []
    for value, one, two in zip(blocks, ones, twos):
        first, second, third = pieces(value)
        rows.append(jnp.where(one, first, jnp.where(two, second, third)))
    return jnp.concatenate(rows, axis=0)


def patterns(first, second, last_first, last_second):
    ones, twos = [], []
    for block in range(4):
        one = two = None
        for k in range(block * 8, block * 8 + 8):
            here_one = (k % 6 in first) if k < 24 else k in last_first
            here_two = (k % 6 in second) if k < 24 else k in last_second
            if here_one:
                one = (sublane() == k % 8) if one is None else one | (sublane() == k % 8)
            if here_two:
                two = (sublane() == k % 8) if two is None else two | (sublane() == k % 8)
        ones.append(one)
        twos.append(two)
    return ones, twos


def source_features(ext_ref, feat_b, scales, first, last):
    ones, twos = patterns((0, 2, 5), (1, 3), (24,), (25,))
    low_six, low_four, low_two, low_three = [sublane() < n for n in (6, 4, 2, 3)]

    def cell(n, cx, cy, cz):
        r = n * 6 + cz

        def row(f):
            return jnp.broadcast_to(ext_ref[cx, cy, cz, f:f + 1, :], (8, 128))

        x = row(0) + (cx - 3).astype(F32)
        y = row(1) + (cy - 2).astype(F32)
        z = row(2) + (cz - 3.0)
        code = row(3)
        scale = by_species(code, scales)
        square = -scale * (x * x + y * y + z * z)
        double = scale + scale
        x, y, z = double * x, double * y, double * z
        blocks = [jnp.where(low_six, scale, x), jnp.where(low_four, x, y), jnp.where(low_two, y, z),
                  jnp.where(low_three, square, 0.0)]
        feat_b[pl.ds(pl.multiple_of(r * KF, KF), KF), :] = assemble(blocks, ones, twos).astype(BF16)

    def column(n, _):
        for z in range(6):
            cell(n, lax.div(n, 4), lax.rem(n, 4), z)
        return 0

    lax.fori_loop(first, last, column, 0)


def fill_wide(ext_ref, slope_ref, wide, ratios):
    def column(n, _):
        cx, cy = lax.div(n, 4), lax.rem(n, 4)
        offset_x, offset_y = (cx - 3).astype(F32), (cy - 2).astype(F32)
        for cz in range(6):
            def row(f):
                return jnp.broadcast_to(ext_ref[cx, cy, cz, f:f + 1, :], (8, 128))

            r = n * 6 + cz
            wide[r, 0] = row(0) + offset_x
            wide[r, 1] = row(1) + offset_y
            wide[r, 2] = row(2) + (cz - 3.0)
            wide[r, 3] = jnp.where(row(3) == 1.0, ratios[1], ratios[0])
            wide[r, 4] = jnp.broadcast_to(slope_ref[cx, cy, cz], (8, 128))
        return 0

    lax.fori_loop(0, 24, column, 0)


def corner(t):
    return (lax.div(t, 8) * 4 + lax.rem(lax.div(t, 4), 2)) * 6 + lax.rem(t, 4)


def target_features(ext_ref, own_t, keep, slope_ref, gains, ratios):
    ones, twos = patterns((0, 1, 4), (2, 3), (24, 25, 26, 27, 29), (28, 30))
    low_six, low_four, low_two, low_three = [sublane() < n for n in (6, 4, 2, 3)]
    low_five, low_seven = sublane() < 5, sublane() < 7

    def cell(n, cx, cy, cz):
        t, place = n * 4 + cz, (cx + 1, cy + 1, cz + 1)

        def row(f):
            return jnp.broadcast_to(ext_ref[place + (slice(f, f + 1), slice(None))], (8, 128))

        x = row(0) + (cx - 2).astype(F32)
        y = row(1) + (cy - 1).astype(F32)
        z = row(2) + (cz - 2.0)
        code = row(3)
        for k, value in enumerate((x, y, z, code)):
            keep[k, pl.ds(t, 1), :] = value[0:1]
        rest = 1.0 - (x * x + y * y + z * z)
        tail = jnp.zeros((8, 128), F32)
        if gains is not None:
            second = code == 1.0
            tilt = jnp.broadcast_to(slope_ref[place], (8, 128)) / jnp.where(second, ratios[1], ratios[0])
            tail = jnp.where(low_five, jnp.where(second, gains[1], gains[0]), jnp.where(low_seven, tilt, 0.0))
        blocks = [jnp.where(low_six, rest, x), jnp.where(low_four, x, y), jnp.where(low_two, y, z),
                  jnp.where(low_three, 1.0, tail)]
        own_t[t] = assemble(blocks, ones, twos).T.astype(BF16)

    def column(n, _):
        for cz in range(4):
            cell(n, lax.div(n, 2), lax.rem(n, 2), cz)
        return 0

    lax.fori_loop(0, 8, column, 0)


def split3(value):
    first = value.astype(BF16)
    rest = value - first.astype(F32)
    second = rest.astype(BF16)
    return first, second, (rest - second.astype(F32)).astype(BF16)


def lane_sums(rows):
    ones = jnp.ones((8, rows.shape[1]), BF16)
    return lax.dot_general(ones, rows, (((1,), (1,)), ((), ())), preferred_element_type=F32)


def right_side(feat_b, cell):
    r = pl.multiple_of(cell * KF, KF)
    return jnp.concatenate([feat_b[pl.ds(r + KF * dz, KF), :] for dz in range(3)], axis=1)


def density_steps(feat_b, own_t, totals, mat):
    lanes = lax.broadcasted_iota(jnp.int32, (128, 128), 1)
    other = lanes != lax.broadcasted_iota(jnp.int32, (128, 128), 0)

    def target(t):
        cx, cy, cz = lax.div(t, 8), lax.rem(lax.div(t, 4), 2), lax.rem(t, 4)
        left = own_t[t]
        total = jnp.zeros((128, 128), F32)
        for dx in range(3):
            for dy in range(3):
                right = right_side(feat_b, ((cx + dx) * 4 + cy + dy) * 6 + cz)
                weight = jnp.dot(left, right, preferred_element_type=F32)
                weight = jnp.maximum(weight, 0.0)
                for dz in range(3):
                    part = weight[:, dz * 128:(dz + 1) * 128]
                    if dx == 1 and dy == 1 and dz == 1:
                        part = jnp.where(other, part, 0.0)
                    total = total + part * part * part
        return total

    def settle(n):
        first, second, _ = split3(totals[...])
        sums = lane_sums(jnp.concatenate([first, second], axis=1))
        mat[pl.ds(2 * n, 1), :] = sums[0:1, 0:128]
        mat[pl.ds(2 * n + 1, 1), :] = sums[0:1, 128:256]

    def both(n, _):
        settle(jnp.maximum(n - 1, 0))
        totals[0:128, :] = target(2 * n)
        totals[128:256, :] = target(2 * n + 1)
        return 0

    def run(first, last):
        lax.fori_loop(first, last, both, 0)

    return run, lambda: settle(15)


def densities(pairs, embeds, density_ref, slope_ref, keep, mat):
    code = keep[3]
    alive = by_species(code, (1.0, 1.0))
    density = mat[0:32, :] * alive
    density_ref[...] = density.reshape(8, 4, 128)
    tilts = [jnp.concatenate([3.0 * embed / (pair * pair)] * 4, axis=0) for embed, pair in zip(embeds, pairs)]
    slope_ref[...] = (by_species(code, tilts) / jnp.sqrt(1.0 + density)).reshape(4, 2, 4, 1, 128)


def force_kernel(count_hbm, amplitude_hbm, pair_hbm, ext_hbm, slope_hbm, given_hbm, electric_hbm, feat_hbm, out_ref, density_ref,
                 count_ref, amplitude_ref, pair_ref, ext_ref, slope_ref, given_ref, electric_ref, feat_b, own_t, keep, wide,
                 near_a, near_b, part_a, part_b, mat, table, load_sem):
    loads = [
        pltpu.make_async_copy(src, dst, load_sem.at[n])
        for n, (src, dst) in enumerate((
            (amplitude_hbm, amplitude_ref), (pair_hbm, pair_ref), (ext_hbm, ext_ref), (slope_hbm, slope_ref),
            (count_hbm, count_ref), (given_hbm, given_ref), (electric_hbm, electric_ref),
            (feat_hbm, feat_b.at[0:144 * KF, :])))
    ]
    for load in loads:
        load.start()
    part_a[...] = jnp.zeros((4, 128, 128), F32)
    part_b[...] = jnp.zeros((4, 128, 128), F32)
    for load in loads[:4]:
        load.wait()
    amplitudes, pairs = [[filled(ref, k) for k in range(2)] for ref in (amplitude_ref, pair_ref)]
    ratios = [amplitude / (pair * pair) for amplitude, pair in zip(amplitudes, pairs)]
    gains = [-4.0 * pair / amplitude for amplitude, pair in zip(amplitudes, pairs)]
    fill_wide(ext_ref, slope_ref, wide, ratios)
    target_features(ext_ref, own_t, keep, slope_ref, gains, ratios)
    feat_b[144 * KF:146 * KF, :] = jnp.concatenate([sel_matrix()[:, 0:128], sel_matrix()[:, 128:256]], axis=0)

    def fill(n, _):
        table[n] = jnp.where(n < 27, (lax.div(n, 9) * 4 + lax.rem(lax.div(n, 3), 3)) * 6 + lax.rem(n, 3),
                             jnp.where(n == 28, 145, 144))
        table[32 + n] = jnp.where(n < 27, 1, 0)
        return 0

    lax.fori_loop(0, 32, fill, 0)
    lane = lax.broadcasted_iota(jnp.int32, (ROWS, 128), 1)
    lane3 = lax.broadcasted_iota(jnp.int32, (ROWS // 8, 8, 128), 2)
    row3 = lax.broadcasted_iota(jnp.int32, (ROWS // 8, 8, 128), 0) * 8 + lax.broadcasted_iota(
        jnp.int32, (ROWS // 8, 8, 128), 1)

    def around(base, k):
        return base + (k // 9 * 4 + k // 3 % 3) * 6 + k % 3

    def multiply(t, near, part):
        left, base = own_t[t], corner(t)
        for k in range(0, 8, 2):
            right = []
            for n in (part * 8 + k, part * 8 + k + 1):
                start = pl.multiple_of((table[n] + table[32 + n] * base) * KF, KF)
                right.append(feat_b[pl.ds(start, KF), :])
            product = jnp.dot(left, jnp.concatenate(right, axis=1), preferred_element_type=F32)
            near[part * 8 + k] = product[:, 0:128]
            near[part * 8 + k + 1] = product[:, 128:256]

    def chunk(t, near, part, c):
        rows = pl.ds(pl.multiple_of(c * ROWS, ROWS), ROWS)
        base = corner(t)

        def block(k):
            return near[k, rows, :].reshape(ROWS // 8, 8, 128)

        gain, tilt = block(27), block(28)
        zero = jnp.zeros((ROWS // 8, 8, 128), F32)
        m0, mx, my, mz = zero, zero, zero, zero
        for k in range(27):
            r = around(base, k)
            w = jnp.maximum(block(k), 0.0)
            if k == 13:
                w = jnp.where(lane3 != row3 + c * ROWS, w, 0.0)
            value = ((tilt * wide[r, 3] + wide[r, 4]) * w + gain) * w
            m0 = m0 + value
            mx = mx + value * wide[r, 0]
            my = my + value * wide[r, 1]
            mz = mz + value * wide[r, 2]
        for m, value in enumerate((m0, mx, my, mz)):
            part[m, rows, :] = value.reshape(ROWS, 128)

    def settle(t, part):
        for m in (0, 2):
            first, second, third = split3(jnp.concatenate([part[m], part[m + 1]], axis=0))
            sums = lane_sums(jnp.concatenate([first, second], axis=1)) + lane_sums(third)
            mat[pl.ds(t * 4 + m, 1), :] = sums[0:1, 0:128]
            mat[pl.ds(t * 4 + m + 1, 1), :] = sums[0:1, 128:256]

    for load in loads[4:]:
        load.wait()
    density_ref[...] = given_ref[...]
    for part in range(4):
        multiply(0, near_a, part)

    def target(t, near, following, part, before):
        later = jnp.minimum(t + 1, 31)

        def rest(c, _):
            chunk(t, near, part, c)
            return 0

        settle(jnp.maximum(t - 1, 0), before)
        for n in range(4):
            multiply(later, following, n)
            chunk(t, near, part, n)
        lax.fori_loop(4, lax.div(count_ref[lax.div(t, 8), lax.rem(lax.div(t, 4), 2), lax.rem(t, 4)] + ROWS - 1, ROWS), rest, 0)

    def pair(n, _):
        target(2 * n, near_a, near_b, part_a, part_b)
        target(2 * n + 1, near_b, near_a, part_b, part_a)
        return 0

    lax.fori_loop(0, 16, pair, 0)
    settle(31, part_b)
    whole = mat[pl.ds(0, 32, stride=4), :]
    amplitude = by_species(keep[3], [jnp.concatenate([value] * 4, axis=0) for value in amplitudes])
    for m in range(3):
        value = amplitude * (mat[pl.ds(m + 1, 32, stride=4), :] - keep[m] * whole)
        out_ref[:, m] = value.reshape(8, 4, 128) + COUPLING * electric_ref[:, m]


def sel_matrix():
    row = lax.broadcasted_iota(jnp.int32, (KF, 256), 0)
    lane = lax.broadcasted_iota(jnp.int32, (KF, 256), 1)
    first = (row >= 27) & (row < 29) & (lane < 128)
    second = (row >= 29) & (row < 31) & (lane >= 128)
    return jnp.where(first | second, 1.0, 0.0).astype(BF16)


def features_scratch():
    return [pltpu.VMEM((146 * KF, 128), BF16), pltpu.VMEM((32, 128, KF), BF16), pltpu.VMEM((4, 32, 128), F32)]


def force_pass(*arrays):
    return pl.pallas_call(
        force_kernel,
        out_shape=[jax.ShapeDtypeStruct((8, 3, 4, 128), F32), jax.ShapeDtypeStruct((8, 4, 128), F32)],
        in_specs=[pl.BlockSpec(memory_space=pltpu.HBM)] * 8,
        out_specs=[VMEM_SPEC] * 2,
        scratch_shapes=[
            pltpu.SMEM((4, 2, 4), jnp.int32),
            pltpu.SMEM((2,), F32),
            pltpu.SMEM((2,), F32),
            pltpu.VMEM((6, 4, 6, 4, 128), F32),
            pltpu.VMEM((6, 4, 6, 1, 128), F32),
            pltpu.VMEM((8, 4, 128), F32),
            pltpu.VMEM((8, 3, 4, 128), F32),
        ] + features_scratch() + [
            pltpu.VMEM((144, 5, 8, 128), F32),
            pltpu.VMEM((32, 128, 128), F32),
            pltpu.VMEM((32, 128, 128), F32),
            pltpu.VMEM((4, 128, 128), F32),
            pltpu.VMEM((4, 128, 128), F32),
            pltpu.VMEM((128, 128), F32),
            pltpu.SMEM((64,), jnp.int32),
            pltpu.SemaphoreType.DMA((8,)),
        ],
        compiler_params=pltpu.CompilerParams(vmem_limit_bytes=67043328),
        cost_estimate=pl.CostEstimate(flops=20_000_000_000, bytes_accessed=1_000_000, transcendentals=0),
        name="force_pass",
    )(*arrays)


EWALD_SPLIT = 0.7


def tables():
    mode = np.arange(256)[:, None]
    point = np.arange(256)[None, :]
    cosine = np.cos(2 * np.pi * (mode * point % 256) / 256) * np.sqrt(2 / 256)
    cosine[0] /= np.sqrt(2)
    cosine[128] /= np.sqrt(2)
    sine = np.sin(2 * np.pi * ((mode - 128) * point % 256) / 256) * np.sqrt(2 / 256)
    table = np.where(mode <= 128, cosine, sine)
    row = np.arange(512)
    xr, cell, s = row // 128, row // 8 % 16, row % 8
    mixed = table[:, cell * 16 + s % 4 * 4 + xr]
    return table, mixed


def parts_of(array):
    parts = []
    for _ in range(3):
        parts.append(array.astype(np.float32).astype(jnp.bfloat16))
        array = array - parts[-1].astype(np.float64)
    return np.stack(parts)


def split(value):
    high = value.astype(BF16)
    return high, (value - high.astype(F32)).astype(BF16)


def dot(a, b):
    return jnp.dot(a, b, preferred_element_type=F32)


def dot3(a, b):
    return dot(a[0], b[0]) + (dot(a[1], b[0]) + dot(a[0], b[1]))


def dot6(a, b):
    small = dot(a[1], b[1]) + (dot(a[2], b[0]) + dot(a[0], b[2]))
    return dot(a[0], b[0]) + (dot(a[1], b[0]) + dot(a[0], b[1]) + small)


def hat(count, lower, weight):
    point = lax.broadcasted_iota(jnp.int32, (count, lower.shape[1]), 0).astype(F32)
    return jnp.where(point == lower, 1.0 - weight, 0.0) + jnp.where(point == lower + 1.0, weight, 0.0)


def spread_and_transform(atoms_ref, charges, table_ref, out_ref, rho, gz, arrivals):
    def layer(cz, _):
        source, cell = lax.div(cz, 4), lax.rem(cz, 4)

        def row(f, shift=0.0):
            first = atoms_ref[source, cell, f:f + 1, :]
            second = atoms_ref[source, cell + 4, f:f + 1, :] + shift
            return jnp.concatenate([first, second], axis=1)

        ox, oy, oz, fx, fy, fz = row(0), row(1, 16.0), row(2), row(3), row(4), row(5)
        charge = by_species(row(6), charges)
        wy = hat(32, oy, fy)
        wz = split(hat(16, oz, fz) * charge)
        parts = []
        for x in range(16):
            wx = jnp.where(ox == x, 1.0 - fx, 0.0) + jnp.where(ox == x - 1, fx, 0.0)
            parts.append(wx * wy)
        plane = split(jnp.concatenate(parts, axis=0))
        dims = (((1,), (1,)), ((), ()))

        def against(a, b):
            return lax.dot_general(a, b, dims, preferred_element_type=F32)

        value = against(wz[0], plane[0]) + (against(wz[1], plane[0]) + against(wz[0], plane[1]))
        rho[pl.ds(pl.multiple_of(cz * 16, 16), 16), :] = value
        return 0

    for n, arrival in enumerate([None] + arrivals):
        if arrival is not None:
            arrival.wait()
        start = lax.rem(gz + 4 - n, 4) * 4
        lax.fori_loop(start, start + 4, layer, 0)
    lines = dot3((table_ref[0], table_ref[1]), split(rho[...]))
    for plane in range(2):
        for xq in range(4):
            out_ref[pl.ds(plane * 4 + xq, 128, stride=8), :] = lines[
                plane * 128:(plane + 1) * 128, xq * 128:(xq + 1) * 128]


def front_kernel(charge_hbm, amplitude_hbm, pair_hbm, embed_hbm, count_hbm, offset_hbm, fraction_hbm, species_hbm, table_hbm,
                 turned_hbm, mixed_hbm, mixed_turned_hbm, ext_ref, density_ref, wide_ref, electric_ref, feat_hbm,
                 charge_ref, amplitude_ref, pair_ref, embed_ref, count_ref, offset_ref, fraction_ref, species_ref, table_ref,
                 turned_ref, mixed_ref, mixed_turned_ref, atoms, got_ref, rho, lines, planes, fields, back, slopes, feat_b, own_t, rows, feat_c, totals, mat, field, out,
                 load_sem, halo_send, halo_recv, column_send, column_recv, slope_send, slope_recv, line_send, line_recv,
                 field_send, field_recv, return_send, return_recv, feat_sem):
    place = here()
    me = place[0] * 32 + place[1] * 4 + place[2]
    loads = [
        pltpu.make_async_copy(src, dst, load_sem.at[n])
        for n, (src, dst) in enumerate((
            (count_hbm, count_ref), (species_hbm, species_ref), (offset_hbm, offset_ref), (fraction_hbm, fraction_ref),
            (charge_hbm, charge_ref), (amplitude_hbm, amplitude_ref), (pair_hbm, pair_ref), (embed_hbm, embed_ref),
            (table_hbm, table_ref), (turned_hbm, turned_ref), (mixed_hbm, mixed_ref), (mixed_turned_hbm, mixed_turned_ref)))
    ]
    for load in loads:
        load.start()
    barrier = pltpu.get_barrier_semaphore()

    def greet(other, _):
        pl.semaphore_signal(barrier, inc=1, device_id=other, device_id_type=pl.DeviceIdType.LOGICAL)
        return 0

    lax.fori_loop(me + 1, 128, greet, 0)
    lax.fori_loop(0, me, greet, 0)
    for load in loads[:4]:
        load.wait()
    slot = lax.broadcasted_iota(jnp.int32, (1, 128), 1)

    def pack(n, _):
        x, y = lax.div(n, 2), lax.rem(n, 2)
        for z in range(4):
            code = jnp.where(slot < count_ref[x, y, z], species_ref[x, y, z:z + 1, :].astype(F32), -1.0)
            for d in range(3):
                offset, fraction = offset_ref[x, y, d, z:z + 1, :].astype(F32), fraction_ref[x, y, d, z:z + 1, :]
                ext_ref[x + 1, y + 1, z + 1, d:d + 1, :] = (offset + 0.5 + fraction) * (1.0 / PPC)
                atoms[x, y * 4 + z, d:d + 1, :] = offset
                atoms[x, y * 4 + z, d + 3:d + 4, :] = fraction
            ext_ref[x + 1, y + 1, z + 1, 3:4, :] = code
            atoms[x, y * 4 + z, 6:7, :] = code
            atoms[x, y * 4 + z, 7:8, :] = code
        return 0

    lax.fori_loop(0, 8, pack, 0)

    def keep_own(n, _):
        got_ref[place[2], n] = atoms[place[2], n]
        return 0

    lax.fori_loop(0, 8, keep_own, 0)
    target_features(ext_ref, own_t, rows, None, None, None)
    for load in loads[4:]:
        load.wait()
    pl.semaphore_wait(barrier, 127)
    columns = column_copies(atoms, got_ref, place, column_send, column_recv)
    halo = halo_copies(ext_ref, 1, ext_ref, place, halo_send, halo_recv)
    charges = [charge_ref[k] for k in range(2)]
    spread_and_transform(got_ref, charges, table_ref, lines, rho, place[2], columns)
    for copy in halo:
        copy.wait()
    amplitudes, pairs, embeds = [[filled(ref, k) for k in range(2)] for ref in (amplitude_ref, pair_ref, embed_ref)]

    def exchange(src, dst, send_sem, recv_sem):
        mine = pl.ds(pl.multiple_of(me * 8, 8), 8)

        def start(_, other):
            other = lax.rem(other + 37, 128)
            pltpu.make_async_remote_copy(
                src_ref=src.at[pl.ds(pl.multiple_of(other * 8, 8), 8), :],
                dst_ref=dst.at[mine, :],
                send_sem=send_sem.at[0],
                recv_sem=recv_sem.at[0],
                device_id=other,
                device_id_type=pl.DeviceIdType.LOGICAL,
            ).start()
            return other

        lax.fori_loop(1, 128, start, me)
        dst[mine, :] = src[mine, :]

        def finish():
            pltpu.make_async_copy(src.at[0:1016, :], dst.at[0:1016, :], recv_sem.at[0]).wait()
            pltpu.make_async_copy(src.at[0:1016, :], dst.at[0:1016, :], send_sem.at[0]).wait()

        return finish

    roots = [cube_root(value) for value in amplitudes]
    source_features(ext_ref, feat_b, roots, 0, 4)
    finish_lines = exchange(lines, planes, line_send, line_recv)
    source_features(ext_ref, feat_b, roots, 4, 24)
    run, end = density_steps(feat_b, own_t, totals, mat)
    totals[...] = jnp.zeros((256, 128), F32)
    run(0, 8)
    finish_lines()
    transform_planes(me, planes, table_ref, turned_ref, mixed_ref, mixed_turned_ref, fields)
    run(8, 9)
    finish_fields = exchange(fields, back, field_send, field_recv)
    run(9, 16)
    end()
    densities(pairs, embeds, density_ref, slopes, rows, mat)

    def keep_slope(t, _):
        x, y, z = lax.div(t, 8), lax.rem(lax.div(t, 4), 2), lax.rem(t, 4)
        wide_ref[x + 1, y + 1, z + 1] = slopes[x, y, z]
        return 0

    lax.fori_loop(0, 32, keep_slope, 0)
    halo = halo_copies(slopes, 0, wide_ref, place, slope_send, slope_recv)
    source_features(ext_ref, feat_c, pairs, 0, 14)
    finish_fields()
    returns = sample(place, charges, back, got_ref, table_ref, electric_ref, field, out, return_send, return_recv)
    source_features(ext_ref, feat_c, pairs, 14, 24)
    for copy in halo:
        copy.wait()
    feat_copy = pltpu.make_async_copy(feat_c, feat_hbm, feat_sem.at[0])
    feat_copy.start()
    for copy in returns:
        copy.wait()
    feat_copy.wait()


def transform_planes(me, in_ref, table_ref, turned_ref, mixed_ref, mixed_turned_ref, out_ref):
    lane = lax.broadcasted_iota(jnp.int32, (16, 8, 128), 2)

    def pick(ref, half, g):
        starts = [(gx * 32 + (half * 4 + g) * 4) * 8 for gx in range(4)]
        return jnp.concatenate([ref[start:start + 32, :] for start in starts], axis=0).reshape(16, 8, 128)

    rows = []
    for xr in range(4):
        pair = []
        for half in range(2):
            value = jnp.zeros((16, 8, 128), F32)
            for g in range(4):
                block = pick(in_ref, half, g)
                if g != xr:
                    block = pltpu.roll(block.reshape(128, 128), (g - xr) * 32 % 128, 1).reshape(16, 8, 128)
                value = jnp.where(lax.div(lane, 32) == g, block, value)
            pair.append(value.reshape(128, 128))
        rows.append(jnp.concatenate(pair, axis=1))
    plane = jnp.concatenate(rows, axis=0)
    turned = (turned_ref[0], turned_ref[1])
    along_y = dot3(split(plane), turned)

    row = lax.broadcasted_iota(jnp.int32, (256, 256), 0)
    col = lax.broadcasted_iota(jnp.int32, (256, 256), 1)
    scale = 2.0 * math.pi / 256
    wave_x = jnp.where(row <= 128, row, row - 128).astype(F32) * scale
    wave_y = jnp.where(col <= 128, col, col - 128).astype(F32) * scale
    flat = wave_x * wave_x + wave_y * wave_y
    side = lax.div(lax.rem(lax.broadcasted_iota(jnp.int32, (512, 256), 0), 8), 4)
    total = None
    for p in range(2):
        mode = me if p == 0 else jnp.where(me == 0, 128, me)
        wave_z = jnp.full((256, 256), mode, jnp.int32).astype(F32) * scale
        squared = flat + wave_z * wave_z
        anchor = squared == 0.0
        green = jnp.where(anchor, 0.0, 4.0 * math.pi * jnp.exp(-squared / (4.0 * EWALD_SPLIT * EWALD_SPLIT))
                          / jnp.where(anchor, 1.0, squared))
        modes = split3(dot3((mixed_ref[0], mixed_ref[1]), split(jnp.where(side == p, along_y, 0.0))) * green)
        part = dot6([mixed_turned_ref[i] for i in range(3)], modes)
        total = part if total is None else jnp.where(side == 0, total, part)
    field = dot6(split3(total), [table_ref[i] for i in range(3)])
    for half in range(2):
        block = [field[xr * 128:(xr + 1) * 128, half * 128:(half + 1) * 128] for xr in range(4)]
        for g in range(4):
            value = jnp.zeros((16, 8, 128), F32)
            for xr in range(4):
                moved = block[xr]
                if g != xr:
                    moved = pltpu.roll(moved, (xr - g) * 32 % 128, 1)
                value = jnp.where(lax.div(lane, 32) == xr, moved.reshape(16, 8, 128), value)
            for gx in range(4):
                start = (gx * 32 + (half * 4 + g) * 4) * 8
                out_ref[start:start + 32, :] = value[gx * 4:(gx + 1) * 4].reshape(32, 128)


def sample(place, charges, in_ref, atoms_ref, table_ref, back_ref, field, out, send_sem, recv_sem):
    columns = [
        jnp.concatenate([in_ref[pl.ds(plane * 4 + xq, 128, stride=8), :] for xq in range(4)], axis=1)
        for plane in range(2)
    ]
    modes = jnp.concatenate(columns, axis=0)
    lines = jnp.concatenate([modes[:, i * 128:(i + 1) * 128].T for i in range(4)], axis=0)
    pieces_of_field = split3(dot6(split3(lines), [table_ref[i] for i in range(3)]))
    for group in range(2):
        for i, piece in enumerate(pieces_of_field):
            field[group, :, i * 128:(i + 1) * 128] = piece[:, group * 128:(group + 1) * 128]
    point = lax.broadcasted_iota(jnp.int32, (128, 128), 0).astype(F32)

    def cell(n):
        owner = lax.rem(place[2] + 1 + lax.div(n, 8), 4)
        own_cell = lax.rem(n, 8)
        cyl, cz = lax.div(own_cell, 4), owner * 4 + lax.rem(own_cell, 4)

        def row(f):
            return atoms_ref[owner, own_cell, f:f + 1, :]

        ox, oy, oz, fx, fy, fz = [row(f) for f in range(6)]
        charge = by_species(row(6), charges)
        lower_z = oz + (lax.rem(cz, 8) * 16).astype(F32)
        lower = jnp.where(point == lower_z, 1.0, 0.0)
        slope = jnp.where(point == lower_z + 1.0, 1.0, 0.0) - lower
        right = jnp.concatenate([lower, slope], axis=1).astype(BF16)
        right = jnp.concatenate([right, right, right], axis=0)
        left = field_rows(field, lax.div(cz, 8), cyl)
        both = dot(left, right)
        tilt = both[:, 128:256].reshape(16, 16, 128)
        plain = both[:, 0:128].reshape(16, 16, 128) + fz * tilt
        spot = lax.broadcasted_iota(jnp.int32, (16, 128), 0).astype(F32)
        low_y, high_y = spot == oy, spot == oy + 1.0
        wy = jnp.where(low_y, 1.0 - fy, 0.0) + jnp.where(high_y, fy, 0.0)
        sy = jnp.where(high_y, 1.0, 0.0) - jnp.where(low_y, 1.0, 0.0)

        def fold(value):
            return value[:, 0:8] + value[:, 8:16]

        plain_w, plain_s, tilt_w = fold(plain * wy), fold(plain * sy), fold(tilt * wy)
        x_sum = jnp.zeros((8, 128), F32)
        y_sum, z_sum = x_sum, x_sum
        for x in range(16):
            low_x, high_x = ox == x, ox == x - 1
            wx = jnp.where(low_x, 1.0 - fx, 0.0) + jnp.where(high_x, fx, 0.0)
            sx = jnp.where(high_x, 1.0, 0.0) - jnp.where(low_x, 1.0, 0.0)
            x_sum = x_sum + sx * plain_w[x]
            y_sum = y_sum + wx * plain_s[x]
            z_sum = z_sum + wx * tilt_w[x]
        for f, value in enumerate((x_sum, y_sum, z_sum)):
            out[owner, cyl, f, pl.ds(lax.rem(own_cell, 4), 1), :] = -charge * jnp.sum(value, axis=0, keepdims=True)

    def group(g, _):
        for n in range(2):
            cell(g * 8 + n)

        @pl.when(g > 0)
        def _():
            column_copy(out, back_ref, place, send_sem, recv_sem, g - 1).start()

        for n in range(2, 8):
            cell(g * 8 + n)
        return 0

    lax.fori_loop(0, 4, group, 0)
    copies = [column_copy(out, back_ref, place, send_sem, recv_sem, n) for n in range(3)]
    back_ref[place[2]] = out[place[2]]
    return copies


def field_rows(field, group, cyl):
    start = pl.multiple_of(cyl * 16, 16)
    return jnp.concatenate([field[group, pl.ds(start + 32 * x, 16), :] for x in range(16)], axis=0)


TABLE, MIXED = tables()


def constants():
    return (parts_of(TABLE), parts_of(TABLE.T)[:2], parts_of(MIXED)[:2], parts_of(MIXED.T))


def front_pass(*arrays):
    hbm = pl.BlockSpec(memory_space=pltpu.HBM)
    small = [pltpu.SMEM((2,), F32)] * 4 + [pltpu.SMEM((4, 2, 4), jnp.int32)]
    return pl.pallas_call(
        front_kernel,
        out_shape=[
            jax.ShapeDtypeStruct((6, 4, 6, 4, 128), F32),
            jax.ShapeDtypeStruct((8, 4, 128), F32),
            jax.ShapeDtypeStruct((6, 4, 6, 1, 128), F32),
            jax.ShapeDtypeStruct((4, 2, 3, 4, 128), F32),
            jax.ShapeDtypeStruct((144 * KF, 128), BF16),
        ],
        in_specs=[hbm] * 12,
        out_specs=[VMEM_SPEC] * 4 + [hbm],
        scratch_shapes=small + [
            pltpu.VMEM((4, 2, 3, 4, 128), jnp.int32),
            pltpu.VMEM((4, 2, 3, 4, 128), F32),
            pltpu.VMEM((4, 2, 4, 128), jnp.int32),
            pltpu.VMEM((3, 256, 256), BF16),
            pltpu.VMEM((2, 256, 256), BF16),
            pltpu.VMEM((2, 256, 512), BF16),
            pltpu.VMEM((3, 512, 256), BF16),
            pltpu.VMEM((4, 8, 8, 128), F32),
            pltpu.VMEM((4, 8, 8, 128), F32),
            pltpu.VMEM((256, 512), F32),
            pltpu.VMEM((1024, 128), F32),
            pltpu.VMEM((1024, 128), F32),
            pltpu.VMEM((1024, 128), F32),
            pltpu.VMEM((1024, 128), F32),
            pltpu.VMEM((4, 2, 4, 1, 128), F32),
        ] + features_scratch() + [
            pltpu.VMEM((144 * KF, 128), BF16),
            pltpu.VMEM((256, 128), F32),
            pltpu.VMEM((128, 128), F32),
            pltpu.VMEM((2, 512, 384), BF16),
            pltpu.VMEM((4, 2, 3, 4, 128), F32),
            DMA((12,)),
            DMA((26,)), DMA((26,)), DMA((3,)), DMA((3,)), DMA((26,)), DMA((26,)), DMA((1,)), DMA((1,)),
            DMA((1,)), DMA((1,)), DMA((3,)), DMA((3,)), DMA((1,)),
        ],
        compiler_params=pltpu.CompilerParams(collective_id=0, has_side_effects=True, vmem_limit_bytes=67043328),
        name="front_pass",
    )(*arrays)


def on_device(cell_counts, grid_offset, fraction, species, species_density, species_pair, species_embed, species_charge):
    table, turned, mixed, mixed_turned = constants()
    order = (0, 1, 3, 2, 4)
    extended, density, wide_slope, electric, features = front_pass(
        species_charge, species_density, species_pair, species_embed, cell_counts, grid_offset.transpose(order),
        fraction.transpose(order), species, table, turned, mixed, mixed_turned)
    forces, density = force_pass(
        cell_counts, species_density, species_pair, extended, wide_slope, density, electric.reshape(8, 3, 4, 128),
        features)
    return forces.reshape(4, 2, 3, 4, 128).transpose(order), density.reshape(4, 2, 4, 128)


def solution(mesh):
    return jax.shard_map(
        on_device,
        mesh=mesh,
        in_specs=(
            P("gx", "gy", "gz"),
            P("gx", "gy", "gz", None, None),
            P("gx", "gy", "gz", None, None),
            P("gx", "gy", "gz", None),
            P(),
            P(),
            P(),
            P(),
        ),
        out_specs=(P("gx", "gy", "gz", None, None), P("gx", "gy", "gz", None)),
        check_vma=False,
    )
```

```python
import itertools
import math

import jax
import jax.numpy as jnp
import numpy as np
from jax import lax
from jax.experimental import pallas as pl
from jax.experimental.pallas import tpu as pltpu
from jax.sharding import PartitionSpec as P

PPC = 16
COUPLING = 8.0
F32, BF16 = jnp.float32, jnp.bfloat16
VMEM_SPEC = pl.BlockSpec(memory_space=pltpu.VMEM)
SMEM_SPEC = pl.BlockSpec(memory_space=pltpu.SMEM)


MESH = pl.DeviceIdType.MESH
AXES = ("gx", "gy", "gz")
SIZES = (4, 8, 4)
SIDES = [side for side in itertools.product((-1, 0, 1), repeat=3) if side != (0, 0, 0)]


def here():
    return [lax.axis_index(axis) for axis in AXES]


def toward(place, side):
    return tuple(lax.rem(p + s + n, n) for p, s, n in zip(place, side, SIZES))


def send(src, dst, send_sem, recv_sem, device):
    copy = pltpu.make_async_remote_copy(
        src_ref=src, dst_ref=dst, send_sem=send_sem, recv_sem=recv_sem, device_id=device, device_id_type=MESH)
    return copy


def halo_copies(own_ref, rim, ext_ref, place, send_sem, recv_sem):
    copies = []
    for n, side in enumerate(SIDES):
        src, dst = [], []
        for s, cells in zip(side, (4, 2, 4)):
            src.append(pl.ds(rim, cells) if s == 0 else pl.ds(rim + (cells - 1 if s == 1 else 0), 1))
            dst.append(pl.ds(1, cells) if s == 0 else pl.ds(0 if s == 1 else cells + 1, 1))
        copies.append(send(own_ref.at[tuple(src)], ext_ref.at[tuple(dst)], send_sem.at[n], recv_sem.at[n],
                           toward(place, side)))
    for copy in copies:
        copy.start()
    return copies


def column_copy(src_ref, dst_ref, place, send_sem, recv_sem, n):
    gx, gy, gz = place
    other = lax.rem(gz + n + 1, 4)
    return send(src_ref.at[other], dst_ref.at[gz], send_sem.at[n], recv_sem.at[n], (gx, gy, other))


def column_copies(src_ref, dst_ref, place, send_sem, recv_sem):
    copies = [column_copy(src_ref, dst_ref, place, send_sem, recv_sem, n) for n in range(3)]
    for copy in copies:
        copy.start()
    return copies


DMA = pltpu.SemaphoreType.DMA


ROWS = 16
KF = 32


def pieces(value):
    first = value.astype(BF16).astype(F32)
    rest = value - first
    second = rest.astype(BF16).astype(F32)
    third = (rest - second).astype(BF16).astype(F32)
    return first, second, third


def by_species(code, values):
    return jnp.where(code == 0.0, values[0], jnp.where(code == 1.0, values[1], 0.0))


def filled(ref, k):
    return jnp.full((8, 128), ref[k], F32)


def cube_root(value):
    guess = jnp.exp(jnp.log(value) * (1.0 / 3.0))
    return guess - (guess * guess * guess - value) / (3.0 * guess * guess)


def sublane():
    return lax.broadcasted_iota(jnp.int32, (8, 128), 0)


def assemble(blocks, ones, twos):
    rows = []
    for value, one, two in zip(blocks, ones, twos):
        first, second, third = pieces(value)
        rows.append(jnp.where(one, first, jnp.where(two, second, third)))
    return jnp.concatenate(rows, axis=0)


def patterns(first, second, last_first, last_second):
    ones, twos = [], []
    for block in range(4):
        one = two = None
        for k in range(block * 8, block * 8 + 8):
            here_one = (k % 6 in first) if k < 24 else k in last_first
            here_two = (k % 6 in second) if k < 24 else k in last_second
            if here_one:
                one = (sublane() == k % 8) if one is None else one | (sublane() == k % 8)
            if here_two:
                two = (sublane() == k % 8) if two is None else two | (sublane() == k % 8)
        ones.append(one)
        twos.append(two)
    return ones, twos


def source_features(ext_ref, feat_b, scales, first, last):
    ones, twos = patterns((0, 2, 5), (1, 3), (24,), (25,))
    low_six, low_four, low_two, low_three = [sublane() < n for n in (6, 4, 2, 3)]

    def cell(n, cx, cy, cz):
        r = n * 6 + cz

        def row(f):
            return jnp.broadcast_to(ext_ref[cx, cy, cz, f:f + 1, :], (8, 128))

        x = row(0) + (cx - 3).astype(F32)
        y = row(1) + (cy - 2).astype(F32)
        z = row(2) + (cz - 3.0)
        code = row(3)
        scale = by_species(code, scales)
        square = -scale * (x * x + y * y + z * z)
        double = scale + scale
        x, y, z = double * x, double * y, double * z
        blocks = [jnp.where(low_six, scale, x), jnp.where(low_four, x, y), jnp.where(low_two, y, z),
                  jnp.where(low_three, square, 0.0)]
        feat_b[pl.ds(pl.multiple_of(r * KF, KF), KF), :] = assemble(blocks, ones, twos).astype(BF16)

    def column(n, _):
        for z in range(6):
            cell(n, lax.div(n, 4), lax.rem(n, 4), z)
        return 0

    lax.fori_loop(first, last, column, 0)


def fill_wide(ext_ref, slope_ref, wide, ratios):
    def column(n, _):
        cx, cy = lax.div(n, 4), lax.rem(n, 4)
        offset_x, offset_y = (cx - 3).astype(F32), (cy - 2).astype(F32)
        for cz in range(6):
            def row(f):
                return jnp.broadcast_to(ext_ref[cx, cy, cz, f:f + 1, :], (8, 128))

            r = n * 6 + cz
            wide[r, 0] = row(0) + offset_x
            wide[r, 1] = row(1) + offset_y
            wide[r, 2] = row(2) + (cz - 3.0)
            wide[r, 3] = jnp.where(row(3) == 1.0, ratios[1], ratios[0])
            wide[r, 4] = jnp.broadcast_to(slope_ref[cx, cy, cz], (8, 128))
        return 0

    lax.fori_loop(0, 24, column, 0)


def corner(t):
    return (lax.div(t, 8) * 4 + lax.rem(lax.div(t, 4), 2)) * 6 + lax.rem(t, 4)


def target_features(ext_ref, own_t, keep, slope_ref, gains, ratios):
    ones, twos = patterns((0, 1, 4), (2, 3), (24, 25, 26, 27, 29), (28, 30))
    low_six, low_four, low_two, low_three = [sublane() < n for n in (6, 4, 2, 3)]
    low_five, low_seven = sublane() < 5, sublane() < 7

    def cell(n, cx, cy, cz):
        t, place = n * 4 + cz, (cx + 1, cy + 1, cz + 1)

        def row(f):
            return jnp.broadcast_to(ext_ref[place + (slice(f, f + 1), slice(None))], (8, 128))

        x = row(0) + (cx - 2).astype(F32)
        y = row(1) + (cy - 1).astype(F32)
        z = row(2) + (cz - 2.0)
        code = row(3)
        for k, value in enumerate((x, y, z, code)):
            keep[k, pl.ds(t, 1), :] = value[0:1]
        rest = 1.0 - (x * x + y * y + z * z)
        tail = jnp.zeros((8, 128), F32)
        if gains is not None:
            second = code == 1.0
            tilt = jnp.broadcast_to(slope_ref[place], (8, 128)) / jnp.where(second, ratios[1], ratios[0])
            tail = jnp.where(low_five, jnp.where(second, gains[1], gains[0]), jnp.where(low_seven, tilt, 0.0))
        blocks = [jnp.where(low_six, rest, x), jnp.where(low_four, x, y), jnp.where(low_two, y, z),
                  jnp.where(low_three, 1.0, tail)]
        own_t[t] = assemble(blocks, ones, twos).T.astype(BF16)

    def column(n, _):
        for cz in range(4):
            cell(n, lax.div(n, 2), lax.rem(n, 2), cz)
        return 0

    lax.fori_loop(0, 8, column, 0)


def split3(value):
    first = value.astype(BF16)
    rest = value - first.astype(F32)
    second = rest.astype(BF16)
    return first, second, (rest - second.astype(F32)).astype(BF16)


def lane_sums(rows):
    ones = jnp.ones((8, rows.shape[1]), BF16)
    return lax.dot_general(ones, rows, (((1,), (1,)), ((), ())), preferred_element_type=F32)


def right_side(feat_b, cell):
    r = pl.multiple_of(cell * KF, KF)
    return jnp.concatenate([feat_b[pl.ds(r + KF * dz, KF), :] for dz in range(3)], axis=1)


def density_steps(feat_b, own_t, totals, mat):
    lanes = lax.broadcasted_iota(jnp.int32, (128, 128), 1)
    other = lanes != lax.broadcasted_iota(jnp.int32, (128, 128), 0)

    def target(t):
        cx, cy, cz = lax.div(t, 8), lax.rem(lax.div(t, 4), 2), lax.rem(t, 4)
        left = own_t[t]
        total = jnp.zeros((128, 128), F32)
        for dx in range(3):
            for dy in range(3):
                right = right_side(feat_b, ((cx + dx) * 4 + cy + dy) * 6 + cz)
                weight = jnp.dot(left, right, preferred_element_type=F32)
                weight = jnp.maximum(weight, 0.0)
                for dz in range(3):
                    part = weight[:, dz * 128:(dz + 1) * 128]
                    if dx == 1 and dy == 1 and dz == 1:
                        part = jnp.where(other, part, 0.0)
                    total = total + part * part * part
        return total

    def settle(n):
        first, second, _ = split3(totals[...])
        sums = lane_sums(jnp.concatenate([first, second], axis=1))
        mat[pl.ds(2 * n, 1), :] = sums[0:1, 0:128]
        mat[pl.ds(2 * n + 1, 1), :] = sums[0:1, 128:256]

    def both(n, _):
        settle(jnp.maximum(n - 1, 0))
        totals[0:128, :] = target(2 * n)
        totals[128:256, :] = target(2 * n + 1)
        return 0

    def run(first, last):
        lax.fori_loop(first, last, both, 0)

    return run, lambda: settle(15)


def densities(pairs, embeds, density_ref, slope_ref, keep, mat):
    code = keep[3]
    alive = by_species(code, (1.0, 1.0))
    density = mat[0:32, :] * alive
    density_ref[...] = density.reshape(8, 4, 128)
    tilts = [jnp.concatenate([3.0 * embed / (pair * pair)] * 4, axis=0) for embed, pair in zip(embeds, pairs)]
    slope_ref[...] = (by_species(code, tilts) / jnp.sqrt(1.0 + density)).reshape(4, 2, 4, 1, 128)


def force_kernel(count_hbm, amplitude_hbm, pair_hbm, ext_hbm, slope_hbm, given_hbm, electric_hbm, feat_hbm, out_ref, density_ref,
                 count_ref, amplitude_ref, pair_ref, ext_ref, slope_ref, given_ref, electric_ref, feat_b, own_t, keep, wide,
                 near_a, near_b, part_a, part_b, mat, table, load_sem):
    loads = [
        pltpu.make_async_copy(src, dst, load_sem.at[n])
        for n, (src, dst) in enumerate((
            (amplitude_hbm, amplitude_ref), (pair_hbm, pair_ref), (ext_hbm, ext_ref), (slope_hbm, slope_ref),
            (count_hbm, count_ref), (given_hbm, given_ref), (electric_hbm, electric_ref),
            (feat_hbm, feat_b.at[0:144 * KF, :])))
    ]
    for load in loads:
        load.start()
    part_a[...] = jnp.zeros((4, 128, 128), F32)
    part_b[...] = jnp.zeros((4, 128, 128), F32)
    for load in loads[:4]:
        load.wait()
    amplitudes, pairs = [[filled(ref, k) for k in range(2)] for ref in (amplitude_ref, pair_ref)]
    ratios = [amplitude / (pair * pair) for amplitude, pair in zip(amplitudes, pairs)]
    gains = [-4.0 * pair / amplitude for amplitude, pair in zip(amplitudes, pairs)]
    fill_wide(ext_ref, slope_ref, wide, ratios)
    target_features(ext_ref, own_t, keep, slope_ref, gains, ratios)
    feat_b[144 * KF:146 * KF, :] = jnp.concatenate([sel_matrix()[:, 0:128], sel_matrix()[:, 128:256]], axis=0)

    def fill(n, _):
        table[n] = jnp.where(n < 27, (lax.div(n, 9) * 4 + lax.rem(lax.div(n, 3), 3)) * 6 + lax.rem(n, 3),
                             jnp.where(n == 28, 145, 144))
        table[32 + n] = jnp.where(n < 27, 1, 0)
        return 0

    lax.fori_loop(0, 32, fill, 0)
    lane = lax.broadcasted_iota(jnp.int32, (ROWS, 128), 1)
    lane3 = lax.broadcasted_iota(jnp.int32, (ROWS // 8, 8, 128), 2)
    row3 = lax.broadcasted_iota(jnp.int32, (ROWS // 8, 8, 128), 0) * 8 + lax.broadcasted_iota(
        jnp.int32, (ROWS // 8, 8, 128), 1)

    def around(base, k):
        return base + (k // 9 * 4 + k // 3 % 3) * 6 + k % 3

    def multiply(t, near, part):
        left, base = own_t[t], corner(t)
        for k in range(0, 8, 2):
            right = []
            for n in (part * 8 + k, part * 8 + k + 1):
                start = pl.multiple_of((table[n] + table[32 + n] * base) * KF, KF)
                right.append(feat_b[pl.ds(start, KF), :])
            product = jnp.dot(left, jnp.concatenate(right, axis=1), preferred_element_type=F32)
            near[part * 8 + k] = product[:, 0:128]
            near[part * 8 + k + 1] = product[:, 128:256]

    def chunk(t, near, part, c):
        rows = pl.ds(pl.multiple_of(c * ROWS, ROWS), ROWS)
        base = corner(t)

        def block(k):
            return near[k, rows, :].reshape(ROWS // 8, 8, 128)

        gain, tilt = block(27), block(28)
        zero = jnp.zeros((ROWS // 8, 8, 128), F32)
        m0, mx, my, mz = zero, zero, zero, zero
        for k in range(27):
            r = around(base, k)
            w = jnp.maximum(block(k), 0.0)
            if k == 13:
                w = jnp.where(lane3 != row3 + c * ROWS, w, 0.0)
            value = ((tilt * wide[r, 3] + wide[r, 4]) * w + gain) * w
            m0 = m0 + value
            mx = mx + value * wide[r, 0]
            my = my + value * wide[r, 1]
            mz = mz + value * wide[r, 2]
        for m, value in enumerate((m0, mx, my, mz)):
            part[m, rows, :] = value.reshape(ROWS, 128)

    def settle(t, part):
        for m in (0, 2):
            first, second, third = split3(jnp.concatenate([part[m], part[m + 1]], axis=0))
            sums = lane_sums(jnp.concatenate([first, second], axis=1)) + lane_sums(third)
            mat[pl.ds(t * 4 + m, 1), :] = sums[0:1, 0:128]
            mat[pl.ds(t * 4 + m + 1, 1), :] = sums[0:1, 128:256]

    for load in loads[4:]:
        load.wait()
    density_ref[...] = given_ref[...]
    for part in range(4):
        multiply(0, near_a, part)

    def target(t, near, following, part, before):
        later = jnp.minimum(t + 1, 31)

        def rest(c, _):
            chunk(t, near, part, c)
            return 0

        settle(jnp.maximum(t - 1, 0), before)
        for n in range(4):
            multiply(later, following, n)
            chunk(t, near, part, n)
        lax.fori_loop(4, lax.div(count_ref[lax.div(t, 8), lax.rem(lax.div(t, 4), 2), lax.rem(t, 4)] + ROWS - 1, ROWS), rest, 0)

    def pair(n, _):
        target(2 * n, near_a, near_b, part_a, part_b)
        target(2 * n + 1, near_b, near_a, part_b, part_a)
        return 0

    lax.fori_loop(0, 16, pair, 0)
    settle(31, part_b)
    whole = mat[pl.ds(0, 32, stride=4), :]
    amplitude = by_species(keep[3], [jnp.concatenate([value] * 4, axis=0) for value in amplitudes])
    for m in range(3):
        value = amplitude * (mat[pl.ds(m + 1, 32, stride=4), :] - keep[m] * whole)
        out_ref[:, m] = value.reshape(8, 4, 128) + COUPLING * electric_ref[:, m]


def sel_matrix():
    row = lax.broadcasted_iota(jnp.int32, (KF, 256), 0)
    lane = lax.broadcasted_iota(jnp.int32, (KF, 256), 1)
    first = (row >= 27) & (row < 29) & (lane < 128)
    second = (row >= 29) & (row < 31) & (lane >= 128)
    return jnp.where(first | second, 1.0, 0.0).astype(BF16)


def features_scratch():
    return [pltpu.VMEM((146 * KF, 128), BF16), pltpu.VMEM((32, 128, KF), BF16), pltpu.VMEM((4, 32, 128), F32)]


def force_pass(*arrays):
    return pl.pallas_call(
        force_kernel,
        out_shape=[jax.ShapeDtypeStruct((8, 3, 4, 128), F32), jax.ShapeDtypeStruct((8, 4, 128), F32)],
        in_specs=[pl.BlockSpec(memory_space=pltpu.HBM)] * 8,
        out_specs=[VMEM_SPEC] * 2,
        scratch_shapes=[
            pltpu.SMEM((4, 2, 4), jnp.int32),
            pltpu.SMEM((2,), F32),
            pltpu.SMEM((2,), F32),
            pltpu.VMEM((6, 4, 6, 4, 128), F32),
            pltpu.VMEM((6, 4, 6, 1, 128), F32),
            pltpu.VMEM((8, 4, 128), F32),
            pltpu.VMEM((8, 3, 4, 128), F32),
        ] + features_scratch() + [
            pltpu.VMEM((144, 5, 8, 128), F32),
            pltpu.VMEM((32, 128, 128), F32),
            pltpu.VMEM((32, 128, 128), F32),
            pltpu.VMEM((4, 128, 128), F32),
            pltpu.VMEM((4, 128, 128), F32),
            pltpu.VMEM((128, 128), F32),
            pltpu.SMEM((64,), jnp.int32),
            pltpu.SemaphoreType.DMA((8,)),
        ],
        compiler_params=pltpu.CompilerParams(vmem_limit_bytes=67043328),
        cost_estimate=pl.CostEstimate(flops=20_000_000_000, bytes_accessed=1_000_000, transcendentals=0),
        name="force_pass",
    )(*arrays)


EWALD_SPLIT = 0.7


def tables():
    mode = np.arange(256)[:, None]
    point = np.arange(256)[None, :]
    cosine = np.cos(2 * np.pi * (mode * point % 256) / 256) * np.sqrt(2 / 256)
    cosine[0] /= np.sqrt(2)
    cosine[128] /= np.sqrt(2)
    sine = np.sin(2 * np.pi * ((mode - 128) * point % 256) / 256) * np.sqrt(2 / 256)
    table = np.where(mode <= 128, cosine, sine)
    row = np.arange(512)
    xr, cell, s = row // 128, row // 8 % 16, row % 8
    mixed = table[:, cell * 16 + s % 4 * 4 + xr]
    return table, mixed


def parts_of(array):
    parts = []
    for _ in range(3):
        parts.append(array.astype(np.float32).astype(jnp.bfloat16))
        array = array - parts[-1].astype(np.float64)
    return np.stack(parts)


def split(value):
    high = value.astype(BF16)
    return high, (value - high.astype(F32)).astype(BF16)


def dot(a, b):
    return jnp.dot(a, b, preferred_element_type=F32)


def dot3(a, b):
    return dot(a[0], b[0]) + (dot(a[1], b[0]) + dot(a[0], b[1]))


def dot6(a, b):
    small = dot(a[1], b[1]) + (dot(a[2], b[0]) + dot(a[0], b[2]))
    return dot(a[0], b[0]) + (dot(a[1], b[0]) + dot(a[0], b[1]) + small)


def hat(count, lower, weight):
    point = lax.broadcasted_iota(jnp.int32, (count, lower.shape[1]), 0).astype(F32)
    return jnp.where(point == lower, 1.0 - weight, 0.0) + jnp.where(point == lower + 1.0, weight, 0.0)


def spread_and_transform(atoms_ref, charges, table_ref, out_ref, rho, gz, arrivals):
    def layer(cz, _):
        source, cell = lax.div(cz, 4), lax.rem(cz, 4)

        def row(f, shift=0.0):
            first = atoms_ref[source, cell, f:f + 1, :]
            second = atoms_ref[source, cell + 4, f:f + 1, :] + shift
            return jnp.concatenate([first, second], axis=1)

        ox, oy, oz, fx, fy, fz = row(0), row(1, 16.0), row(2), row(3), row(4), row(5)
        charge = by_species(row(6), charges)
        wy = hat(32, oy, fy)
        wz = split(hat(16, oz, fz) * charge)
        parts = []
        for x in range(16):
            wx = jnp.where(ox == x, 1.0 - fx, 0.0) + jnp.where(ox == x - 1, fx, 0.0)
            parts.append(wx * wy)
        plane = split(jnp.concatenate(parts, axis=0))
        dims = (((1,), (1,)), ((), ()))

        def against(a, b):
            return lax.dot_general(a, b, dims, preferred_element_type=F32)

        value = against(wz[0], plane[0]) + (against(wz[1], plane[0]) + against(wz[0], plane[1]))
        rho[pl.ds(pl.multiple_of(cz * 16, 16), 16), :] = value
        return 0

    for n, arrival in enumerate([None] + arrivals):
        if arrival is not None:
            arrival.wait()
        start = lax.rem(gz + 4 - n, 4) * 4
        lax.fori_loop(start, start + 4, layer, 0)
    lines = dot3((table_ref[0], table_ref[1]), split(rho[...]))
    for plane in range(2):
        for xq in range(4):
            out_ref[pl.ds(plane * 4 + xq, 128, stride=8), :] = lines[
                plane * 128:(plane + 1) * 128, xq * 128:(xq + 1) * 128]


def front_kernel(charge_hbm, amplitude_hbm, pair_hbm, embed_hbm, count_hbm, offset_hbm, fraction_hbm, species_hbm, table_hbm,
                 turned_hbm, mixed_hbm, mixed_turned_hbm, ext_ref, density_ref, wide_ref, electric_ref, feat_hbm,
                 charge_ref, amplitude_ref, pair_ref, embed_ref, count_ref, offset_ref, fraction_ref, species_ref, table_ref,
                 turned_ref, mixed_ref, mixed_turned_ref, atoms, got_ref, rho, lines, planes, fields, back, slopes, feat_b, own_t, rows, feat_c, totals, mat, field, out,
                 load_sem, halo_send, halo_recv, column_send, column_recv, slope_send, slope_recv, line_send, line_recv,
                 field_send, field_recv, return_send, return_recv, feat_sem):
    place = here()
    me = place[0] * 32 + place[1] * 4 + place[2]
    loads = [
        pltpu.make_async_copy(src, dst, load_sem.at[n])
        for n, (src, dst) in enumerate((
            (count_hbm, count_ref), (species_hbm, species_ref), (offset_hbm, offset_ref), (fraction_hbm, fraction_ref),
            (charge_hbm, charge_ref), (amplitude_hbm, amplitude_ref), (pair_hbm, pair_ref), (embed_hbm, embed_ref),
            (table_hbm, table_ref), (turned_hbm, turned_ref), (mixed_hbm, mixed_ref), (mixed_turned_hbm, mixed_turned_ref)))
    ]
    for load in loads:
        load.start()
    barrier = pltpu.get_barrier_semaphore()

    def greet(other, _):
        pl.semaphore_signal(barrier, inc=1, device_id=other, device_id_type=pl.DeviceIdType.LOGICAL)
        return 0

    lax.fori_loop(me + 1, 128, greet, 0)
    lax.fori_loop(0, me, greet, 0)
    for load in loads[:4]:
        load.wait()
    slot = lax.broadcasted_iota(jnp.int32, (1, 128), 1)

    def pack(n, _):
        x, y = lax.div(n, 2), lax.rem(n, 2)
        for z in range(4):
            code = jnp.where(slot < count_ref[x, y, z], species_ref[x, y, z:z + 1, :].astype(F32), -1.0)
            for d in range(3):
                offset, fraction = offset_ref[x, y, d, z:z + 1, :].astype(F32), fraction_ref[x, y, d, z:z + 1, :]
                ext_ref[x + 1, y + 1, z + 1, d:d + 1, :] = (offset + 0.5 + fraction) * (1.0 / PPC)
                atoms[x, y * 4 + z, d:d + 1, :] = offset
                atoms[x, y * 4 + z, d + 3:d + 4, :] = fraction
            ext_ref[x + 1, y + 1, z + 1, 3:4, :] = code
            atoms[x, y * 4 + z, 6:7, :] = code
            atoms[x, y * 4 + z, 7:8, :] = code
        return 0

    lax.fori_loop(0, 8, pack, 0)

    def keep_own(n, _):
        got_ref[place[2], n] = atoms[place[2], n]
        return 0

    lax.fori_loop(0, 8, keep_own, 0)
    target_features(ext_ref, own_t, rows, None, None, None)
    for load in loads[4:]:
        load.wait()
    pl.semaphore_wait(barrier, 127)
    columns = column_copies(atoms, got_ref, place, column_send, column_recv)
    halo = halo_copies(ext_ref, 1, ext_ref, place, halo_send, halo_recv)
    charges = [charge_ref[k] for k in range(2)]
    spread_and_transform(got_ref, charges, table_ref, lines, rho, place[2], columns)
    for copy in halo:
        copy.wait()
    amplitudes, pairs, embeds = [[filled(ref, k) for k in range(2)] for ref in (amplitude_ref, pair_ref, embed_ref)]

    def exchange(src, dst, send_sem, recv_sem):
        mine = pl.ds(pl.multiple_of(me * 8, 8), 8)

        def start(other):
            pltpu.make_async_remote_copy(
                src_ref=src.at[pl.ds(pl.multiple_of(other * 8, 8), 8), :],
                dst_ref=dst.at[mine, :],
                send_sem=send_sem.at[0],
                recv_sem=recv_sem.at[0],
                device_id=other,
                device_id_type=pl.DeviceIdType.LOGICAL,
            ).start()

        def both_ways(i, _):
            start(lax.rem(me + i, 128))
            start(lax.rem(me + 128 - i, 128))
            return 0

        lax.fori_loop(1, 64, both_ways, 0)
        start(lax.rem(me + 64, 128))
        dst[mine, :] = src[mine, :]

        def finish():
            pltpu.make_async_copy(src.at[0:1016, :], dst.at[0:1016, :], recv_sem.at[0]).wait()
            pltpu.make_async_copy(src.at[0:1016, :], dst.at[0:1016, :], send_sem.at[0]).wait()

        return finish

    roots = [cube_root(value) for value in amplitudes]
    source_features(ext_ref, feat_b, roots, 0, 4)
    finish_lines = exchange(lines, planes, line_send, line_recv)
    source_features(ext_ref, feat_b, roots, 4, 24)
    run, end = density_steps(feat_b, own_t, totals, mat)
    totals[...] = jnp.zeros((256, 128), F32)
    run(0, 8)
    finish_lines()
    transform_planes(me, planes, table_ref, turned_ref, mixed_ref, mixed_turned_ref, fields)
    run(8, 9)
    finish_fields = exchange(fields, back, field_send, field_recv)
    run(9, 16)
    end()
    densities(pairs, embeds, density_ref, slopes, rows, mat)

    def keep_slope(t, _):
        x, y, z = lax.div(t, 8), lax.rem(lax.div(t, 4), 2), lax.rem(t, 4)
        wide_ref[x + 1, y + 1, z + 1] = slopes[x, y, z]
        return 0

    lax.fori_loop(0, 32, keep_slope, 0)
    halo = halo_copies(slopes, 0, wide_ref, place, slope_send, slope_recv)
    source_features(ext_ref, feat_c, pairs, 0, 14)
    finish_fields()
    returns = sample(place, charges, back, got_ref, table_ref, electric_ref, field, out, return_send, return_recv)
    source_features(ext_ref, feat_c, pairs, 14, 24)
    for copy in halo:
        copy.wait()
    feat_copy = pltpu.make_async_copy(feat_c, feat_hbm, feat_sem.at[0])
    feat_copy.start()
    for copy in returns:
        copy.wait()
    feat_copy.wait()


def transform_planes(me, in_ref, table_ref, turned_ref, mixed_ref, mixed_turned_ref, out_ref):
    lane = lax.broadcasted_iota(jnp.int32, (16, 8, 128), 2)

    def pick(ref, half, g):
        starts = [(gx * 32 + (half * 4 + g) * 4) * 8 for gx in range(4)]
        return jnp.concatenate([ref[start:start + 32, :] for start in starts], axis=0).reshape(16, 8, 128)

    rows = []
    for xr in range(4):
        pair = []
        for half in range(2):
            value = jnp.zeros((16, 8, 128), F32)
            for g in range(4):
                block = pick(in_ref, half, g)
                if g != xr:
                    block = pltpu.roll(block.reshape(128, 128), (g - xr) * 32 % 128, 1).reshape(16, 8, 128)
                value = jnp.where(lax.div(lane, 32) == g, block, value)
            pair.append(value.reshape(128, 128))
        rows.append(jnp.concatenate(pair, axis=1))
    plane = jnp.concatenate(rows, axis=0)
    turned = (turned_ref[0], turned_ref[1])
    along_y = dot3(split(plane), turned)

    row = lax.broadcasted_iota(jnp.int32, (256, 256), 0)
    col = lax.broadcasted_iota(jnp.int32, (256, 256), 1)
    scale = 2.0 * math.pi / 256
    wave_x = jnp.where(row <= 128, row, row - 128).astype(F32) * scale
    wave_y = jnp.where(col <= 128, col, col - 128).astype(F32) * scale
    flat = wave_x * wave_x + wave_y * wave_y
    side = lax.div(lax.rem(lax.broadcasted_iota(jnp.int32, (512, 256), 0), 8), 4)
    total = None
    for p in range(2):
        mode = me if p == 0 else jnp.where(me == 0, 128, me)
        wave_z = jnp.full((256, 256), mode, jnp.int32).astype(F32) * scale
        squared = flat + wave_z * wave_z
        anchor = squared == 0.0
        green = jnp.where(anchor, 0.0, 4.0 * math.pi * jnp.exp(-squared / (4.0 * EWALD_SPLIT * EWALD_SPLIT))
                          / jnp.where(anchor, 1.0, squared))
        modes = split3(dot3((mixed_ref[0], mixed_ref[1]), split(jnp.where(side == p, along_y, 0.0))) * green)
        part = dot6([mixed_turned_ref[i] for i in range(3)], modes)
        total = part if total is None else jnp.where(side == 0, total, part)
    field = dot6(split3(total), [table_ref[i] for i in range(3)])
    for half in range(2):
        block = [field[xr * 128:(xr + 1) * 128, half * 128:(half + 1) * 128] for xr in range(4)]
        for g in range(4):
            value = jnp.zeros((16, 8, 128), F32)
            for xr in range(4):
                moved = block[xr]
                if g != xr:
                    moved = pltpu.roll(moved, (xr - g) * 32 % 128, 1)
                value = jnp.where(lax.div(lane, 32) == xr, moved.reshape(16, 8, 128), value)
            for gx in range(4):
                start = (gx * 32 + (half * 4 + g) * 4) * 8
                out_ref[start:start + 32, :] = value[gx * 4:(gx + 1) * 4].reshape(32, 128)


def sample(place, charges, in_ref, atoms_ref, table_ref, back_ref, field, out, send_sem, recv_sem):
    columns = [
        jnp.concatenate([in_ref[pl.ds(plane * 4 + xq, 128, stride=8), :] for xq in range(4)], axis=1)
        for plane in range(2)
    ]
    modes = jnp.concatenate(columns, axis=0)
    lines = jnp.concatenate([modes[:, i * 128:(i + 1) * 128].T for i in range(4)], axis=0)
    pieces_of_field = split3(dot6(split3(lines), [table_ref[i] for i in range(3)]))
    for group in range(2):
        for i, piece in enumerate(pieces_of_field):
            field[group, :, i * 128:(i + 1) * 128] = piece[:, group * 128:(group + 1) * 128]
    point = lax.broadcasted_iota(jnp.int32, (128, 128), 0).astype(F32)

    def cell(n):
        owner = lax.rem(place[2] + 1 + lax.div(n, 8), 4)
        own_cell = lax.rem(n, 8)
        cyl, cz = lax.div(own_cell, 4), owner * 4 + lax.rem(own_cell, 4)

        def row(f):
            return atoms_ref[owner, own_cell, f:f + 1, :]

        ox, oy, oz, fx, fy, fz = [row(f) for f in range(6)]
        charge = by_species(row(6), charges)
        lower_z = oz + (lax.rem(cz, 8) * 16).astype(F32)
        lower = jnp.where(point == lower_z, 1.0, 0.0)
        slope = jnp.where(point == lower_z + 1.0, 1.0, 0.0) - lower
        right = jnp.concatenate([lower, slope], axis=1).astype(BF16)
        right = jnp.concatenate([right, right, right], axis=0)
        left = field_rows(field, lax.div(cz, 8), cyl)
        both = dot(left, right)
        tilt = both[:, 128:256].reshape(16, 16, 128)
        plain = both[:, 0:128].reshape(16, 16, 128) + fz * tilt
        spot = lax.broadcasted_iota(jnp.int32, (16, 128), 0).astype(F32)
        low_y, high_y = spot == oy, spot == oy + 1.0
        wy = jnp.where(low_y, 1.0 - fy, 0.0) + jnp.where(high_y, fy, 0.0)
        sy = jnp.where(high_y, 1.0, 0.0) - jnp.where(low_y, 1.0, 0.0)

        def fold(value):
            return value[:, 0:8] + value[:, 8:16]

        plain_w, plain_s, tilt_w = fold(plain * wy), fold(plain * sy), fold(tilt * wy)
        x_sum = jnp.zeros((8, 128), F32)
        y_sum, z_sum = x_sum, x_sum
        for x in range(16):
            low_x, high_x = ox == x, ox == x - 1
            wx = jnp.where(low_x, 1.0 - fx, 0.0) + jnp.where(high_x, fx, 0.0)
            sx = jnp.where(high_x, 1.0, 0.0) - jnp.where(low_x, 1.0, 0.0)
            x_sum = x_sum + sx * plain_w[x]
            y_sum = y_sum + wx * plain_s[x]
            z_sum = z_sum + wx * tilt_w[x]
        for f, value in enumerate((x_sum, y_sum, z_sum)):
            out[owner, cyl, f, pl.ds(lax.rem(own_cell, 4), 1), :] = -charge * jnp.sum(value, axis=0, keepdims=True)

    def group(g, _):
        for n in range(2):
            cell(g * 8 + n)

        @pl.when(g > 0)
        def _():
            column_copy(out, back_ref, place, send_sem, recv_sem, g - 1).start()

        for n in range(2, 8):
            cell(g * 8 + n)
        return 0

    lax.fori_loop(0, 4, group, 0)
    copies = [column_copy(out, back_ref, place, send_sem, recv_sem, n) for n in range(3)]
    back_ref[place[2]] = out[place[2]]
    return copies


def field_rows(field, group, cyl):
    start = pl.multiple_of(cyl * 16, 16)
    return jnp.concatenate([field[group, pl.ds(start + 32 * x, 16), :] for x in range(16)], axis=0)


TABLE, MIXED = tables()


def constants():
    return (parts_of(TABLE), parts_of(TABLE.T)[:2], parts_of(MIXED)[:2], parts_of(MIXED.T))


def front_pass(*arrays):
    hbm = pl.BlockSpec(memory_space=pltpu.HBM)
    small = [pltpu.SMEM((2,), F32)] * 4 + [pltpu.SMEM((4, 2, 4), jnp.int32)]
    return pl.pallas_call(
        front_kernel,
        out_shape=[
            jax.ShapeDtypeStruct((6, 4, 6, 4, 128), F32),
            jax.ShapeDtypeStruct((8, 4, 128), F32),
            jax.ShapeDtypeStruct((6, 4, 6, 1, 128), F32),
            jax.ShapeDtypeStruct((4, 2, 3, 4, 128), F32),
            jax.ShapeDtypeStruct((144 * KF, 128), BF16),
        ],
        in_specs=[hbm] * 12,
        out_specs=[VMEM_SPEC] * 4 + [hbm],
        scratch_shapes=small + [
            pltpu.VMEM((4, 2, 3, 4, 128), jnp.int32),
            pltpu.VMEM((4, 2, 3, 4, 128), F32),
            pltpu.VMEM((4, 2, 4, 128), jnp.int32),
            pltpu.VMEM((3, 256, 256), BF16),
            pltpu.VMEM((2, 256, 256), BF16),
            pltpu.VMEM((2, 256, 512), BF16),
            pltpu.VMEM((3, 512, 256), BF16),
            pltpu.VMEM((4, 8, 8, 128), F32),
            pltpu.VMEM((4, 8, 8, 128), F32),
            pltpu.VMEM((256, 512), F32),
            pltpu.VMEM((1024, 128), F32),
            pltpu.VMEM((1024, 128), F32),
            pltpu.VMEM((1024, 128), F32),
            pltpu.VMEM((1024, 128), F32),
            pltpu.VMEM((4, 2, 4, 1, 128), F32),
        ] + features_scratch() + [
            pltpu.VMEM((144 * KF, 128), BF16),
            pltpu.VMEM((256, 128), F32),
            pltpu.VMEM((128, 128), F32),
            pltpu.VMEM((2, 512, 384), BF16),
            pltpu.VMEM((4, 2, 3, 4, 128), F32),
            DMA((12,)),
            DMA((26,)), DMA((26,)), DMA((3,)), DMA((3,)), DMA((26,)), DMA((26,)), DMA((1,)), DMA((1,)),
            DMA((1,)), DMA((1,)), DMA((3,)), DMA((3,)), DMA((1,)),
        ],
        compiler_params=pltpu.CompilerParams(collective_id=0, has_side_effects=True, vmem_limit_bytes=67043328),
        name="front_pass",
    )(*arrays)


def on_device(cell_counts, grid_offset, fraction, species, species_density, species_pair, species_embed, species_charge):
    table, turned, mixed, mixed_turned = constants()
    order = (0, 1, 3, 2, 4)
    extended, density, wide_slope, electric, features = front_pass(
        species_charge, species_density, species_pair, species_embed, cell_counts, grid_offset.transpose(order),
        fraction.transpose(order), species, table, turned, mixed, mixed_turned)
    forces, density = force_pass(
        cell_counts, species_density, species_pair, extended, wide_slope, density, electric.reshape(8, 3, 4, 128),
        features)
    return forces.reshape(4, 2, 3, 4, 128).transpose(order), density.reshape(4, 2, 4, 128)


def solution(mesh):
    return jax.shard_map(
        on_device,
        mesh=mesh,
        in_specs=(
            P("gx", "gy", "gz"),
            P("gx", "gy", "gz", None, None),
            P("gx", "gy", "gz", None, None),
            P("gx", "gy", "gz", None),
            P(),
            P(),
            P(),
            P(),
        ),
        out_specs=(P("gx", "gy", "gz", None, None), P("gx", "gy", "gz", None)),
        check_vma=False,
    )
```
